8 devices in a mesh: dp: 2 (over z, y), tp: 4 (over x, core).
Axes of the slice: x: 2, y: 2, z: 1, core: 2. Of those that a mesh axis runs over, the one named last changes fastest.
Arguments:
- irreps: bfloat16 [256, 25, 128], P('dp', None, 'tp')
- norm_gain: float32 [5, 128], P(None, 'tp')
- w_up: bfloat16 [5, 128, 512], P(None, None, 'tp')
- w_gate: bfloat16 [128, 512], P(None, 'tp')
- w_down: bfloat16 [5, 512, 128], P(None, 'tp')
- to_grid: float32 [25, 324], replicated
- from_grid: float32 [324, 24], replicated
- grad_out: bfloat16 [256, 25, 128], P('dp', None, 'tp')
Outputs:
- output 1: bfloat16 [256, 25, 128], P('dp', None, 'tp')
- output 2: bfloat16 [256, 25, 128], P('dp', None, 'tp')
- output 3: bfloat16 [5, 128, 512], P(None, None, 'tp')
- output 4: bfloat16 [128, 512], P(None, 'tp')
- output 5: bfloat16 [5, 512, 128], P(None, 'tp')
All inputs are finite; a program needn't handle non-finite values.
Results may differ from the reference program's by a relative error of at most 0.0125651.
Values are sent between devices in bfloat16 or wider.
A program may use at most 1 GiB of HBM per device.

```python
import math
import jax
import jax.numpy as jnp
from jax import lax

N_NODES = 256
CHANNELS = 128
HIDDEN = 512
DEG_MAX = 4
GRID_PTS = 324

DEGREES = DEG_MAX + 1
COEFS = DEGREES * DEGREES
ROW_BLOCK = math.gcd(N_NODES, 128)
NORM_EPS = 1e-5


def setup_inputs(seed: int = 0) -> dict:
    key_list = jax.random.split(jax.random.key(seed), 11)
    chan_pos = jnp.arange(CHANNELS, dtype=jnp.float32) / CHANNELS
    chan_scale = jnp.exp(2.4 * (chan_pos - 0.5) + 0.3 * jax.random.normal(key_list[0], (CHANNELS,)))
    node_scale = jnp.exp(0.4 * jax.random.normal(key_list[1], (N_NODES, 1, 1)))
    scalar_row = (jnp.arange(COEFS) == 0).astype(jnp.float32)[:, None]
    offsets = 0.8 * jax.random.normal(key_list[2], (CHANNELS,))
    noise_draw = jax.random.normal(key_list[3], (N_NODES, COEFS, CHANNELS))
    irreps = node_scale * chan_scale * (noise_draw + scalar_row * offsets)
    norm_gain = 0.6 + 0.8 * jax.random.uniform(key_list[4], (DEGREES, CHANNELS))
    w_up = jax.random.normal(key_list[5], (DEGREES, CHANNELS, HIDDEN)) * CHANNELS ** -0.5
    w_gate = jax.random.normal(key_list[6], (CHANNELS, HIDDEN)) * CHANNELS ** -0.5
    w_down = jax.random.normal(key_list[7], (DEGREES, HIDDEN, CHANNELS)) * HIDDEN ** -0.5
    to_grid = jax.random.normal(key_list[8], (COEFS, GRID_PTS)) * COEFS ** -0.5
    from_grid = jax.random.normal(key_list[9], (GRID_PTS, COEFS - 1)) * GRID_PTS ** -0.5
    grad_out = jax.random.normal(key_list[10], (N_NODES, COEFS, CHANNELS))
    return {'irreps': irreps.astype(jnp.bfloat16), 'norm_gain': norm_gain, 'w_up': w_up.astype(jnp.bfloat16), 'w_gate': w_gate.astype(jnp.bfloat16), 'w_down': w_down.astype(jnp.bfloat16), 'to_grid': to_grid, 'from_grid': from_grid, 'grad_out': grad_out.astype(jnp.bfloat16)}


def expand_rows(per_degree):
    return jnp.concatenate([jnp.broadcast_to(per_degree[degree:degree + 1], (2 * degree + 1,) + per_degree.shape[1:]) for degree in range(per_degree.shape[0])], axis=0)


def block_forward(x_blk, norm_gain, up_f, gate_f, down_f, grid_in, grid_back):
    x_f = x_blk.astype(jnp.float32)
    scalar = x_f[:, 0, :]
    mean_s = jnp.mean(scalar, axis=-1, keepdims=True)
    centered = scalar - mean_s
    var_s = jnp.mean(centered * centered, axis=-1, keepdims=True)
    vector = x_f[:, 1:, :]
    mean_sq = jnp.mean(vector * vector, axis=(1, 2), keepdims=True)
    normed = jnp.concatenate([(centered * lax.rsqrt(var_s + NORM_EPS))[:, None, :], vector * lax.rsqrt(mean_sq + NORM_EPS)], axis=1)
    normed = (normed * expand_rows(norm_gain)).astype(jnp.bfloat16).astype(jnp.float32)
    hidden_act = jnp.einsum('nkc,kch->nkh', normed, expand_rows(up_f)).astype(jnp.bfloat16).astype(jnp.float32)
    pre_gate = jnp.einsum('nc,ch->nh', normed[:, 0, :], gate_f).astype(jnp.bfloat16).astype(jnp.float32)
    gate_val = jax.nn.silu(pre_gate).astype(jnp.bfloat16)
    pre_grid = jnp.einsum('nkh,kg->ngh', hidden_act, grid_in).astype(jnp.bfloat16).astype(jnp.float32)
    grid_val = jax.nn.silu(pre_grid).astype(jnp.bfloat16).astype(jnp.float32)
    back_proj = jnp.einsum('ngh,gk->nkh', grid_val, grid_back).astype(jnp.bfloat16)
    mixed_act = jnp.concatenate([gate_val[:, None, :], back_proj], axis=1).astype(jnp.float32)
    ffn_delta = jnp.einsum('nkh,khc->nkc', mixed_act, expand_rows(down_f))
    return (x_f + ffn_delta).astype(jnp.bfloat16)


def reference(irreps, norm_gain, w_up, w_gate, w_down, to_grid, from_grid, grad_out):
    up_f = w_up.astype(jnp.float32)
    gate_f = w_gate.astype(jnp.float32)
    down_f = w_down.astype(jnp.float32)
    grid_in = to_grid.astype(jnp.bfloat16).astype(jnp.float32)
    grid_back = from_grid.astype(jnp.bfloat16).astype(jnp.float32)
    blk_count = N_NODES // ROW_BLOCK
    x_blocks = irreps.reshape(blk_count, ROW_BLOCK, COEFS, CHANNELS)
    g_blocks = grad_out.reshape(blk_count, ROW_BLOCK, COEFS, CHANNELS)

    def scan_step(grad_sums, blk_pair):
        def local_fn(x_in, up_in, gate_in, down_in):
            return block_forward(x_in, norm_gain, up_in, gate_in, down_in, grid_in, grid_back)
        out_blk, pull_back = jax.vjp(local_fn, blk_pair[0], up_f, gate_f, down_f)
        dx_blk, d_up, d_gate, d_down = pull_back(blk_pair[1])
        new_sums = (grad_sums[0] + d_up, grad_sums[1] + d_gate, grad_sums[2] + d_down)
        return new_sums, (out_blk, dx_blk)

    init_sums = (jnp.zeros_like(up_f), jnp.zeros_like(gate_f), jnp.zeros_like(down_f))
    total_sums, (out_blocks, dx_blocks) = lax.scan(scan_step, init_sums, (x_blocks, g_blocks))
    out_irreps = out_blocks.reshape(N_NODES, COEFS, CHANNELS)
    d_irreps = dx_blocks.reshape(N_NODES, COEFS, CHANNELS)
    return (out_irreps, d_irreps, total_sums[0].astype(jnp.bfloat16), total_sums[1].astype(jnp.bfloat16), total_sums[2].astype(jnp.bfloat16))
```

```python
import functools
import math
import jax
import jax.numpy as jnp
from jax import lax
from jax.experimental import pallas as pl
from jax.experimental.pallas import tpu as pltpu
from jax.sharding import PartitionSpec as P

NORM_EPS = 1e-5
MESH = pl.DeviceIdType.MESH
F32 = jnp.float32
BF16 = jnp.bfloat16
COEFS = 25
KPAD = 32
YSTRIDE = 40
UNROLL = 2


def degree_of(k):
    return math.isqrt(k)


def rows_dot(a, b):
    return lax.dot_general(a, b, (((1,), (0,)), ((), ())), preferred_element_type=F32)


def lanes_dot(a, b):
    return lax.dot_general(a, b, (((1,), (1,)), ((), ())), preferred_element_type=F32)


def kernel(tp_size, grid_pts, x_hbm, gain_hbm, up_hbm, gate_hbm, down_hbm, tog_hbm, frg_hbm, g_hbm,
           out_ref, dx_ref, dup_ref, dgate_ref, ddown_ref,
           xg, gg, xn, mb, dyb, dpart, npart, ya, yb, zs, hs,
           gain_in, gain_snd, gain_all, gcol, up, gate, down, upt, gatet, downt,
           tog, frg, tt, tmat, fmat, ft, rb1, sb, rb2, nrb1, nsb, nrb2,
           st_snd, st_all, gdn, gdn_rb, gup, gup_rb, amat,
           loc_sem, snd_sem, rcv_sem):
    dp = lax.axis_index("dp")
    t = lax.axis_index("tp")
    core = lax.rem(t, 2)
    t1 = t + 1 - 2 * core
    t2 = lax.rem(t + 2, 4)
    t3 = lax.rem(t1 + 2, 4)
    odp = 1 - dp
    cl = xg.shape[1] // tp_size
    ch = xg.shape[1]
    nat = xg.shape[2]
    pp = tt.shape[0]

    def blk(i):
        return pl.ds(pl.multiple_of(i * cl, cl), cl)

    def local(src, dst, i):
        c = pltpu.make_async_copy(src, dst, loc_sem.at[i])
        c.start()
        return c

    def remote(src, dst, i, dev):
        return pltpu.make_async_remote_copy(src_ref=src, dst_ref=dst, send_sem=snd_sem.at[i], recv_sem=rcv_sem.at[i],
                                            device_id=dev, device_id_type=MESH)

    c_gain = local(gain_hbm, gain_in, 0)
    c_x = local(x_hbm, xg.at[:, blk(t), :], 1)
    c_tog = local(tog_hbm, tog, 2)
    c_frg = local(frg_hbm, frg, 3)
    c_up = local(up_hbm, up, 4)
    c_gate = local(gate_hbm, gate, 5)
    c_down = local(down_hbm, down, 6)
    c_g = local(g_hbm, gg.at[:, blk(t), :], 7)

    barrier = pltpu.get_barrier_semaphore()
    for dev in ({"tp": t1}, {"tp": t2}, {"tp": t3}, {"dp": odp}):
        pl.semaphore_signal(barrier, inc=1, device_id=dev, device_id_type=MESH)
    pl.semaphore_wait(barrier, 4)

    ksplit = ((0, 7), (7, 13), (13, 19), (19, 25))

    def gather_start(src, dst, base):
        far, near = [], None
        for j, (k0, k1) in enumerate(ksplit):
            c = remote(src.at[k0:k1], dst.at[k0:k1, blk(t), :], base + j, {"tp": t2})
            c.start()
            far.append(c)
        near = remote(src, dst.at[:, blk(t), :], base + 4, {"tp": t1})
        near.start()
        return far, near

    def gather_finish(far, near, dst, base):
        fwd = []
        for j, (k0, k1) in enumerate(ksplit):
            far[j].wait_recv()
            c = remote(dst.at[k0:k1, blk(t2), :], dst.at[k0:k1, blk(t2), :], base + 5 + j, {"tp": t1})
            c.start()
            fwd.append(c)
        near.wait_recv()
        for c in fwd:
            c.wait_recv()
        return fwd

    far_x, near_x = gather_start(x_hbm, xg, 0)

    gain_snd[...] = jnp.zeros_like(gain_snd)
    c_gain.wait()
    gain_snd[0:5, 0:cl] = gain_in[...]
    placed = pltpu.roll(gain_snd[...], t * cl, 1)
    gain_snd[...] = placed
    gsend = []
    for j, dev in enumerate((t1, t2, t3)):
        c = remote(gain_snd, gain_all.at[j], 20 + j, {"tp": dev})
        c.start()
        gsend.append(c)

    c_tog.wait()
    c_frg.wait()
    tpad = jnp.zeros((KPAD, 384), F32)
    tmat[...] = tpad.astype(BF16)
    ft[...] = tpad.astype(BF16)
    tmat[0:COEFS, 0:grid_pts] = tog[...].astype(BF16)
    frg_pad = jnp.concatenate([jnp.zeros((1, grid_pts), F32), frg[...]], axis=0)
    ft[0:COEFS, 0:grid_pts] = frg_pad.astype(BF16)
    for src, dst in ((tmat, tt), (ft, fmat)):
        wide = jnp.concatenate([src[...].astype(F32) * 0.5, jnp.zeros((128 - KPAD, 384), F32)], axis=0)
        for j in range(3):
            tr = wide[:, 128 * j:128 * (j + 1)].T
            rows = min(128, pp - 128 * j)
            dst[128 * j:128 * j + rows, :] = tr[0:rows, 0:KPAD].astype(BF16)
    c_up.wait()
    c_gate.wait()
    c_down.wait()
    for l in range(5):
        upt[l] = up[l].astype(F32).T.astype(BF16)
        downt[l] = down[l].astype(F32).T.astype(BF16)
    gatet[...] = gate[...].astype(F32).T.astype(BF16)
    ya[...] = jnp.zeros_like(ya)
    yb[...] = jnp.zeros_like(yb)
    for c in gsend:
        c.wait_recv()
    gain_full = placed + gain_all[0] + gain_all[1] + gain_all[2]
    for l in range(5):
        gcol[l] = jnp.broadcast_to(gain_full[l:l + 1, :], (ch, ch)).T

    c_x.wait()
    fwd_x = gather_finish(far_x, near_x, xg, 0)
    for c in far_x:
        c.wait_send()
    far_g, near_g = gather_start(g_hbm, gg, 10)

    x0 = xg[0].astype(F32)
    mean_s = jnp.sum(x0, axis=0, keepdims=True) / ch
    cent = x0 - mean_s
    inv_s = lax.rsqrt(jnp.sum(cent * cent, axis=0, keepdims=True) / ch + NORM_EPS)
    hat_s = cent * inv_s
    acc = jnp.zeros((ch, nat), F32)
    for k in range(1, COEFS):
        v = xg[k].astype(F32)
        acc = acc + v * v
    inv_v = lax.rsqrt(jnp.sum(acc, axis=0, keepdims=True) / (ch * (COEFS - 1)) + NORM_EPS)
    xn[0] = (hat_s * gcol[0]).astype(BF16)
    for k in range(1, COEFS):
        xn[k] = (xg[k].astype(F32) * inv_v * gcol[degree_of(k)]).astype(BF16)

    def spread(get, lhs_of):
        for l in range(5):
            k0, k1 = l * l, (l + 1) * (l + 1)
            lhs = lhs_of(l)
            for k in range(k0, k1):
                r = rows_dot(lhs, get(k))
                ya[pl.ds(k, 64, stride=YSTRIDE), :] = r[0:64]
                yb[pl.ds(k, 64, stride=YSTRIDE), :] = r[64:128]

    spread(lambda k: xn[k], lambda l: upt[l])
    a_r = rows_dot(gatet[...], xn[0]).astype(BF16)
    amat[...] = a_r
    a_h = a_r.astype(F32) * 0.5
    mb[0] = (a_h * (1.0 + jnp.tanh(a_h))).astype(BF16)

    def pair(i):
        base = pl.multiple_of(i * YSTRIDE, 8)
        return jnp.concatenate([ya[pl.ds(base, KPAD), :], yb[pl.ds(base, KPAD), :]], axis=1).astype(BF16)

    def put(i, r):
        zs[pl.ds(i, KPAD, stride=136), :] = r[:, 0:128]
        zs[pl.ds(i + 64, KPAD, stride=136), :] = r[:, 128:256]

    def fwd_body(it, carry):
        for j in range(UNROLL):
            i = it * UNROLL + j
            hb = rows_dot(tt[...], pair(i)).astype(BF16)
            hs[pl.ds(pl.multiple_of(i * pp, 16), pp), :] = hb
            h = hb.astype(F32)
            s = (h * (1.0 + jnp.tanh(h))).astype(BF16)
            put(i, rows_dot(ft[:, 0:pp], s))
        return carry

    lax.fori_loop(0, 64 // UNROLL, fwd_body, 0)

    for k in range(1, COEFS):
        mb[k] = zs[k * 136:k * 136 + 128, :].astype(BF16)
    for k in range(COEFS):
        dpart[k] = rows_dot(downt[degree_of(k)], mb[k]).astype(BF16)

    def scatter_near(part, rb, base):
        cs = []
        for j, b in enumerate((t3, t1)):
            c = remote(part.at[:, blk(b), :], rb.at[j], base + j, {"tp": t1})
            c.start()
            cs.append(c)
        return cs

    near_d = scatter_near(dpart, rb1, 23)

    fwd_g = gather_finish(far_g, near_g, gg, 10)
    c_g.wait()
    spread(lambda k: gg[k], lambda l: down[l])
    dm0 = rows_dot(down[0], gg[0]).astype(BF16).astype(F32)
    a_h = amat[...].astype(F32) * 0.5
    w_a = 1.0 + jnp.tanh(a_h)
    da = (dm0 * (0.5 * w_a * (1.0 + a_h * (2.0 - w_a)))).astype(BF16)

    near_d[0].wait_recv()
    sb[...] = (dpart[:, blk(t2), :].astype(F32) + rb1[0].astype(F32)).astype(BF16)
    for l in range(5):
        acc = jnp.zeros((128, ch), F32)
        for k in range(l * l, (l + 1) * (l + 1)):
            acc = acc + lanes_dot(mb[k], gg[k])
        gdn[l] = acc
    far_d = remote(sb, rb2, 25, {"tp": t2})
    far_d.start()
    half = 64
    mine = pl.ds(pl.multiple_of(dp * half, half), half)
    theirs = pl.ds(pl.multiple_of(odp * half, half), half)
    ex_dn = remote(gdn.at[:, theirs, :], gdn_rb, 26, {"dp": odp})
    ex_dn.start()

    def bwd_body(it, carry):
        for j in range(UNROLL):
            i = it * UNROLL + j
            dg = rows_dot(fmat[...], pair(i)).astype(BF16).astype(F32)
            h = hs[pl.ds(pl.multiple_of(i * pp, 16), pp), :].astype(F32)
            w = 1.0 + jnp.tanh(h)
            dpre = (dg * (w * (1.0 + h * (2.0 - w)))).astype(BF16)
            put(i, rows_dot(tmat[:, 0:pp], dpre))
        return carry

    lax.fori_loop(0, 64 // UNROLL, bwd_body, 0)

    for k in range(COEFS):
        dyb[k] = zs[k * 136:k * 136 + 128, :].astype(BF16)
    s3 = jnp.zeros((ch, nat), F32)
    for k in range(COEFS):
        r = rows_dot(up[degree_of(k)], dyb[k])
        if k == 0:
            r = r + rows_dot(gate[...], da)
        rb = r.astype(BF16)
        npart[k] = rb
        rf = rb.astype(F32) * gcol[degree_of(k)]
        if k == 0:
            st0 = jnp.sum(rf, axis=0, keepdims=True)
            st1 = jnp.sum(rf * hat_s, axis=0, keepdims=True)
        else:
            s3 = s3 + rf * xg[k].astype(F32)
    st2 = jnp.sum(s3, axis=0, keepdims=True)
    near_n = scatter_near(npart, nrb1, 27)
    stat = jnp.concatenate([st0, st1, st2, jnp.zeros((5, nat), F32)], axis=0)
    st_snd[...] = stat

    for l in range(5):
        acc = jnp.zeros((ch, 128), F32)
        for k in range(l * l, (l + 1) * (l + 1)):
            acc = acc + lanes_dot(xn[k], dyb[k])
        gup[l] = acc
    gup[5] = lanes_dot(xn[0], da)
    ssend = []
    for j, dev in enumerate((t1, t2, t3)):
        c = remote(st_snd, st_all.at[j], 30 + j, {"tp": dev})
        c.start()
        ssend.append(c)
    near_n[0].wait_recv()
    nsb[...] = (npart[:, blk(t2), :].astype(F32) + nrb1[0].astype(F32)).astype(BF16)
    ex_up = remote(gup.at[:, theirs, :], gup_rb, 33, {"dp": odp})
    ex_up.start()
    far_n = remote(nsb, nrb2, 29, {"tp": t2})
    far_n.start()

    ex_dn.wait_recv()
    ddown_ref[:, mine, :] = (gdn[:, mine, :] + gdn_rb[...]).astype(BF16)
    near_d[1].wait_recv()
    far_d.wait_recv()
    own = dpart[:, blk(t), :].astype(F32) + rb1[1].astype(F32) + rb2[...].astype(F32)
    out_ref[...] = (xg[:, blk(t), :].astype(F32) + own).astype(BF16)
    bk_dn = remote(ddown_ref.at[:, mine, :], ddown_ref.at[:, mine, :], 34, {"dp": odp})
    bk_dn.start()

    ex_up.wait_recv()
    dup_ref[:, mine, :] = (gup[0:5, mine, :] + gup_rb[0:5]).astype(BF16)
    dgate_ref[mine, :] = (gup[5, mine, :] + gup_rb[5]).astype(BF16)
    for c in ssend:
        c.wait_recv()
    stat = st_snd[...] + st_all[0] + st_all[1] + st_all[2]
    bk_up = remote(dup_ref.at[:, mine, :], dup_ref.at[:, mine, :], 35, {"dp": odp})
    bk_up.start()
    bk_gt = remote(dgate_ref.at[mine, :], dgate_ref.at[mine, :], 36, {"dp": odp})
    bk_gt.start()
    b0 = stat[0:1] / ch
    b1 = stat[1:2] / ch
    b2 = (inv_v * inv_v * inv_v) * (stat[2:3] / (ch * (COEFS - 1)))
    near_n[1].wait_recv()
    far_n.wait_recv()
    for k in range(COEFS):
        dn = (npart[k, blk(t), :].astype(F32) + nrb1[1, k].astype(F32) + nrb2[k].astype(F32)).astype(BF16).astype(F32)
        dhat = dn * gcol[degree_of(k), blk(t), :]
        xk = xg[k, blk(t), :].astype(F32)
        if k == 0:
            dxk = inv_s * (dhat - b0 - (xk - mean_s) * inv_s * b1)
        else:
            dxk = inv_v * dhat - xk * b2
        dx_ref[k] = (dxk + gg[k, blk(t), :].astype(F32)).astype(BF16)

    bk_dn.wait_recv()
    bk_up.wait_recv()
    bk_gt.wait_recv()
    for c in far_g + fwd_x + fwd_g + gsend + near_d + near_n + ssend + [near_x, near_g, far_d, far_n, ex_dn, ex_up, bk_dn, bk_up, bk_gt]:
        c.wait_send()


def solution(mesh):
    tp_size = mesh.shape['tp']
    act_spec = P('dp', None, 'tp')
    in_specs = (act_spec, P(None, 'tp'), P(None, None, 'tp'), P(None, 'tp'), P(None, 'tp', None), P(None, None), P(None, None), act_spec)
    out_specs = (act_spec, act_spec, P(None, None, 'tp'), P(None, 'tp'), P(None, 'tp', None))

    def local_step(x_loc, gain_loc, up_loc, gate_loc, down_loc, to_grid, from_grid, grad_loc):
        nat, coefs, cl = x_loc.shape
        ch = cl * tp_size
        grid_pts = to_grid.shape[1]
        pp = -(-grid_pts // 16) * 16
        xt = x_loc.transpose(1, 2, 0)
        gt = grad_loc.transpose(1, 2, 0)
        any_spec = pl.BlockSpec(memory_space=pl.ANY)
        vmem = pl.BlockSpec(memory_space=pltpu.VMEM)
        full = pltpu.VMEM((coefs, ch, nat), BF16)
        blkb = pltpu.VMEM((coefs, cl, nat), BF16)
        sq = lambda n, d: pltpu.VMEM((n, 128, 128), d)
        outs = pl.pallas_call(
            functools.partial(kernel, tp_size, grid_pts),
            out_shape=(jax.ShapeDtypeStruct(xt.shape, BF16), jax.ShapeDtypeStruct(xt.shape, BF16),
                       jax.ShapeDtypeStruct(up_loc.shape, BF16), jax.ShapeDtypeStruct(gate_loc.shape, BF16),
                       jax.ShapeDtypeStruct(down_loc.shape, BF16)),
            in_specs=[any_spec] * 8,
            out_specs=[vmem] * 5,
            scratch_shapes=[
                full, full, full, full, full, full, full,
                pltpu.VMEM((64 * YSTRIDE, 128), F32), pltpu.VMEM((64 * YSTRIDE, 128), F32),
                pltpu.VMEM((KPAD * 136, 128), F32), pltpu.VMEM((64 * pp, 256), BF16),
                pltpu.VMEM(gain_loc.shape, F32), pltpu.VMEM((8, 128), F32), pltpu.VMEM((3, 8, 128), F32), sq(5, F32),
                sq(5, BF16), pltpu.VMEM((128, 128), BF16), sq(5, BF16), sq(5, BF16), pltpu.VMEM((128, 128), BF16), sq(5, BF16),
                pltpu.VMEM(to_grid.shape, F32), pltpu.VMEM(from_grid.shape[::-1], F32),
                pltpu.VMEM((pp, KPAD), BF16), pltpu.VMEM((KPAD, 384), BF16), pltpu.VMEM((pp, KPAD), BF16), pltpu.VMEM((KPAD, 384), BF16),
                pltpu.VMEM((2, coefs, cl, nat), BF16), blkb, blkb, pltpu.VMEM((2, coefs, cl, nat), BF16), blkb, blkb,
                pltpu.VMEM((8, 128), F32), pltpu.VMEM((3, 8, 128), F32),
                sq(5, F32), pltpu.VMEM((5, 64, 128), F32), sq(6, F32), pltpu.VMEM((6, 64, 128), F32),
                pltpu.VMEM((128, nat), BF16),
                pltpu.SemaphoreType.DMA((8,)), pltpu.SemaphoreType.DMA((40,)), pltpu.SemaphoreType.DMA((40,)),
            ],
            compiler_params=pltpu.CompilerParams(collective_id=0, has_side_effects=True, vmem_limit_bytes=60 * 1024 * 1024),
        )(xt, gain_loc, up_loc, gate_loc, down_loc, to_grid, from_grid.T, gt)
        out_t, dx_t, d_up, d_gate, d_down = outs
        return out_t.transpose(2, 0, 1), dx_t.transpose(2, 0, 1), d_up, d_gate, d_down

    return jax.shard_map(local_step, mesh=mesh, in_specs=in_specs, out_specs=out_specs, check_vma=False)
```

```python
import functools
import math
import jax
import jax.numpy as jnp
from jax import lax
from jax.experimental import pallas as pl
from jax.experimental.pallas import tpu as pltpu
from jax.sharding import PartitionSpec as P

NORM_EPS = 1e-5
MESH = pl.DeviceIdType.MESH
F32 = jnp.float32
BF16 = jnp.bfloat16
COEFS = 25
KPAD = 32
YSTRIDE = 40
UNROLL = 2


def degree_of(k):
    return math.isqrt(k)


def rows_dot(a, b):
    return lax.dot_general(a, b, (((1,), (0,)), ((), ())), preferred_element_type=F32)


def lanes_dot(a, b):
    return lax.dot_general(a, b, (((1,), (1,)), ((), ())), preferred_element_type=F32)


def kernel(tp_size, grid_pts, x_hbm, gain_hbm, up_hbm, gate_hbm, down_hbm, tog_hbm, frg_hbm, g_hbm,
           out_ref, dx_ref, dup_ref, dgate_ref, ddown_ref,
           xg, gg, xn, mb, dyb, dpart, npart, ya, yb, zs, hs,
           gain_in, gain_snd, gain_all, gcol, up, gate, down, upt, gatet, downt,
           tog, frg, tt, tmat, fmat, ft, rb1, sb, rb2, nrb1, nsb, nrb2,
           st_snd, st_all, gdn, gdn_rb, gup, gup_rb, amat, sbuf0, sbuf1, gbuf0, gbuf1,
           loc_sem, snd_sem, rcv_sem):
    sbuf, gbuf = (sbuf0, sbuf1), (gbuf0, gbuf1)
    dp = lax.axis_index("dp")
    t = lax.axis_index("tp")
    core = lax.rem(t, 2)
    t1 = t + 1 - 2 * core
    t2 = lax.rem(t + 2, 4)
    t3 = lax.rem(t1 + 2, 4)
    odp = 1 - dp
    cl = xg.shape[1] // tp_size
    ch = xg.shape[1]
    nat = xg.shape[2]
    pp = tt.shape[0]

    def blk(i):
        return pl.ds(pl.multiple_of(i * cl, cl), cl)

    def local(src, dst, i):
        c = pltpu.make_async_copy(src, dst, loc_sem.at[i])
        c.start()
        return c

    def remote(src, dst, i, dev):
        return pltpu.make_async_remote_copy(src_ref=src, dst_ref=dst, send_sem=snd_sem.at[i], recv_sem=rcv_sem.at[i],
                                            device_id=dev, device_id_type=MESH)

    c_gain = local(gain_hbm, gain_in, 0)
    c_x = local(x_hbm, xg.at[:, blk(t), :], 1)
    c_tog = local(tog_hbm, tog, 2)
    c_frg = local(frg_hbm, frg, 3)
    c_up = local(up_hbm, up, 4)
    c_gate = local(gate_hbm, gate, 5)
    c_down = local(down_hbm, down, 6)
    c_g = local(g_hbm, gg.at[:, blk(t), :], 7)

    barrier = pltpu.get_barrier_semaphore()
    for dev in ({"tp": t1}, {"tp": t2}, {"tp": t3}, {"dp": odp}):
        pl.semaphore_signal(barrier, inc=1, device_id=dev, device_id_type=MESH)
    pl.semaphore_wait(barrier, 4)

    ksplit = ((0, 7), (7, 13), (13, 19), (19, 25))

    def gather_start(src, dst, base):
        far, near = [], None
        for j, (k0, k1) in enumerate(ksplit):
            c = remote(src.at[k0:k1], dst.at[k0:k1, blk(t), :], base + j, {"tp": t2})
            c.start()
            far.append(c)
        near = remote(src, dst.at[:, blk(t), :], base + 4, {"tp": t1})
        near.start()
        return far, near

    def gather_finish(far, near, dst, base):
        fwd = []
        for j, (k0, k1) in enumerate(ksplit):
            far[j].wait_recv()
            c = remote(dst.at[k0:k1, blk(t2), :], dst.at[k0:k1, blk(t2), :], base + 5 + j, {"tp": t1})
            c.start()
            fwd.append(c)
        near.wait_recv()
        for c in fwd:
            c.wait_recv()
        return fwd

    far_x, near_x = gather_start(x_hbm, xg, 0)

    gain_snd[...] = jnp.zeros_like(gain_snd)
    c_gain.wait()
    gain_snd[0:5, 0:cl] = gain_in[...]
    placed = pltpu.roll(gain_snd[...], t * cl, 1)
    gain_snd[...] = placed
    gsend = []
    for j, dev in enumerate((t1, t2, t3)):
        c = remote(gain_snd, gain_all.at[j], 20 + j, {"tp": dev})
        c.start()
        gsend.append(c)

    c_tog.wait()
    c_frg.wait()
    tpad = jnp.zeros((KPAD, 384), F32)
    tmat[...] = tpad.astype(BF16)
    ft[...] = tpad.astype(BF16)
    tmat[0:COEFS, 0:grid_pts] = tog[...].astype(BF16)
    frg_pad = jnp.concatenate([jnp.zeros((1, grid_pts), F32), frg[...]], axis=0)
    ft[0:COEFS, 0:grid_pts] = frg_pad.astype(BF16)
    for src, dst in ((tmat, tt), (ft, fmat)):
        wide = jnp.concatenate([src[...].astype(F32) * 0.5, jnp.zeros((128 - KPAD, 384), F32)], axis=0)
        for j in range(3):
            tr = wide[:, 128 * j:128 * (j + 1)].T
            rows = min(128, pp - 128 * j)
            dst[128 * j:128 * j + rows, :] = tr[0:rows, 0:KPAD].astype(BF16)
    c_up.wait()
    c_gate.wait()
    c_down.wait()
    for l in range(5):
        upt[l] = up[l].astype(F32).T.astype(BF16)
        downt[l] = down[l].astype(F32).T.astype(BF16)
    gatet[...] = gate[...].astype(F32).T.astype(BF16)
    ya[...] = jnp.zeros_like(ya)
    yb[...] = jnp.zeros_like(yb)
    for c in gsend:
        c.wait_recv()
    gain_full = placed + gain_all[0] + gain_all[1] + gain_all[2]
    for l in range(5):
        gcol[l] = jnp.broadcast_to(gain_full[l:l + 1, :], (ch, ch)).T

    c_x.wait()
    fwd_x = gather_finish(far_x, near_x, xg, 0)
    for c in far_x:
        c.wait_send()
    far_g, near_g = gather_start(g_hbm, gg, 10)

    x0 = xg[0].astype(F32)
    mean_s = jnp.sum(x0, axis=0, keepdims=True) / ch
    cent = x0 - mean_s
    inv_s = lax.rsqrt(jnp.sum(cent * cent, axis=0, keepdims=True) / ch + NORM_EPS)
    hat_s = cent * inv_s
    acc = jnp.zeros((ch, nat), F32)
    for k in range(1, COEFS):
        v = xg[k].astype(F32)
        acc = acc + v * v
    inv_v = lax.rsqrt(jnp.sum(acc, axis=0, keepdims=True) / (ch * (COEFS - 1)) + NORM_EPS)
    xn[0] = (hat_s * gcol[0]).astype(BF16)
    for k in range(1, COEFS):
        xn[k] = (xg[k].astype(F32) * inv_v * gcol[degree_of(k)]).astype(BF16)

    def spread(get, lhs_of):
        for l in range(5):
            k0, k1 = l * l, (l + 1) * (l + 1)
            lhs = lhs_of(l)
            for k in range(k0, k1):
                r = rows_dot(lhs, get(k))
                ya[pl.ds(k, 64, stride=YSTRIDE), :] = r[0:64]
                yb[pl.ds(k, 64, stride=YSTRIDE), :] = r[64:128]

    spread(lambda k: xn[k], lambda l: upt[l])
    a_r = rows_dot(gatet[...], xn[0]).astype(BF16)
    amat[...] = a_r
    a_h = a_r.astype(F32) * 0.5
    mb[0] = (a_h * (1.0 + jnp.tanh(a_h))).astype(BF16)

    def pair(i):
        base = pl.multiple_of(i * YSTRIDE, 8)
        return jnp.concatenate([ya[pl.ds(base, KPAD), :], yb[pl.ds(base, KPAD), :]], axis=1).astype(BF16)

    def put(i, r):
        zs[pl.ds(i, KPAD, stride=136), :] = r[:, 0:128]
        zs[pl.ds(i + 64, KPAD, stride=136), :] = r[:, 128:256]

    def stage_u(p, dst):
        dst[...] = rows_dot(tt[...], pair(p)).astype(BF16)

    def stage_s(p, src, dst):
        hb = src[...]
        hs[pl.ds(pl.multiple_of(p * pp, 16), pp), :] = hb
        h = hb.astype(F32)
        dst[...] = (h * (1.0 + jnp.tanh(h))).astype(BF16)

    def stage_z(p, src, lhs):
        put(p, rows_dot(lhs[:, 0:pp], src[...]))

    stage_u(0, gbuf[0])

    def fwd_body(it, carry):
        for j in range(UNROLL):
            p = it * UNROLL + j
            stage_z(jnp.maximum(p - 1, 0), sbuf[(j + 1) % 2], ft)
            stage_u(p + 1, gbuf[(j + 1) % 2])
            stage_s(p, gbuf[j % 2], sbuf[j % 2])
        return carry

    lax.fori_loop(0, 64 // UNROLL, fwd_body, 0)
    stage_z(63, sbuf[1], ft)

    for k in range(1, COEFS):
        mb[k] = zs[k * 136:k * 136 + 128, :].astype(BF16)
    for k in range(COEFS):
        dpart[k] = rows_dot(downt[degree_of(k)], mb[k]).astype(BF16)

    def scatter_near(part, rb, base):
        cs = []
        for j, b in enumerate((t3, t1)):
            c = remote(part.at[:, blk(b), :], rb.at[j], base + j, {"tp": t1})
            c.start()
            cs.append(c)
        return cs

    near_d = scatter_near(dpart, rb1, 23)

    fwd_g = gather_finish(far_g, near_g, gg, 10)
    c_g.wait()
    spread(lambda k: gg[k], lambda l: down[l])
    dm0 = rows_dot(down[0], gg[0]).astype(BF16).astype(F32)
    a_h = amat[...].astype(F32) * 0.5
    w_a = 1.0 + jnp.tanh(a_h)
    da = (dm0 * (0.5 * w_a * (1.0 + a_h * (2.0 - w_a)))).astype(BF16)

    near_d[0].wait_recv()
    sb[...] = (dpart[:, blk(t2), :].astype(F32) + rb1[0].astype(F32)).astype(BF16)
    for l in range(5):
        acc = jnp.zeros((128, ch), F32)
        for k in range(l * l, (l + 1) * (l + 1)):
            acc = acc + lanes_dot(mb[k], gg[k])
        gdn[l] = acc
    far_d = remote(sb, rb2, 25, {"tp": t2})
    far_d.start()
    half = 64
    mine = pl.ds(pl.multiple_of(dp * half, half), half)
    theirs = pl.ds(pl.multiple_of(odp * half, half), half)
    ex_dn = remote(gdn.at[:, theirs, :], gdn_rb, 26, {"dp": odp})
    ex_dn.start()

    def stage_g(p, dst):
        dst[...] = rows_dot(fmat[...], pair(p)).astype(BF16)

    def stage_e(p, src, dst):
        dg = src[...].astype(F32)
        h = hs[pl.ds(pl.multiple_of(p * pp, 16), pp), :].astype(F32)
        w = 1.0 + jnp.tanh(h)
        dst[...] = (dg * (w * (1.0 + h * (2.0 - w)))).astype(BF16)

    stage_g(0, gbuf[0])

    def bwd_body(it, carry):
        for j in range(UNROLL):
            p = it * UNROLL + j
            stage_z(jnp.maximum(p - 1, 0), sbuf[(j + 1) % 2], tmat)
            stage_g(p + 1, gbuf[(j + 1) % 2])
            stage_e(p, gbuf[j % 2], sbuf[j % 2])
        return carry

    lax.fori_loop(0, 64 // UNROLL, bwd_body, 0)
    stage_z(63, sbuf[1], tmat)

    for k in range(COEFS):
        dyb[k] = zs[k * 136:k * 136 + 128, :].astype(BF16)
    s3 = jnp.zeros((ch, nat), F32)
    for k in range(COEFS):
        r = rows_dot(up[degree_of(k)], dyb[k])
        if k == 0:
            r = r + rows_dot(gate[...], da)
        rb = r.astype(BF16)
        npart[k] = rb
        rf = rb.astype(F32) * gcol[degree_of(k)]
        if k == 0:
            st0 = jnp.sum(rf, axis=0, keepdims=True)
            st1 = jnp.sum(rf * hat_s, axis=0, keepdims=True)
        else:
            s3 = s3 + rf * xg[k].astype(F32)
    st2 = jnp.sum(s3, axis=0, keepdims=True)
    near_n = scatter_near(npart, nrb1, 27)
    stat = jnp.concatenate([st0, st1, st2, jnp.zeros((5, nat), F32)], axis=0)
    st_snd[...] = stat

    for l in range(5):
        acc = jnp.zeros((ch, 128), F32)
        for k in range(l * l, (l + 1) * (l + 1)):
            acc = acc + lanes_dot(xn[k], dyb[k])
        gup[l] = acc
    gup[5] = lanes_dot(xn[0], da)
    ssend = []
    for j, dev in enumerate((t1, t2, t3)):
        c = remote(st_snd, st_all.at[j], 30 + j, {"tp": dev})
        c.start()
        ssend.append(c)
    near_n[0].wait_recv()
    nsb[...] = (npart[:, blk(t2), :].astype(F32) + nrb1[0].astype(F32)).astype(BF16)
    ex_up = remote(gup.at[:, theirs, :], gup_rb, 33, {"dp": odp})
    ex_up.start()
    far_n = remote(nsb, nrb2, 29, {"tp": t2})
    far_n.start()

    ex_dn.wait_recv()
    ddown_ref[:, mine, :] = (gdn[:, mine, :] + gdn_rb[...]).astype(BF16)
    near_d[1].wait_recv()
    far_d.wait_recv()
    own = dpart[:, blk(t), :].astype(F32) + rb1[1].astype(F32) + rb2[...].astype(F32)
    out_ref[...] = (xg[:, blk(t), :].astype(F32) + own).astype(BF16)
    bk_dn = remote(ddown_ref.at[:, mine, :], ddown_ref.at[:, mine, :], 34, {"dp": odp})
    bk_dn.start()

    ex_up.wait_recv()
    dup_ref[:, mine, :] = (gup[0:5, mine, :] + gup_rb[0:5]).astype(BF16)
    dgate_ref[mine, :] = (gup[5, mine, :] + gup_rb[5]).astype(BF16)
    for c in ssend:
        c.wait_recv()
    stat = st_snd[...] + st_all[0] + st_all[1] + st_all[2]
    bk_up = remote(dup_ref.at[:, mine, :], dup_ref.at[:, mine, :], 35, {"dp": odp})
    bk_up.start()
    bk_gt = remote(dgate_ref.at[mine, :], dgate_ref.at[mine, :], 36, {"dp": odp})
    bk_gt.start()
    b0 = stat[0:1] / ch
    b1 = stat[1:2] / ch
    b2 = (inv_v * inv_v * inv_v) * (stat[2:3] / (ch * (COEFS - 1)))
    near_n[1].wait_recv()
    far_n.wait_recv()
    for k in range(COEFS):
        dn = (npart[k, blk(t), :].astype(F32) + nrb1[1, k].astype(F32) + nrb2[k].astype(F32)).astype(BF16).astype(F32)
        dhat = dn * gcol[degree_of(k), blk(t), :]
        xk = xg[k, blk(t), :].astype(F32)
        if k == 0:
            dxk = inv_s * (dhat - b0 - (xk - mean_s) * inv_s * b1)
        else:
            dxk = inv_v * dhat - xk * b2
        dx_ref[k] = (dxk + gg[k, blk(t), :].astype(F32)).astype(BF16)

    bk_dn.wait_recv()
    bk_up.wait_recv()
    bk_gt.wait_recv()
    for c in far_g + fwd_x + fwd_g + gsend + near_d + near_n + ssend + [near_x, near_g, far_d, far_n, ex_dn, ex_up, bk_dn, bk_up, bk_gt]:
        c.wait_send()


def solution(mesh):
    tp_size = mesh.shape['tp']
    act_spec = P('dp', None, 'tp')
    in_specs = (act_spec, P(None, 'tp'), P(None, None, 'tp'), P(None, 'tp'), P(None, 'tp', None), P(None, None), P(None, None), act_spec)
    out_specs = (act_spec, act_spec, P(None, None, 'tp'), P(None, 'tp'), P(None, 'tp', None))

    def local_step(x_loc, gain_loc, up_loc, gate_loc, down_loc, to_grid, from_grid, grad_loc):
        nat, coefs, cl = x_loc.shape
        ch = cl * tp_size
        grid_pts = to_grid.shape[1]
        pp = -(-grid_pts // 16) * 16
        xt = x_loc.transpose(1, 2, 0)
        gt = grad_loc.transpose(1, 2, 0)
        any_spec = pl.BlockSpec(memory_space=pl.ANY)
        vmem = pl.BlockSpec(memory_space=pltpu.VMEM)
        full = pltpu.VMEM((coefs, ch, nat), BF16)
        blkb = pltpu.VMEM((coefs, cl, nat), BF16)
        sq = lambda n, d: pltpu.VMEM((n, 128, 128), d)
        outs = pl.pallas_call(
            functools.partial(kernel, tp_size, grid_pts),
            out_shape=(jax.ShapeDtypeStruct(xt.shape, BF16), jax.ShapeDtypeStruct(xt.shape, BF16),
                       jax.ShapeDtypeStruct(up_loc.shape, BF16), jax.ShapeDtypeStruct(gate_loc.shape, BF16),
                       jax.ShapeDtypeStruct(down_loc.shape, BF16)),
            in_specs=[any_spec] * 8,
            out_specs=[vmem] * 5,
            scratch_shapes=[
                full, full, full, full, full, full, full,
                pltpu.VMEM((65 * YSTRIDE, 128), F32), pltpu.VMEM((65 * YSTRIDE, 128), F32),
                pltpu.VMEM((KPAD * 136, 128), F32), pltpu.VMEM((65 * pp, 256), BF16),
                pltpu.VMEM(gain_loc.shape, F32), pltpu.VMEM((8, 128), F32), pltpu.VMEM((3, 8, 128), F32), sq(5, F32),
                sq(5, BF16), pltpu.VMEM((128, 128), BF16), sq(5, BF16), sq(5, BF16), pltpu.VMEM((128, 128), BF16), sq(5, BF16),
                pltpu.VMEM(to_grid.shape, F32), pltpu.VMEM(from_grid.shape[::-1], F32),
                pltpu.VMEM((pp, KPAD), BF16), pltpu.VMEM((KPAD, 384), BF16), pltpu.VMEM((pp, KPAD), BF16), pltpu.VMEM((KPAD, 384), BF16),
                pltpu.VMEM((2, coefs, cl, nat), BF16), blkb, blkb, pltpu.VMEM((2, coefs, cl, nat), BF16), blkb, blkb,
                pltpu.VMEM((8, 128), F32), pltpu.VMEM((3, 8, 128), F32),
                sq(5, F32), pltpu.VMEM((5, 64, 128), F32), sq(6, F32), pltpu.VMEM((6, 64, 128), F32),
                pltpu.VMEM((128, nat), BF16),
                pltpu.VMEM((pp, 256), BF16), pltpu.VMEM((pp, 256), BF16), pltpu.VMEM((pp, 256), BF16), pltpu.VMEM((pp, 256), BF16),
                pltpu.SemaphoreType.DMA((8,)), pltpu.SemaphoreType.DMA((40,)), pltpu.SemaphoreType.DMA((40,)),
            ],
            compiler_params=pltpu.CompilerParams(collective_id=0, has_side_effects=True, vmem_limit_bytes=60 * 1024 * 1024),
        )(xt, gain_loc, up_loc, gate_loc, down_loc, to_grid, from_grid.T, gt)
        out_t, dx_t, d_up, d_gate, d_down = outs
        return out_t.transpose(2, 0, 1), dx_t.transpose(2, 0, 1), d_up, d_gate, d_down

    return jax.shard_map(local_step, mesh=mesh, in_specs=in_specs, out_specs=out_specs, check_vma=False)
```

```python
import functools
import math
import jax
import jax.numpy as jnp
from jax import lax
from jax.experimental import pallas as pl
from jax.experimental.pallas import tpu as pltpu
from jax.sharding import PartitionSpec as P

NORM_EPS = 1e-5
MESH = pl.DeviceIdType.MESH
F32 = jnp.float32
BF16 = jnp.bfloat16
COEFS = 25
KPAD = 32
YSTRIDE = 40
UNROLL = 2
QR = 32


def degree_of(k):
    return math.isqrt(k)


def rows_dot(a, b):
    return lax.dot_general(a, b, (((1,), (0,)), ((), ())), preferred_element_type=F32)


def lanes_dot(a, b):
    return lax.dot_general(a, b, (((1,), (1,)), ((), ())), preferred_element_type=F32)


def kernel(tp_size, grid_pts, x_hbm, gain_hbm, up_hbm, gate_hbm, down_hbm, tog_hbm, frg_hbm, g_hbm,
           out_ref, dx_ref, dup_ref, dgate_ref, ddown_ref,
           xg, gg, xn, mb, dyb, dpart, npart, ya, yb, zs, hs,
           gain_in, gain_snd, gain_all, gcol, up, gate, down, upt, gatet, downt,
           tog, frg, tt, tmat, fmat, ft, rb1, sb, rb2, nrb1, nsb, nrb2,
           st_snd, st_all, gdn, gdn_rb, gup, gup_rb, gfin, gfin_dn, amat, sbuf0, sbuf1, gbuf0, gbuf1,
           loc_sem, snd_sem, rcv_sem):
    sbuf, gbuf = (sbuf0, sbuf1), (gbuf0, gbuf1)
    dp = lax.axis_index("dp")
    t = lax.axis_index("tp")
    core = lax.rem(t, 2)
    t1 = t + 1 - 2 * core
    t2 = lax.rem(t + 2, 4)
    t3 = lax.rem(t1 + 2, 4)
    odp = 1 - dp
    cl = xg.shape[1] // tp_size
    ch = xg.shape[1]
    nat = xg.shape[2]
    pp = tt.shape[0]

    def blk(i):
        return pl.ds(pl.multiple_of(i * cl, cl), cl)

    def local(src, dst, i):
        c = pltpu.make_async_copy(src, dst, loc_sem.at[i])
        c.start()
        return c

    def remote(src, dst, i, dev):
        return pltpu.make_async_remote_copy(src_ref=src, dst_ref=dst, send_sem=snd_sem.at[i], recv_sem=rcv_sem.at[i],
                                            device_id=dev, device_id_type=MESH)

    ksplit = ((0, 7), (7, 13), (13, 19), (19, 25))
    c_x = [local(x_hbm.at[k0:k1], xg.at[k0:k1, blk(t), :], 7 + j) for j, (k0, k1) in enumerate(ksplit)]
    c_gain = local(gain_hbm, gain_in, 0)
    c_tog = local(tog_hbm, tog, 2)
    c_frg = local(frg_hbm, frg, 3)
    c_up = local(up_hbm, up, 4)
    c_gate = local(gate_hbm, gate, 5)
    c_down = local(down_hbm, down, 6)
    c_g = local(g_hbm, gg.at[:, blk(t), :], 1)

    barrier = pltpu.get_barrier_semaphore()
    for dev in ({"tp": t1}, {"tp": t2}, {"tp": t3}, {"dp": odp}):
        pl.semaphore_signal(barrier, inc=1, device_id=dev, device_id_type=MESH)
    pl.semaphore_wait(barrier, 4)

    def gather_start(dst, base, ready=None):
        far = []
        for j, (k0, k1) in enumerate(ksplit):
            if ready:
                ready[j].wait()
            c = remote(dst.at[k0:k1, blk(t), :], dst.at[k0:k1, blk(t), :], base + j, {"tp": t2})
            c.start()
            far.append(c)
        near = remote(dst.at[:, blk(t), :], dst.at[:, blk(t), :], base + 4, {"tp": t1})
        near.start()
        return far, near

    def gather_finish(far, near, dst, base):
        fwd = []
        for j, (k0, k1) in enumerate(ksplit):
            far[j].wait_recv()
            c = remote(dst.at[k0:k1, blk(t2), :], dst.at[k0:k1, blk(t2), :], base + 5 + j, {"tp": t1})
            c.start()
            fwd.append(c)
        near.wait_recv()
        for c in fwd:
            c.wait_recv()
        return fwd

    far_x, near_x = gather_start(xg, 0, c_x)

    gain_snd[...] = jnp.zeros_like(gain_snd)
    c_gain.wait()
    gain_snd[0:5, 0:cl] = gain_in[...]
    placed = pltpu.roll(gain_snd[...], t * cl, 1)
    gain_snd[...] = placed
    gsend = []
    for j, dev in enumerate((t1, t2, t3)):
        c = remote(gain_snd, gain_all.at[j], 20 + j, {"tp": dev})
        c.start()
        gsend.append(c)

    c_tog.wait()
    c_frg.wait()
    tpad = jnp.zeros((KPAD, 384), F32)
    tmat[...] = tpad.astype(BF16)
    ft[...] = tpad.astype(BF16)
    tmat[0:COEFS, 0:grid_pts] = tog[...].astype(BF16)
    frg_pad = jnp.concatenate([jnp.zeros((1, grid_pts), F32), frg[...]], axis=0)
    ft[0:COEFS, 0:grid_pts] = frg_pad.astype(BF16)
    for src, dst in ((tmat, tt), (ft, fmat)):
        wide = jnp.concatenate([src[...].astype(F32) * 0.5, jnp.zeros((128 - KPAD, 384), F32)], axis=0)
        for j in range(3):
            tr = wide[:, 128 * j:128 * (j + 1)].T
            rows = min(128, pp - 128 * j)
            dst[128 * j:128 * j + rows, :] = tr[0:rows, 0:KPAD].astype(BF16)
    c_up.wait()
    c_gate.wait()
    c_down.wait()
    for l in range(5):
        upt[l] = up[l].astype(F32).T.astype(BF16)
        downt[l] = down[l].astype(F32).T.astype(BF16)
    gatet[...] = gate[...].astype(F32).T.astype(BF16)
    ya[...] = jnp.zeros_like(ya)
    yb[...] = jnp.zeros_like(yb)
    for c in gsend:
        c.wait_recv()
    gain_full = placed + gain_all[0] + gain_all[1] + gain_all[2]
    for l in range(5):
        gcol[l] = jnp.broadcast_to(gain_full[l:l + 1, :], (ch, ch)).T

    fwd_x = gather_finish(far_x, near_x, xg, 0)
    for c in far_x:
        c.wait_send()
    c_g.wait()
    far_g, near_g = gather_start(gg, 10)

    x0 = xg[0].astype(F32)
    mean_s = jnp.sum(x0, axis=0, keepdims=True) / ch
    cent = x0 - mean_s
    inv_s = lax.rsqrt(jnp.sum(cent * cent, axis=0, keepdims=True) / ch + NORM_EPS)
    hat_s = cent * inv_s
    acc = jnp.zeros((ch, nat), F32)
    for k in range(1, COEFS):
        v = xg[k].astype(F32)
        acc = acc + v * v
    inv_v = lax.rsqrt(jnp.sum(acc, axis=0, keepdims=True) / (ch * (COEFS - 1)) + NORM_EPS)
    xn[0] = (hat_s * gcol[0]).astype(BF16)
    for k in range(1, COEFS):
        xn[k] = (xg[k].astype(F32) * inv_v * gcol[degree_of(k)]).astype(BF16)

    def spread(get, lhs_of):
        for l in range(5):
            k0, k1 = l * l, (l + 1) * (l + 1)
            lhs = lhs_of(l)
            for k in range(k0, k1):
                r = rows_dot(lhs, get(k))
                ya[pl.ds(k, 64, stride=YSTRIDE), :] = r[0:64]
                yb[pl.ds(k, 64, stride=YSTRIDE), :] = r[64:128]

    spread(lambda k: xn[k], lambda l: upt[l])
    a_r = rows_dot(gatet[...], xn[0]).astype(BF16)
    amat[...] = a_r
    a_h = a_r.astype(F32) * 0.5
    mb[0] = (a_h * (1.0 + jnp.tanh(a_h))).astype(BF16)

    def pair(i):
        base = pl.multiple_of(i * YSTRIDE, 8)
        return jnp.concatenate([ya[pl.ds(base, KPAD), :], yb[pl.ds(base, KPAD), :]], axis=1).astype(BF16)

    def put(i, r):
        zs[pl.ds(i, KPAD, stride=136), :] = r[:, 0:128]
        zs[pl.ds(i + 64, KPAD, stride=136), :] = r[:, 128:256]

    def stage_u(p, dst):
        dst[...] = rows_dot(tt[...], pair(p)).astype(BF16)

    def stage_s(p, src, dst):
        hb = src[...]
        hs[pl.ds(pl.multiple_of(p * pp, 16), pp), :] = hb
        h = hb.astype(F32)
        dst[...] = (h * (1.0 + jnp.tanh(h))).astype(BF16)

    def stage_z(p, src, lhs):
        put(p, rows_dot(lhs[:, 0:pp], src[...]))

    stage_u(0, gbuf[0])

    def fwd_body(it, carry):
        for j in range(UNROLL):
            p = it * UNROLL + j
            stage_z(jnp.maximum(p - 1, 0), sbuf[(j + 1) % 2], ft)
            stage_u(p + 1, gbuf[(j + 1) % 2])
            stage_s(p, gbuf[j % 2], sbuf[j % 2])
        return carry

    lax.fori_loop(0, 64 // UNROLL, fwd_body, 0)
    stage_z(63, sbuf[1], ft)

    for k in range(1, COEFS):
        mb[k] = zs[k * 136:k * 136 + 128, :].astype(BF16)
    for k in range(COEFS):
        dpart[k] = rows_dot(downt[degree_of(k)], mb[k]).astype(BF16)

    def scatter_near(part, rb, base):
        cs = []
        for j, b in enumerate((t3, t1)):
            c = remote(part.at[:, blk(b), :], rb.at[j], base + j, {"tp": t1})
            c.start()
            cs.append(c)
        return cs

    near_d = scatter_near(dpart, rb1, 23)

    fwd_g = gather_finish(far_g, near_g, gg, 10)
    spread(lambda k: gg[k], lambda l: down[l])
    dm0 = rows_dot(down[0], gg[0]).astype(BF16).astype(F32)
    a_h = amat[...].astype(F32) * 0.5
    w_a = 1.0 + jnp.tanh(a_h)
    da = (dm0 * (0.5 * w_a * (1.0 + a_h * (2.0 - w_a)))).astype(BF16)

    near_d[0].wait_recv()
    sb[...] = (dpart[:, blk(t2), :].astype(F32) + rb1[0].astype(F32)).astype(BF16)
    for l in range(5):
        acc = jnp.zeros((128, ch), F32)
        for k in range(l * l, (l + 1) * (l + 1)):
            acc = acc + lanes_dot(mb[k], gg[k])
        gdn[l] = acc
    gdn[5] = lanes_dot(da, xn[0])
    far_d = remote(sb, rb2, 25, {"tp": t2})
    far_d.start()
    half = 64
    mine = pl.ds(pl.multiple_of(dp * half, half), half)
    theirs = pl.ds(pl.multiple_of(odp * half, half), half)
    ex_dn = remote(gdn.at[:, theirs, :], gdn_rb, 26, {"dp": odp})
    ex_dn.start()

    def stage_g(p, dst):
        dst[...] = rows_dot(fmat[...], pair(p)).astype(BF16)

    def stage_e(p, src, dst):
        dg = src[...].astype(F32)
        h = hs[pl.ds(pl.multiple_of(p * pp, 16), pp), :].astype(F32)
        w = 1.0 + jnp.tanh(h)
        dst[...] = (dg * (w * (1.0 + h * (2.0 - w)))).astype(BF16)

    stage_g(0, gbuf[0])

    def bwd_body(it, carry):
        for j in range(UNROLL):
            p = it * UNROLL + j
            stage_z(jnp.maximum(p - 1, 0), sbuf[(j + 1) % 2], tmat)
            stage_g(p + 1, gbuf[(j + 1) % 2])
            stage_e(p, gbuf[j % 2], sbuf[j % 2])
        return carry

    def grad_up(k_rows, lo):
        for l in range(5):
            acc = jnp.zeros((2 * QR, ch), F32)
            for k in range(l * l, (l + 1) * (l + 1)):
                dy = jnp.concatenate([zs[k * 136 + lo:k * 136 + lo + QR, :].astype(BF16),
                                      zs[k * 136 + 64 + lo:k * 136 + 64 + lo + QR, :].astype(BF16)], axis=0)
                dyb[k, lo:lo + QR, :] = dy[0:QR]
                dyb[k, 64 + lo:64 + lo + QR, :] = dy[QR:2 * QR]
                acc = acc + lanes_dot(dy, xn[k])
            gup[l, lo:lo + QR, :] = acc[0:QR]
            gup[l, 64 + lo:64 + lo + QR, :] = acc[QR:2 * QR]

    def rows_of(d, lo):
        return pl.ds(pl.multiple_of(d * half + lo, QR), QR)

    mid_steps = (QR + 2) // UNROLL
    lax.fori_loop(0, mid_steps, bwd_body, 0)

    grad_up(None, 0)
    ex_up0 = remote(gup.at[:, rows_of(odp, 0), :], gup_rb.at[:, 0:QR, :], 33, {"dp": odp})
    ex_up0.start()
    ex_dn.wait_recv()
    gfin_dn[:, mine, :] = (gdn[:, mine, :] + gdn_rb[...]).astype(BF16)
    near_d[1].wait_recv()
    far_d.wait_recv()
    own = dpart[:, blk(t), :].astype(F32) + rb1[1].astype(F32) + rb2[...].astype(F32)
    out_ref[...] = (xg[:, blk(t), :].astype(F32) + own).astype(BF16)
    bk_dn = remote(gfin_dn.at[:, mine, :], gfin_dn.at[:, mine, :], 34, {"dp": odp})
    bk_dn.start()

    lax.fori_loop(mid_steps, 64 // UNROLL, bwd_body, 0)
    stage_z(63, sbuf[1], tmat)

    for k in range(COEFS):
        for o in (QR, 64 + QR):
            dyb[k, o:o + QR, :] = zs[k * 136 + o:k * 136 + o + QR, :].astype(BF16)
    nsplit = ((0, 9), (9, 16), (16, 25))
    near_n = []
    s3 = jnp.zeros((ch, nat), F32)
    for j, (k0, k1) in enumerate(nsplit):
        for k in range(k0, k1):
            r = rows_dot(up[degree_of(k)], dyb[k])
            if k == 0:
                r = r + rows_dot(gate[...], da)
            npart[k] = r.astype(BF16)
        c = remote(npart.at[k0:k1, blk(t3), :], nrb1.at[0, k0:k1], 27 + j, {"tp": t1})
        c.start()
        near_n.append(c)
    near_o = remote(npart.at[:, blk(t1), :], nrb1.at[1], 30, {"tp": t1})
    near_o.start()
    ex_up0.wait_recv()
    gfin[:, rows_of(dp, 0), :] = (gup[:, rows_of(dp, 0), :] + gup_rb[:, 0:QR, :]).astype(BF16)
    for k in range(COEFS):
        rf = npart[k].astype(F32) * gcol[degree_of(k)]
        if k == 0:
            st0 = jnp.sum(rf, axis=0, keepdims=True)
            st1 = jnp.sum(rf * hat_s, axis=0, keepdims=True)
        else:
            s3 = s3 + rf * xg[k].astype(F32)
    st2 = jnp.sum(s3, axis=0, keepdims=True)
    st_snd[...] = jnp.concatenate([st0, st1, st2, jnp.zeros((5, nat), F32)], axis=0)
    bk_up0 = remote(gfin.at[:, rows_of(dp, 0), :], gfin.at[:, rows_of(dp, 0), :], 35, {"dp": odp})
    bk_up0.start()

    far_n = []

    def far_step(j):
        k0, k1 = nsplit[j]
        near_n[j].wait_recv()
        nsb[k0:k1] = (npart[k0:k1, blk(t2), :].astype(F32) + nrb1[0, k0:k1].astype(F32)).astype(BF16)

    def far_send(j):
        k0, k1 = nsplit[j]
        c = remote(nsb.at[k0:k1], nrb2.at[k0:k1], 41 + j, {"tp": t2})
        c.start()
        far_n.append(c)

    far_step(0)
    grad_up(None, QR)
    far_send(0)
    ex_up1 = remote(gup.at[:, rows_of(odp, QR), :], gup_rb.at[:, QR:2 * QR, :], 36, {"dp": odp})
    ex_up1.start()
    far_step(1)
    far_step(2)
    far_send(1)
    far_send(2)
    ssend = []
    for j, dev in enumerate((t1, t2, t3)):
        c = remote(st_snd, st_all.at[j], 37 + j, {"tp": dev})
        c.start()
        ssend.append(c)

    bk_dn.wait_recv()
    ddown_ref[...] = gfin_dn[0:5]
    dgate_ref[...] = gfin_dn[5].astype(F32).T.astype(BF16)
    ex_up1.wait_recv()
    gfin[:, rows_of(dp, QR), :] = (gup[:, rows_of(dp, QR), :] + gup_rb[:, QR:2 * QR, :]).astype(BF16)
    for c in ssend:
        c.wait_recv()
    stat = st_snd[...] + st_all[0] + st_all[1] + st_all[2]
    b0 = stat[0:1] / ch
    b1 = stat[1:2] / ch
    b2 = (inv_v * inv_v * inv_v) * (stat[2:3] / (ch * (COEFS - 1)))
    bk_up1 = remote(gfin.at[:, rows_of(dp, QR), :], gfin.at[:, rows_of(dp, QR), :], 40, {"dp": odp})
    bk_up1.start()
    near_o.wait_recv()
    for j, (k0, k1) in enumerate(nsplit):
        far_n[j].wait_recv()
        for k in range(k0, k1):
            dn = (npart[k, blk(t), :].astype(F32) + nrb1[1, k].astype(F32) + nrb2[k].astype(F32)).astype(BF16).astype(F32)
            dhat = dn * gcol[degree_of(k), blk(t), :]
            xk = xg[k, blk(t), :].astype(F32)
            if k == 0:
                dxk = inv_s * (dhat - b0 - (xk - mean_s) * inv_s * b1)
            else:
                dxk = inv_v * dhat - xk * b2
            dx_ref[k] = (dxk + gg[k, blk(t), :].astype(F32)).astype(BF16)

    bk_up0.wait_recv()
    bk_up1.wait_recv()
    for l in range(5):
        dup_ref[l] = gfin[l].astype(F32).T.astype(BF16)
    for c in far_g + fwd_x + fwd_g + gsend + near_d + near_n + far_n + ssend + [near_x, near_g, near_o, far_d, ex_dn, ex_up0, ex_up1, bk_dn, bk_up0, bk_up1]:
        c.wait_send()


def flush(a, b, c, d, e, oa, ob, oc, od, oe, sem):
    cs = [pltpu.make_async_copy(i, o, sem.at[j]) for j, (i, o) in enumerate(zip((a, b, c, d, e), (oa, ob, oc, od, oe)))]
    for x in cs:
        x.start()
    for x in cs:
        x.wait()


def solution(mesh):
    tp_size = mesh.shape['tp']
    act_spec = P('dp', None, 'tp')
    in_specs = (act_spec, P(None, 'tp'), P(None, None, 'tp'), P(None, 'tp'), P(None, 'tp', None), P(None, None), P(None, None), act_spec)
    out_specs = (act_spec, act_spec, P(None, None, 'tp'), P(None, 'tp'), P(None, 'tp', None))

    def local_step(x_loc, gain_loc, up_loc, gate_loc, down_loc, to_grid, from_grid, grad_loc):
        nat, coefs, cl = x_loc.shape
        ch = cl * tp_size
        grid_pts = to_grid.shape[1]
        pp = -(-grid_pts // 16) * 16
        xt = x_loc.transpose(1, 2, 0)
        gt = grad_loc.transpose(1, 2, 0)
        any_spec = pl.BlockSpec(memory_space=pl.ANY)
        vmem = pl.BlockSpec(memory_space=pltpu.VMEM)
        full = pltpu.VMEM((coefs, ch, nat), BF16)
        blkb = pltpu.VMEM((coefs, cl, nat), BF16)
        sq = lambda n, d: pltpu.VMEM((n, 128, 128), d)
        shapes = (xt.shape, xt.shape, up_loc.shape, gate_loc.shape, down_loc.shape)
        outs = pl.pallas_call(
            functools.partial(kernel, tp_size, grid_pts),
            out_shape=tuple(pltpu.VMEM(sh, BF16) for sh in shapes),
            in_specs=[any_spec] * 8,
            out_specs=[vmem] * 5,
            scratch_shapes=[
                full, full, full, full, full, full, full,
                pltpu.VMEM((65 * YSTRIDE, 128), F32), pltpu.VMEM((65 * YSTRIDE, 128), F32),
                pltpu.VMEM((KPAD * 136, 128), F32), pltpu.VMEM((65 * pp, 256), BF16),
                pltpu.VMEM(gain_loc.shape, F32), pltpu.VMEM((8, 128), F32), pltpu.VMEM((3, 8, 128), F32), sq(5, F32),
                sq(5, BF16), pltpu.VMEM((128, 128), BF16), sq(5, BF16), sq(5, BF16), pltpu.VMEM((128, 128), BF16), sq(5, BF16),
                pltpu.VMEM(to_grid.shape, F32), pltpu.VMEM(from_grid.shape[::-1], F32),
                pltpu.VMEM((pp, KPAD), BF16), pltpu.VMEM((KPAD, 384), BF16), pltpu.VMEM((pp, KPAD), BF16), pltpu.VMEM((KPAD, 384), BF16),
                pltpu.VMEM((2, coefs, cl, nat), BF16), blkb, blkb, pltpu.VMEM((2, coefs, cl, nat), BF16), blkb, blkb,
                pltpu.VMEM((8, 128), F32), pltpu.VMEM((3, 8, 128), F32),
                sq(6, F32), pltpu.VMEM((6, 64, 128), F32), sq(5, F32), pltpu.VMEM((5, 64, 128), F32), sq(5, BF16), sq(6, BF16),
                pltpu.VMEM((128, nat), BF16),
                pltpu.VMEM((pp, 256), BF16), pltpu.VMEM((pp, 256), BF16), pltpu.VMEM((pp, 256), BF16), pltpu.VMEM((pp, 256), BF16),
                pltpu.SemaphoreType.DMA((12,)), pltpu.SemaphoreType.DMA((44,)), pltpu.SemaphoreType.DMA((44,)),
            ],
            compiler_params=pltpu.CompilerParams(collective_id=0, has_side_effects=True, vmem_limit_bytes=60 * 1024 * 1024),
        )(xt, gain_loc, up_loc, gate_loc, down_loc, to_grid, from_grid.T, gt)
        out_t, dx_t, d_up, d_gate, d_down = pl.pallas_call(
            flush,
            out_shape=tuple(jax.ShapeDtypeStruct(sh, BF16) for sh in shapes),
            in_specs=[vmem] * 5,
            out_specs=[any_spec] * 5,
            scratch_shapes=[pltpu.SemaphoreType.DMA((5,))],
        )(*[pltpu.with_memory_space_constraint(o, pltpu.VMEM) for o in outs])
        return out_t.transpose(2, 0, 1), dx_t.transpose(2, 0, 1), d_up, d_gate, d_down

    return jax.shard_map(local_step, mesh=mesh, in_specs=in_specs, out_specs=out_specs, check_vma=False)
```

```python
import functools
import math
import jax
import jax.numpy as jnp
from jax import lax
from jax.experimental import pallas as pl
from jax.experimental.pallas import tpu as pltpu
from jax.sharding import PartitionSpec as P

NORM_EPS = 1e-5
MESH = pl.DeviceIdType.MESH
F32 = jnp.float32
BF16 = jnp.bfloat16
COEFS = 25
KPAD = 32
YSTRIDE = 40
UNROLL = 2
QR = 32


def degree_of(k):
    return math.isqrt(k)


def rows_dot(a, b):
    return lax.dot_general(a, b, (((1,), (0,)), ((), ())), preferred_element_type=F32)


def lanes_dot(a, b):
    return lax.dot_general(a, b, (((1,), (1,)), ((), ())), preferred_element_type=F32)


def kernel(tp_size, grid_pts, x_hbm, gain_hbm, up_hbm, gate_hbm, down_hbm, tog_hbm, frg_hbm, g_hbm,
           out_ref, dx_ref, dup_ref, dgate_ref, ddown_ref,
           xg, gg, xn, mb, dyb, dpart, npart, ya, yb, zs, hs,
           gain_in, gain_snd, gain_all, gcol, up, gate, down, upt, gatet, downt,
           tog, frg, tt, tmat, fmat, ft, rb1, sb, rb2, nrb1, nsb, nrb2,
           st_snd, st_all, gdn, gdn_rb, gup, gup_rb, gfin, gfin_dn, amat, sbuf0, sbuf1, gbuf0, gbuf1,
           loc_sem, snd_sem, rcv_sem):
    sbuf, gbuf = (sbuf0, sbuf1), (gbuf0, gbuf1)
    dp = lax.axis_index("dp")
    t = lax.axis_index("tp")
    core = lax.rem(t, 2)
    t1 = t + 1 - 2 * core
    t2 = lax.rem(t + 2, 4)
    t3 = lax.rem(t1 + 2, 4)
    odp = 1 - dp
    cl = xg.shape[1] // tp_size
    ch = xg.shape[1]
    nat = xg.shape[2]
    pp = tt.shape[0]

    def blk(i):
        return pl.ds(pl.multiple_of(i * cl, cl), cl)

    def local(src, dst, i):
        c = pltpu.make_async_copy(src, dst, loc_sem.at[i])
        c.start()
        return c

    def remote(src, dst, i, dev):
        return pltpu.make_async_remote_copy(src_ref=src, dst_ref=dst, send_sem=snd_sem.at[i], recv_sem=rcv_sem.at[i],
                                            device_id=dev, device_id_type=MESH)

    ksplit = ((0, 7), (7, 13), (13, 19), (19, 25))
    c_x = [local(x_hbm.at[k0:k1], xg.at[k0:k1, blk(t), :], 7 + j) for j, (k0, k1) in enumerate(ksplit)]
    c_gain = local(gain_hbm, gain_in, 0)
    c_tog = local(tog_hbm, tog, 2)
    c_frg = local(frg_hbm, frg, 3)
    c_up = local(up_hbm, up, 4)
    c_gate = local(gate_hbm, gate, 5)
    c_down = local(down_hbm, down, 6)
    c_g = local(g_hbm, gg.at[:, blk(t), :], 1)

    barrier = pltpu.get_barrier_semaphore()
    for dev in ({"tp": t1}, {"tp": t2}, {"tp": t3}, {"dp": odp}):
        pl.semaphore_signal(barrier, inc=1, device_id=dev, device_id_type=MESH)
    pl.semaphore_wait(barrier, 4)

    def gather_start(dst, base, ready=None):
        far = []
        for j, (k0, k1) in enumerate(ksplit):
            if ready:
                ready[j].wait()
            c = remote(dst.at[k0:k1, blk(t), :], dst.at[k0:k1, blk(t), :], base + j, {"tp": t2})
            c.start()
            far.append(c)
        near = remote(dst.at[:, blk(t), :], dst.at[:, blk(t), :], base + 4, {"tp": t1})
        near.start()
        return far, near

    def gather_finish(far, near, dst, base):
        fwd = []
        for j, (k0, k1) in enumerate(ksplit):
            far[j].wait_recv()
            c = remote(dst.at[k0:k1, blk(t2), :], dst.at[k0:k1, blk(t2), :], base + 5 + j, {"tp": t1})
            c.start()
            fwd.append(c)
        near.wait_recv()
        for c in fwd:
            c.wait_recv()
        return fwd

    far_x, near_x = gather_start(xg, 0, c_x)

    gain_snd[...] = jnp.zeros_like(gain_snd)
    c_gain.wait()
    gain_snd[0:5, 0:cl] = gain_in[...]
    placed = pltpu.roll(gain_snd[...], t * cl, 1)
    gain_snd[...] = placed
    gsend = []
    for j, dev in enumerate((t1, t2, t3)):
        c = remote(gain_snd, gain_all.at[j], 20 + j, {"tp": dev})
        c.start()
        gsend.append(c)

    c_tog.wait()
    c_frg.wait()
    tpad = jnp.zeros((KPAD, 384), F32)
    tmat[...] = tpad.astype(BF16)
    ft[...] = tpad.astype(BF16)
    tmat[0:COEFS, 0:grid_pts] = tog[...].astype(BF16)
    frg_pad = jnp.concatenate([jnp.zeros((1, grid_pts), F32), frg[...]], axis=0)
    ft[0:COEFS, 0:grid_pts] = frg_pad.astype(BF16)
    for src, dst in ((tmat, tt), (ft, fmat)):
        wide = jnp.concatenate([src[...].astype(F32) * 0.5, jnp.zeros((128 - KPAD, 384), F32)], axis=0)
        for j in range(3):
            tr = wide[:, 128 * j:128 * (j + 1)].T
            rows = min(128, pp - 128 * j)
            dst[128 * j:128 * j + rows, :] = tr[0:rows, 0:KPAD].astype(BF16)
    c_up.wait()
    c_gate.wait()
    c_down.wait()
    for l in range(5):
        upt[l] = up[l].astype(F32).T.astype(BF16)
        downt[l] = down[l].astype(F32).T.astype(BF16)
    gatet[...] = gate[...].astype(F32).T.astype(BF16)
    ya[...] = jnp.zeros_like(ya)
    yb[...] = jnp.zeros_like(yb)
    for c in gsend:
        c.wait_recv()
    gain_full = placed + gain_all[0] + gain_all[1] + gain_all[2]
    for l in range(5):
        gcol[l] = jnp.broadcast_to(gain_full[l:l + 1, :], (ch, ch)).T

    fwd_x = gather_finish(far_x, near_x, xg, 0)
    for c in far_x:
        c.wait_send()
    c_g.wait()
    far_g, near_g = gather_start(gg, 10)

    x0 = xg[0].astype(F32)
    mean_s = jnp.sum(x0, axis=0, keepdims=True) / ch
    cent = x0 - mean_s
    inv_s = lax.rsqrt(jnp.sum(cent * cent, axis=0, keepdims=True) / ch + NORM_EPS)
    hat_s = cent * inv_s
    acc = jnp.zeros((ch, nat), F32)
    for k in range(1, COEFS):
        v = xg[k].astype(F32)
        acc = acc + v * v
    inv_v = lax.rsqrt(jnp.sum(acc, axis=0, keepdims=True) / (ch * (COEFS - 1)) + NORM_EPS)
    xn[0] = (hat_s * gcol[0]).astype(BF16)
    for k in range(1, COEFS):
        xn[k] = (xg[k].astype(F32) * inv_v * gcol[degree_of(k)]).astype(BF16)

    def by_degree(lhs_of, get, lo=0, hi=COEFS):
        for l in range(5):
            k = max(l * l, lo)
            k1 = min((l + 1) * (l + 1), hi)
            while k < k1:
                n = min(2, k1 - k)
                r = rows_dot(lhs_of(l), get(k) if n == 1 else jnp.concatenate([get(k), get(k + 1)], axis=1))
                for j in range(n):
                    yield k + j, r[:, nat * j:nat * (j + 1)]
                k += n

    def over_degree(a_of, b_of, l):
        ks = range(l * l, (l + 1) * (l + 1))
        return lanes_dot(jnp.concatenate([a_of(k) for k in ks], axis=1), jnp.concatenate([b_of(k) for k in ks], axis=1))

    def spread(get, lhs_of):
        for k, r in by_degree(lhs_of, get):
            ya[pl.ds(k, 64, stride=YSTRIDE), :] = r[0:64]
            yb[pl.ds(k, 64, stride=YSTRIDE), :] = r[64:128]

    spread(lambda k: xn[k], lambda l: upt[l])
    a_r = rows_dot(gatet[...], xn[0]).astype(BF16)
    amat[...] = a_r
    a_h = a_r.astype(F32) * 0.5
    mb[0] = (a_h * (1.0 + jnp.tanh(a_h))).astype(BF16)

    def pair(i):
        base = pl.multiple_of(i * YSTRIDE, 8)
        return jnp.concatenate([ya[pl.ds(base, KPAD), :], yb[pl.ds(base, KPAD), :]], axis=1).astype(BF16)

    def put(i, r):
        zs[pl.ds(i, KPAD, stride=136), :] = r[:, 0:128]
        zs[pl.ds(i + 64, KPAD, stride=136), :] = r[:, 128:256]

    def stage_u(p, dst):
        dst[...] = rows_dot(tt[...], pair(p)).astype(BF16)

    def stage_s(p, src, dst):
        h = src[...].astype(F32)
        w = 1.0 + jnp.tanh(h)
        s = h * w
        dst[...] = s.astype(BF16)
        hs[pl.ds(pl.multiple_of(p * pp, 16), pp), :] = w + s * (2.0 - w)

    def stage_z(p, src, lhs):
        put(p, rows_dot(lhs[:, 0:pp], src[...]))

    stage_u(0, gbuf[0])

    def fwd_body(it, carry):
        for j in range(UNROLL):
            p = it * UNROLL + j
            stage_z(jnp.maximum(p - 1, 0), sbuf[(j + 1) % 2], ft)
            stage_u(p + 1, gbuf[(j + 1) % 2])
            stage_s(p, gbuf[j % 2], sbuf[j % 2])
        return carry

    lax.fori_loop(0, 64 // UNROLL, fwd_body, 0)
    stage_z(63, sbuf[1], ft)

    for k in range(1, COEFS):
        mb[k] = zs[k * 136:k * 136 + 128, :].astype(BF16)
    for k, r in by_degree(lambda l: downt[l], lambda k: mb[k]):
        dpart[k] = r.astype(BF16)

    def scatter_near(part, rb, base):
        cs = []
        for j, b in enumerate((t3, t1)):
            c = remote(part.at[:, blk(b), :], rb.at[j], base + j, {"tp": t1})
            c.start()
            cs.append(c)
        return cs

    near_d = scatter_near(dpart, rb1, 23)

    fwd_g = gather_finish(far_g, near_g, gg, 10)
    spread(lambda k: gg[k], lambda l: down[l])
    dm0 = rows_dot(down[0], gg[0]).astype(BF16).astype(F32)
    a_h = amat[...].astype(F32) * 0.5
    w_a = 1.0 + jnp.tanh(a_h)
    da = (dm0 * (0.5 * w_a * (1.0 + a_h * (2.0 - w_a)))).astype(BF16)

    for l in range(5):
        gdn[l] = over_degree(lambda k: mb[k], lambda k: gg[k], l)
    gdn[5] = lanes_dot(da, xn[0])
    near_d[0].wait_recv()
    sb[...] = (dpart[:, blk(t2), :].astype(F32) + rb1[0].astype(F32)).astype(BF16)
    half = 64
    mine = pl.ds(pl.multiple_of(dp * half, half), half)
    theirs = pl.ds(pl.multiple_of(odp * half, half), half)
    ex_dn = remote(gdn.at[:, theirs, :], gdn_rb, 26, {"dp": odp})
    ex_dn.start()
    far_d = remote(sb, rb2, 25, {"tp": t2})
    far_d.start()

    def stage_g(p, dst):
        dst[...] = rows_dot(fmat[...], pair(p)).astype(BF16)

    def stage_e(p, src, dst):
        gp = hs[pl.ds(pl.multiple_of(p * pp, 16), pp), :]
        dst[...] = (src[...].astype(F32) * gp).astype(BF16)

    stage_g(0, gbuf[0])

    def bwd_body(it, carry):
        for j in range(UNROLL):
            p = it * UNROLL + j
            stage_z(jnp.maximum(p - 1, 0), sbuf[(j + 1) % 2], tmat)
            stage_g(p + 1, gbuf[(j + 1) % 2])
            stage_e(p, gbuf[j % 2], sbuf[j % 2])
        return carry

    def grad_up(lo):
        def dy(k):
            return jnp.concatenate([dyb[k, lo:lo + QR, :], dyb[k, 64 + lo:64 + lo + QR, :]], axis=0)

        for k in range(COEFS):
            for o in (lo, 64 + lo):
                dyb[k, o:o + QR, :] = zs[k * 136 + o:k * 136 + o + QR, :].astype(BF16)
        for l in range(5):
            acc = over_degree(dy, lambda k: xn[k], l)
            gup[l, lo:lo + QR, :] = acc[0:QR]
            gup[l, 64 + lo:64 + lo + QR, :] = acc[QR:2 * QR]

    def rows_of(d, lo):
        return pl.ds(pl.multiple_of(d * half + lo, QR), QR)

    mid_steps = (QR + 2) // UNROLL
    late_steps = 52 // UNROLL
    lax.fori_loop(0, mid_steps, bwd_body, 0)

    grad_up(0)
    ex_up0 = remote(gup.at[:, rows_of(odp, 0), :], gup_rb.at[:, 0:QR, :], 33, {"dp": odp})
    ex_up0.start()

    lax.fori_loop(mid_steps, late_steps, bwd_body, 0)

    ex_dn.wait_recv()
    gfin_dn[:, mine, :] = (gdn[:, mine, :] + gdn_rb[...]).astype(BF16)
    near_d[1].wait_recv()
    far_d.wait_recv()
    own = dpart[:, blk(t), :].astype(F32) + rb1[1].astype(F32) + rb2[...].astype(F32)
    out_ref[...] = (xg[:, blk(t), :].astype(F32) + own).astype(BF16)
    bk_dn = remote(gfin_dn.at[:, mine, :], gfin_dn.at[:, mine, :], 34, {"dp": odp})
    bk_dn.start()

    lax.fori_loop(late_steps, 64 // UNROLL, bwd_body, 0)
    stage_z(63, sbuf[1], tmat)

    def full_dy(k):
        return jnp.concatenate([dyb[k, 0:QR, :], zs[k * 136 + QR:k * 136 + 64, :].astype(BF16),
                                dyb[k, 64:64 + QR, :], zs[k * 136 + 64 + QR:k * 136 + 128, :].astype(BF16)], axis=0)

    nsplit = ((0, 9), (9, 16), (16, 25))
    near_n = []
    for j, (k0, k1) in enumerate(nsplit):
        for k, r in by_degree(lambda l: up[l], full_dy, k0, k1):
            if k == 0:
                r = r + rows_dot(gate[...], da)
            npart[k] = r.astype(BF16)
        c = remote(npart.at[k0:k1, blk(t3), :], nrb1.at[0, k0:k1], 27 + j, {"tp": t1})
        c.start()
        near_n.append(c)
    grad_up(QR)
    near_o = remote(npart.at[:, blk(t1), :], nrb1.at[1], 30, {"tp": t1})
    near_o.start()

    far_n = []

    def far_step(j):
        k0, k1 = nsplit[j]
        near_n[j].wait_recv()
        nsb[k0:k1] = (npart[k0:k1, blk(t2), :].astype(F32) + nrb1[0, k0:k1].astype(F32)).astype(BF16)

    def far_send(j):
        k0, k1 = nsplit[j]
        c = remote(nsb.at[k0:k1], nrb2.at[k0:k1], 41 + j, {"tp": t2})
        c.start()
        far_n.append(c)

    far_step(0)
    ex_up1 = remote(gup.at[:, rows_of(odp, QR), :], gup_rb.at[:, QR:2 * QR, :], 36, {"dp": odp})
    ex_up1.start()
    far_step(1)
    far_send(0)
    far_step(2)
    far_send(1)
    ex_up0.wait_recv()
    gfin[:, rows_of(dp, 0), :] = (gup[:, rows_of(dp, 0), :] + gup_rb[:, 0:QR, :]).astype(BF16)
    far_send(2)

    s3 = jnp.zeros((ch, nat), F32)
    for k in range(COEFS):
        rf = npart[k].astype(F32) * gcol[degree_of(k)]
        if k == 0:
            st0 = jnp.sum(rf, axis=0, keepdims=True)
            st1 = jnp.sum(rf * hat_s, axis=0, keepdims=True)
        else:
            s3 = s3 + rf * xg[k].astype(F32)
    st2 = jnp.sum(s3, axis=0, keepdims=True)
    st_snd[...] = jnp.concatenate([st0, st1, st2, jnp.zeros((5, nat), F32)], axis=0)
    bk_up0 = remote(gfin.at[:, rows_of(dp, 0), :], gfin.at[:, rows_of(dp, 0), :], 35, {"dp": odp})
    bk_up0.start()
    ssend = []
    for j, dev in enumerate((t1, t2, t3)):
        c = remote(st_snd, st_all.at[j], 37 + j, {"tp": dev})
        c.start()
        ssend.append(c)

    bk_dn.wait_recv()
    ddown_ref[...] = gfin_dn[0:5]
    dgate_ref[...] = gfin_dn[5].astype(F32).T.astype(BF16)
    ex_up1.wait_recv()
    gfin[:, rows_of(dp, QR), :] = (gup[:, rows_of(dp, QR), :] + gup_rb[:, QR:2 * QR, :]).astype(BF16)
    for c in ssend:
        c.wait_recv()
    stat = st_snd[...] + st_all[0] + st_all[1] + st_all[2]
    b0 = stat[0:1] / ch
    b1 = stat[1:2] / ch
    b2 = (inv_v * inv_v * inv_v) * (stat[2:3] / (ch * (COEFS - 1)))
    bk_up1 = remote(gfin.at[:, rows_of(dp, QR), :], gfin.at[:, rows_of(dp, QR), :], 40, {"dp": odp})
    bk_up1.start()
    near_o.wait_recv()
    for j, (k0, k1) in enumerate(nsplit):
        far_n[j].wait_recv()
        for k in range(k0, k1):
            dn = (npart[k, blk(t), :].astype(F32) + nrb1[1, k].astype(F32) + nrb2[k].astype(F32)).astype(BF16).astype(F32)
            dhat = dn * gcol[degree_of(k), blk(t), :]
            xk = xg[k, blk(t), :].astype(F32)
            if k == 0:
                dxk = inv_s * (dhat - b0 - (xk - mean_s) * inv_s * b1)
            else:
                dxk = inv_v * dhat - xk * b2
            dx_ref[k] = (dxk + gg[k, blk(t), :].astype(F32)).astype(BF16)

    bk_up0.wait_recv()
    bk_up1.wait_recv()
    for l in range(5):
        dup_ref[l] = gfin[l].astype(F32).T.astype(BF16)
    for c in far_g + fwd_x + fwd_g + gsend + near_d + near_n + far_n + ssend + [near_x, near_g, near_o, far_d, ex_dn, ex_up0, ex_up1, bk_dn, bk_up0, bk_up1]:
        c.wait_send()


def flush(a, b, c, d, e, oa, ob, oc, od, oe, sem):
    cs = [pltpu.make_async_copy(i, o, sem.at[j]) for j, (i, o) in enumerate(zip((a, b, c, d, e), (oa, ob, oc, od, oe)))]
    for x in cs:
        x.start()
    for x in cs:
        x.wait()


def solution(mesh):
    tp_size = mesh.shape['tp']
    act_spec = P('dp', None, 'tp')
    in_specs = (act_spec, P(None, 'tp'), P(None, None, 'tp'), P(None, 'tp'), P(None, 'tp', None), P(None, None), P(None, None), act_spec)
    out_specs = (act_spec, act_spec, P(None, None, 'tp'), P(None, 'tp'), P(None, 'tp', None))

    def local_step(x_loc, gain_loc, up_loc, gate_loc, down_loc, to_grid, from_grid, grad_loc):
        nat, coefs, cl = x_loc.shape
        ch = cl * tp_size
        grid_pts = to_grid.shape[1]
        pp = -(-grid_pts // 16) * 16
        xt = x_loc.transpose(1, 2, 0)
        gt = grad_loc.transpose(1, 2, 0)
        any_spec = pl.BlockSpec(memory_space=pl.ANY)
        vmem = pl.BlockSpec(memory_space=pltpu.VMEM)
        full = pltpu.VMEM((coefs, ch, nat), BF16)
        blkb = pltpu.VMEM((coefs, cl, nat), BF16)
        sq = lambda n, d: pltpu.VMEM((n, 128, 128), d)
        shapes = (xt.shape, xt.shape, up_loc.shape, gate_loc.shape, down_loc.shape)
        outs = pl.pallas_call(
            functools.partial(kernel, tp_size, grid_pts),
            out_shape=tuple(pltpu.VMEM(sh, BF16) for sh in shapes),
            in_specs=[any_spec] * 8,
            out_specs=[vmem] * 5,
            scratch_shapes=[
                full, full, full, full, full, full, full,
                pltpu.VMEM((65 * YSTRIDE, 128), F32), pltpu.VMEM((65 * YSTRIDE, 128), F32),
                pltpu.VMEM((KPAD * 136, 128), F32), pltpu.VMEM((64 * pp, 256), F32),
                pltpu.VMEM(gain_loc.shape, F32), pltpu.VMEM((8, 128), F32), pltpu.VMEM((3, 8, 128), F32), sq(5, F32),
                sq(5, BF16), pltpu.VMEM((128, 128), BF16), sq(5, BF16), sq(5, BF16), pltpu.VMEM((128, 128), BF16), sq(5, BF16),
                pltpu.VMEM(to_grid.shape, F32), pltpu.VMEM(from_grid.shape[::-1], F32),
                pltpu.VMEM((pp, KPAD), BF16), pltpu.VMEM((KPAD, 384), BF16), pltpu.VMEM((pp, KPAD), BF16), pltpu.VMEM((KPAD, 384), BF16),
                pltpu.VMEM((2, coefs, cl, nat), BF16), blkb, blkb, pltpu.VMEM((2, coefs, cl, nat), BF16), blkb, blkb,
                pltpu.VMEM((8, 128), F32), pltpu.VMEM((3, 8, 128), F32),
                sq(6, F32), pltpu.VMEM((6, 64, 128), F32), sq(5, F32), pltpu.VMEM((5, 64, 128), F32), sq(5, BF16), sq(6, BF16),
                pltpu.VMEM((128, nat), BF16),
                pltpu.VMEM((pp, 256), BF16), pltpu.VMEM((pp, 256), BF16), pltpu.VMEM((pp, 256), BF16), pltpu.VMEM((pp, 256), BF16),
                pltpu.SemaphoreType.DMA((12,)), pltpu.SemaphoreType.DMA((44,)), pltpu.SemaphoreType.DMA((44,)),
            ],
            compiler_params=pltpu.CompilerParams(collective_id=0, has_side_effects=True, vmem_limit_bytes=60 * 1024 * 1024),
        )(xt, gain_loc, up_loc, gate_loc, down_loc, to_grid, from_grid.T, gt)
        out_t, dx_t, d_up, d_gate, d_down = pl.pallas_call(
            flush,
            out_shape=tuple(jax.ShapeDtypeStruct(sh, BF16) for sh in shapes),
            in_specs=[vmem] * 5,
            out_specs=[any_spec] * 5,
            scratch_shapes=[pltpu.SemaphoreType.DMA((5,))],
        )(*[pltpu.with_memory_space_constraint(o, pltpu.VMEM) for o in outs])
        return out_t.transpose(2, 0, 1), dx_t.transpose(2, 0, 1), d_up, d_gate, d_down

    return jax.shard_map(local_step, mesh=mesh, in_specs=in_specs, out_specs=out_specs, check_vma=False)
```

```python
import functools
import math
import jax
import jax.numpy as jnp
from jax import lax
from jax.experimental import pallas as pl
from jax.experimental.pallas import tpu as pltpu
from jax.sharding import PartitionSpec as P

NORM_EPS = 1e-5
MESH = pl.DeviceIdType.MESH
F32 = jnp.float32
BF16 = jnp.bfloat16
COEFS = 25
KPAD = 32
YSTRIDE = 40
UNROLL = 2
QR = 32


def degree_of(k):
    return math.isqrt(k)


def rows_dot(a, b):
    return lax.dot_general(a, b, (((1,), (0,)), ((), ())), preferred_element_type=F32)


def lanes_dot(a, b):
    return lax.dot_general(a, b, (((1,), (1,)), ((), ())), preferred_element_type=F32)


def kernel(tp_size, grid_pts, x_hbm, gain_hbm, up_hbm, gate_hbm, down_hbm, tog_hbm, frg_hbm, g_hbm,
           out_ref, dx_ref, dup_ref, dgate_ref, ddown_ref,
           xg, gg, xn, mb, dyb, dpart, npart, ya, yb, zs, hs,
           gain_in, gain_snd, gain_all, gcol, up, gate, down, upt, gatet, downt,
           tog, frg, tt, tmat, fmat, ft, rb1, sb, rb2, nrb1, nsb, nrb2,
           st_snd, st_all, gdn, gdn_rb, gup, gup_rb, gfin, gfin_dn, amat, sbuf0, sbuf1, gbuf0, gbuf1,
           loc_sem, snd_sem, rcv_sem):
    sbuf, gbuf = (sbuf0, sbuf1), (gbuf0, gbuf1)
    dp = lax.axis_index("dp")
    t = lax.axis_index("tp")
    core = lax.rem(t, 2)
    t1 = t + 1 - 2 * core
    t2 = lax.rem(t + 2, 4)
    t3 = lax.rem(t1 + 2, 4)
    odp = 1 - dp
    cl = xg.shape[1] // tp_size
    ch = xg.shape[1]
    nat = xg.shape[2]
    pp = tt.shape[0]

    def blk(i):
        return pl.ds(pl.multiple_of(i * cl, cl), cl)

    def local(src, dst, i):
        c = pltpu.make_async_copy(src, dst, loc_sem.at[i])
        c.start()
        return c

    def remote(src, dst, i, dev):
        return pltpu.make_async_remote_copy(src_ref=src, dst_ref=dst, send_sem=snd_sem.at[i], recv_sem=rcv_sem.at[i],
                                            device_id=dev, device_id_type=MESH)

    c_gain = local(gain_hbm, gain_in, 0)
    ksplit = ((0, 7), (7, 13), (13, 19), (19, 25))
    c_x = [local(x_hbm.at[k0:k1], xg.at[k0:k1, blk(t), :], 7 + j) for j, (k0, k1) in enumerate(ksplit)]
    c_tog = local(tog_hbm, tog, 2)
    c_frg = local(frg_hbm, frg, 3)
    c_up = local(up_hbm, up, 4)
    c_gate = local(gate_hbm, gate, 5)
    c_down = local(down_hbm, down, 6)
    c_g = local(g_hbm, gg.at[:, blk(t), :], 1)

    barrier = pltpu.get_barrier_semaphore()
    for dev in ({"tp": t1}, {"tp": t2}, {"tp": t3}, {"dp": odp}):
        pl.semaphore_signal(barrier, inc=1, device_id=dev, device_id_type=MESH)
    c_gain.wait()
    gain_snd[...] = jnp.zeros_like(gain_snd)
    gain_snd[0:5, 0:cl] = gain_in[...]
    placed = pltpu.roll(gain_snd[...], t * cl, 1)
    gain_snd[...] = placed
    pl.semaphore_wait(barrier, 4)
    gsend = []
    for j, dev in enumerate((t1, t2, t3)):
        c = remote(gain_snd, gain_all.at[j], 20 + j, {"tp": dev})
        c.start()
        gsend.append(c)

    def gather_start(dst, base, ready=None):
        far = []
        for j, (k0, k1) in enumerate(ksplit):
            if ready:
                ready[j].wait()
            c = remote(dst.at[k0:k1, blk(t), :], dst.at[k0:k1, blk(t), :], base + j, {"tp": t2})
            c.start()
            far.append(c)
        near = remote(dst.at[:, blk(t), :], dst.at[:, blk(t), :], base + 4, {"tp": t1})
        near.start()
        return far, near

    def gather_finish(far, near, dst, base):
        fwd = []
        for j, (k0, k1) in enumerate(ksplit):
            far[j].wait_recv()
            c = remote(dst.at[k0:k1, blk(t2), :], dst.at[k0:k1, blk(t2), :], base + 5 + j, {"tp": t1})
            c.start()
            fwd.append(c)
        return fwd

    def gather_wait(near, fwd):
        near.wait_recv()
        for c in fwd:
            c.wait_recv()

    far_x, near_x = gather_start(xg, 0, c_x)

    c_tog.wait()
    c_frg.wait()
    tpad = jnp.zeros((KPAD, 384), F32)
    tmat[...] = tpad.astype(BF16)
    ft[...] = tpad.astype(BF16)
    tmat[0:COEFS, 0:grid_pts] = tog[...].astype(BF16)
    frg_pad = jnp.concatenate([jnp.zeros((1, grid_pts), F32), frg[...]], axis=0)
    ft[0:COEFS, 0:grid_pts] = frg_pad.astype(BF16)
    for src, dst in ((tmat, tt), (ft, fmat)):
        wide = jnp.concatenate([src[...].astype(F32) * 0.5, jnp.zeros((128 - KPAD, 384), F32)], axis=0)
        for j in range(3):
            tr = wide[:, 128 * j:128 * (j + 1)].T
            rows = min(128, pp - 128 * j)
            dst[128 * j:128 * j + rows, :] = tr[0:rows, 0:KPAD].astype(BF16)
    c_up.wait()
    c_gate.wait()
    c_down.wait()
    for l in range(5):
        upt[l] = up[l].astype(F32).T.astype(BF16)
        downt[l] = down[l].astype(F32).T.astype(BF16)
    gatet[...] = gate[...].astype(F32).T.astype(BF16)
    ya[...] = jnp.zeros_like(ya)
    yb[...] = jnp.zeros_like(yb)
    for c in gsend:
        c.wait_recv()
    gain_full = placed + gain_all[0] + gain_all[1] + gain_all[2]
    for l in range(5):
        gcol[l] = jnp.broadcast_to(gain_full[l:l + 1, :], (ch, ch)).T

    fwd_x = gather_finish(far_x, near_x, xg, 0)
    gather_wait(near_x, fwd_x)
    for c in far_x:
        c.wait_send()
    c_g.wait()
    far_g, near_g = gather_start(gg, 10)

    x0 = xg[0].astype(F32)
    mean_s = jnp.sum(x0, axis=0, keepdims=True) / ch
    cent = x0 - mean_s
    inv_s = lax.rsqrt(jnp.sum(cent * cent, axis=0, keepdims=True) / ch + NORM_EPS)
    hat_s = cent * inv_s
    acc = jnp.zeros((ch, nat), F32)
    for k in range(1, COEFS):
        v = xg[k].astype(F32)
        acc = acc + v * v
    inv_v = lax.rsqrt(jnp.sum(acc, axis=0, keepdims=True) / (ch * (COEFS - 1)) + NORM_EPS)
    xn[0] = (hat_s * gcol[0]).astype(BF16)
    for k in range(1, COEFS):
        xn[k] = (xg[k].astype(F32) * inv_v * gcol[degree_of(k)]).astype(BF16)

    def by_degree(lhs_of, get, lo=0, hi=COEFS):
        for l in range(5):
            k = max(l * l, lo)
            k1 = min((l + 1) * (l + 1), hi)
            while k < k1:
                n = min(2, k1 - k)
                r = rows_dot(lhs_of(l), get(k) if n == 1 else jnp.concatenate([get(k), get(k + 1)], axis=1))
                for j in range(n):
                    yield k + j, r[:, nat * j:nat * (j + 1)]
                k += n

    def over_degree(a_of, b_of, l):
        ks = range(l * l, (l + 1) * (l + 1))
        return lanes_dot(jnp.concatenate([a_of(k) for k in ks], axis=1), jnp.concatenate([b_of(k) for k in ks], axis=1))

    def spread(get, lhs_of):
        for k, r in by_degree(lhs_of, get):
            ya[pl.ds(k, 64, stride=YSTRIDE), :] = r[0:64]
            yb[pl.ds(k, 64, stride=YSTRIDE), :] = r[64:128]

    spread(lambda k: xn[k], lambda l: upt[l])
    a_r = rows_dot(gatet[...], xn[0]).astype(BF16)
    amat[...] = a_r
    a_h = a_r.astype(F32) * 0.5
    mb[0] = (a_h * (1.0 + jnp.tanh(a_h))).astype(BF16)

    def pair(i):
        base = pl.multiple_of(i * YSTRIDE, 8)
        return jnp.concatenate([ya[pl.ds(base, KPAD), :], yb[pl.ds(base, KPAD), :]], axis=1).astype(BF16)

    def put(i, r):
        zs[pl.ds(i, KPAD, stride=136), :] = r[:, 0:128]
        zs[pl.ds(i + 64, KPAD, stride=136), :] = r[:, 128:256]

    def stage_u(p, dst):
        dst[...] = rows_dot(tt[...], pair(p)).astype(BF16)

    def stage_s(p, src, dst):
        h = src[...].astype(F32)
        w = 1.0 + jnp.tanh(h)
        s = h * w
        dst[...] = s.astype(BF16)
        hs[pl.ds(pl.multiple_of(p * pp, 16), pp), :] = w + s * (2.0 - w)

    def stage_z(p, src, lhs):
        put(p, rows_dot(lhs[:, 0:pp], src[...]))

    stage_u(0, gbuf[0])

    def fwd_body(it, carry):
        for j in range(UNROLL):
            p = it * UNROLL + j
            stage_z(jnp.maximum(p - 1, 0), sbuf[(j + 1) % 2], ft)
            stage_u(p + 1, gbuf[(j + 1) % 2])
            stage_s(p, gbuf[j % 2], sbuf[j % 2])
        return carry

    lax.fori_loop(0, 50 // UNROLL, fwd_body, 0)
    fwd_g = gather_finish(far_g, near_g, gg, 10)
    lax.fori_loop(50 // UNROLL, 64 // UNROLL, fwd_body, 0)
    stage_z(63, sbuf[1], ft)

    for k in range(1, COEFS):
        mb[k] = zs[k * 136:k * 136 + 128, :].astype(BF16)
    for k, r in by_degree(lambda l: downt[l], lambda k: mb[k]):
        dpart[k] = r.astype(BF16)

    def scatter_near(part, rb, base):
        cs = []
        for j, b in enumerate((t3, t1)):
            c = remote(part.at[:, blk(b), :], rb.at[j], base + j, {"tp": t1})
            c.start()
            cs.append(c)
        return cs

    near_d = scatter_near(dpart, rb1, 23)

    gather_wait(near_g, fwd_g)
    spread(lambda k: gg[k], lambda l: down[l])
    dm0 = rows_dot(down[0], gg[0]).astype(BF16).astype(F32)
    a_h = amat[...].astype(F32) * 0.5
    w_a = 1.0 + jnp.tanh(a_h)
    da = (dm0 * (0.5 * w_a * (1.0 + a_h * (2.0 - w_a)))).astype(BF16)

    for l in range(5):
        gdn[l] = over_degree(lambda k: mb[k], lambda k: gg[k], l)
    gdn[5] = lanes_dot(da, xn[0])
    half = 64
    mine = pl.ds(pl.multiple_of(dp * half, half), half)
    theirs = pl.ds(pl.multiple_of(odp * half, half), half)
    ex_dn = remote(gdn.at[:, theirs, :], gdn_rb, 26, {"dp": odp})
    ex_dn.start()

    def stage_g(p, dst):
        dst[...] = rows_dot(fmat[...], pair(p)).astype(BF16)

    def stage_e(p, src, dst):
        gp = hs[pl.ds(pl.multiple_of(p * pp, 16), pp), :]
        dst[...] = (src[...].astype(F32) * gp).astype(BF16)

    stage_g(0, gbuf[0])

    def bwd_body(it, carry):
        for j in range(UNROLL):
            p = it * UNROLL + j
            stage_z(jnp.maximum(p - 1, 0), sbuf[(j + 1) % 2], tmat)
            stage_g(p + 1, gbuf[(j + 1) % 2])
            stage_e(p, gbuf[j % 2], sbuf[j % 2])
        return carry

    def grad_up(lo):
        def dy(k):
            return jnp.concatenate([dyb[k, lo:lo + QR, :], dyb[k, 64 + lo:64 + lo + QR, :]], axis=0)

        for k in range(COEFS):
            for o in (lo, 64 + lo):
                dyb[k, o:o + QR, :] = zs[k * 136 + o:k * 136 + o + QR, :].astype(BF16)
        for l in range(5):
            acc = over_degree(dy, lambda k: xn[k], l)
            gup[l, lo:lo + QR, :] = acc[0:QR]
            gup[l, 64 + lo:64 + lo + QR, :] = acc[QR:2 * QR]

    def rows_of(d, lo):
        return pl.ds(pl.multiple_of(d * half + lo, QR), QR)

    mid_steps = (QR + 2) // UNROLL
    late_steps = 56 // UNROLL
    lax.fori_loop(0, 6 // UNROLL, bwd_body, 0)
    near_d[0].wait_recv()
    sb[...] = (dpart[:, blk(t2), :].astype(F32) + rb1[0].astype(F32)).astype(BF16)
    far_d = remote(sb, rb2, 25, {"tp": t2})
    far_d.start()
    lax.fori_loop(6 // UNROLL, mid_steps, bwd_body, 0)

    grad_up(0)
    ex_up0 = remote(gup.at[:, rows_of(odp, 0), :], gup_rb.at[:, 0:QR, :], 33, {"dp": odp})
    ex_up0.start()

    lax.fori_loop(mid_steps, late_steps, bwd_body, 0)

    ex_dn.wait_recv()
    gfin_dn[:, mine, :] = (gdn[:, mine, :] + gdn_rb[...]).astype(BF16)
    near_d[1].wait_recv()
    far_d.wait_recv()
    own = dpart[:, blk(t), :].astype(F32) + rb1[1].astype(F32) + rb2[...].astype(F32)
    out_ref[...] = (xg[:, blk(t), :].astype(F32) + own).astype(BF16)
    bk_dn = remote(gfin_dn.at[:, mine, :], gfin_dn.at[:, mine, :], 34, {"dp": odp})
    bk_dn.start()

    lax.fori_loop(late_steps, 64 // UNROLL, bwd_body, 0)
    stage_z(63, sbuf[1], tmat)

    def full_dy(k):
        return jnp.concatenate([dyb[k, 0:QR, :], zs[k * 136 + QR:k * 136 + 64, :].astype(BF16),
                                dyb[k, 64:64 + QR, :], zs[k * 136 + 64 + QR:k * 136 + 128, :].astype(BF16)], axis=0)

    nsplit = ((0, 9), (9, 16), (16, 25))
    near_n = []
    for j, (k0, k1) in enumerate(nsplit):
        for k, r in by_degree(lambda l: up[l], full_dy, k0, k1):
            if k == 0:
                r = r + rows_dot(gate[...], da)
            npart[k] = r.astype(BF16)
        c = remote(npart.at[k0:k1, blk(t3), :], nrb1.at[0, k0:k1], 27 + j, {"tp": t1})
        c.start()
        near_n.append(c)
    grad_up(QR)
    near_o = remote(npart.at[:, blk(t1), :], nrb1.at[1], 30, {"tp": t1})
    near_o.start()

    far_n = []

    def far_step(j):
        k0, k1 = nsplit[j]
        near_n[j].wait_recv()
        nsb[k0:k1] = (npart[k0:k1, blk(t2), :].astype(F32) + nrb1[0, k0:k1].astype(F32)).astype(BF16)

    def far_send(j):
        k0, k1 = nsplit[j]
        c = remote(nsb.at[k0:k1], nrb2.at[k0:k1], 41 + j, {"tp": t2})
        c.start()
        far_n.append(c)

    far_step(0)
    ex_up1 = remote(gup.at[:, rows_of(odp, QR), :], gup_rb.at[:, QR:2 * QR, :], 36, {"dp": odp})
    ex_up1.start()
    far_step(1)
    far_send(0)
    far_step(2)
    far_send(1)
    ex_up0.wait_recv()
    gfin[:, rows_of(dp, 0), :] = (gup[:, rows_of(dp, 0), :] + gup_rb[:, 0:QR, :]).astype(BF16)
    far_send(2)

    s3 = jnp.zeros((ch, nat), F32)
    for k in range(COEFS):
        rf = npart[k].astype(F32) * gcol[degree_of(k)]
        if k == 0:
            st0 = jnp.sum(rf, axis=0, keepdims=True)
            st1 = jnp.sum(rf * hat_s, axis=0, keepdims=True)
        else:
            s3 = s3 + rf * xg[k].astype(F32)
    st2 = jnp.sum(s3, axis=0, keepdims=True)
    st_snd[...] = jnp.concatenate([st0, st1, st2, jnp.zeros((5, nat), F32)], axis=0)
    bk_up0 = remote(gfin.at[:, rows_of(dp, 0), :], gfin.at[:, rows_of(dp, 0), :], 35, {"dp": odp})
    bk_up0.start()
    ssend = []
    for j, dev in enumerate((t1, t2, t3)):
        c = remote(st_snd, st_all.at[j], 37 + j, {"tp": dev})
        c.start()
        ssend.append(c)

    bk_dn.wait_recv()
    ddown_ref[...] = gfin_dn[0:5]
    dgate_ref[...] = gfin_dn[5].astype(F32).T.astype(BF16)
    ex_up1.wait_recv()
    gfin[:, rows_of(dp, QR), :] = (gup[:, rows_of(dp, QR), :] + gup_rb[:, QR:2 * QR, :]).astype(BF16)
    for c in ssend:
        c.wait_recv()
    stat = st_snd[...] + st_all[0] + st_all[1] + st_all[2]
    b0 = stat[0:1] / ch
    b1 = stat[1:2] / ch
    b2 = (inv_v * inv_v * inv_v) * (stat[2:3] / (ch * (COEFS - 1)))
    bk_up1 = remote(gfin.at[:, rows_of(dp, QR), :], gfin.at[:, rows_of(dp, QR), :], 40, {"dp": odp})
    bk_up1.start()
    near_o.wait_recv()
    for j, (k0, k1) in enumerate(nsplit):
        far_n[j].wait_recv()
        for k in range(k0, k1):
            dn = (npart[k, blk(t), :].astype(F32) + nrb1[1, k].astype(F32) + nrb2[k].astype(F32)).astype(BF16).astype(F32)
            dhat = dn * gcol[degree_of(k), blk(t), :]
            xk = xg[k, blk(t), :].astype(F32)
            if k == 0:
                dxk = inv_s * (dhat - b0 - (xk - mean_s) * inv_s * b1)
            else:
                dxk = inv_v * dhat - xk * b2
            dx_ref[k] = (dxk + gg[k, blk(t), :].astype(F32)).astype(BF16)

    bk_up0.wait_recv()
    bk_up1.wait_recv()
    for l in range(5):
        dup_ref[l] = gfin[l].astype(F32).T.astype(BF16)
    for c in far_g + fwd_x + fwd_g + gsend + near_d + near_n + far_n + ssend + [near_x, near_g, near_o, far_d, ex_dn, ex_up0, ex_up1, bk_dn, bk_up0, bk_up1]:
        c.wait_send()


def flush(a, b, c, d, e, oa, ob, oc, od, oe, sem):
    cs = [pltpu.make_async_copy(i, o, sem.at[j]) for j, (i, o) in enumerate(zip((a, b, c, d, e), (oa, ob, oc, od, oe)))]
    for x in cs:
        x.start()
    for x in cs:
        x.wait()


def solution(mesh):
    tp_size = mesh.shape['tp']
    act_spec = P('dp', None, 'tp')
    in_specs = (act_spec, P(None, 'tp'), P(None, None, 'tp'), P(None, 'tp'), P(None, 'tp', None), P(None, None), P(None, None), act_spec)
    out_specs = (act_spec, act_spec, P(None, None, 'tp'), P(None, 'tp'), P(None, 'tp', None))

    def local_step(x_loc, gain_loc, up_loc, gate_loc, down_loc, to_grid, from_grid, grad_loc):
        nat, coefs, cl = x_loc.shape
        ch = cl * tp_size
        grid_pts = to_grid.shape[1]
        pp = -(-grid_pts // 16) * 16
        xt = x_loc.transpose(1, 2, 0)
        gt = grad_loc.transpose(1, 2, 0)
        any_spec = pl.BlockSpec(memory_space=pl.ANY)
        vmem = pl.BlockSpec(memory_space=pltpu.VMEM)
        full = pltpu.VMEM((coefs, ch, nat), BF16)
        blkb = pltpu.VMEM((coefs, cl, nat), BF16)
        sq = lambda n, d: pltpu.VMEM((n, 128, 128), d)
        shapes = (xt.shape, xt.shape, up_loc.shape, gate_loc.shape, down_loc.shape)
        outs = pl.pallas_call(
            functools.partial(kernel, tp_size, grid_pts),
            out_shape=tuple(pltpu.VMEM(sh, BF16) for sh in shapes),
            in_specs=[any_spec] * 8,
            out_specs=[vmem] * 5,
            scratch_shapes=[
                full, full, full, full, full, full, full,
                pltpu.VMEM((65 * YSTRIDE, 128), F32), pltpu.VMEM((65 * YSTRIDE, 128), F32),
                pltpu.VMEM((KPAD * 136, 128), F32), pltpu.VMEM((64 * pp, 256), F32),
                pltpu.VMEM(gain_loc.shape, F32), pltpu.VMEM((8, 128), F32), pltpu.VMEM((3, 8, 128), F32), sq(5, F32),
                sq(5, BF16), pltpu.VMEM((128, 128), BF16), sq(5, BF16), sq(5, BF16), pltpu.VMEM((128, 128), BF16), sq(5, BF16),
                pltpu.VMEM(to_grid.shape, F32), pltpu.VMEM(from_grid.shape[::-1], F32),
                pltpu.VMEM((pp, KPAD), BF16), pltpu.VMEM((KPAD, 384), BF16), pltpu.VMEM((pp, KPAD), BF16), pltpu.VMEM((KPAD, 384), BF16),
                pltpu.VMEM((2, coefs, cl, nat), BF16), blkb, blkb, pltpu.VMEM((2, coefs, cl, nat), BF16), blkb, blkb,
                pltpu.VMEM((8, 128), F32), pltpu.VMEM((3, 8, 128), F32),
                sq(6, F32), pltpu.VMEM((6, 64, 128), F32), sq(5, F32), pltpu.VMEM((5, 64, 128), F32), sq(5, BF16), sq(6, BF16),
                pltpu.VMEM((128, nat), BF16),
                pltpu.VMEM((pp, 256), BF16), pltpu.VMEM((pp, 256), BF16), pltpu.VMEM((pp, 256), BF16), pltpu.VMEM((pp, 256), BF16),
                pltpu.SemaphoreType.DMA((12,)), pltpu.SemaphoreType.DMA((44,)), pltpu.SemaphoreType.DMA((44,)),
            ],
            compiler_params=pltpu.CompilerParams(collective_id=0, has_side_effects=True, vmem_limit_bytes=60 * 1024 * 1024),
        )(xt, gain_loc, up_loc, gate_loc, down_loc, to_grid, from_grid.T, gt)
        out_t, dx_t, d_up, d_gate, d_down = pl.pallas_call(
            flush,
            out_shape=tuple(jax.ShapeDtypeStruct(sh, BF16) for sh in shapes),
            in_specs=[vmem] * 5,
            out_specs=[any_spec] * 5,
            scratch_shapes=[pltpu.SemaphoreType.DMA((5,))],
        )(*[pltpu.with_memory_space_constraint(o, pltpu.VMEM) for o in outs])
        return out_t.transpose(2, 0, 1), dx_t.transpose(2, 0, 1), d_up, d_gate, d_down

    return jax.shard_map(local_step, mesh=mesh, in_specs=in_specs, out_specs=out_specs, check_vma=False)
```

```python
import functools
import math
import jax
import jax.numpy as jnp
from jax import lax
from jax.experimental import pallas as pl
from jax.experimental.pallas import tpu as pltpu
from jax.sharding import PartitionSpec as P

NORM_EPS = 1e-5
MESH = pl.DeviceIdType.MESH
F32 = jnp.float32
BF16 = jnp.bfloat16
COEFS = 25
KPAD = 32
YSTRIDE = 40
UNROLL = 4
QR = 32


def degree_of(k):
    return math.isqrt(k)


def rows_dot(a, b):
    return lax.dot_general(a, b, (((1,), (0,)), ((), ())), preferred_element_type=F32)


def lanes_dot(a, b):
    return lax.dot_general(a, b, (((1,), (1,)), ((), ())), preferred_element_type=F32)


def kernel(tp_size, grid_pts, x_hbm, gain_hbm, up_hbm, gate_hbm, down_hbm, tog_hbm, frg_hbm, g_hbm,
           out_ref, dx_ref, dup_ref, dgate_ref, ddown_ref,
           xg, gg, xn, mb, dyb, dpart, npart, ya, yb, zs, hs,
           gain_in, gain_snd, gain_all, gcol, up, gate, down, upt, gatet, downt,
           tog, frg, tt, tmat, fmat, ft, rb1, sb, rb2, nrb1, nsb, nrb2,
           st_snd, st_all, gdn, gdn_rb, gup, gup_rb, gfin, gfin_dn, amat, sbuf0, sbuf1, sbuf2, sbuf3, gbuf0, gbuf1, gbuf2, gbuf3,
           loc_sem, snd_sem, rcv_sem):
    sbuf, gbuf = (sbuf0, sbuf1, sbuf2, sbuf3), (gbuf0, gbuf1, gbuf2, gbuf3)
    dp = lax.axis_index("dp")
    t = lax.axis_index("tp")
    core = lax.rem(t, 2)
    t1 = t + 1 - 2 * core
    t2 = lax.rem(t + 2, 4)
    t3 = lax.rem(t1 + 2, 4)
    odp = 1 - dp
    cl = xg.shape[1] // tp_size
    ch = xg.shape[1]
    nat = xg.shape[2]
    pp = tt.shape[0]

    def blk(i):
        return pl.ds(pl.multiple_of(i * cl, cl), cl)

    def local(src, dst, i):
        c = pltpu.make_async_copy(src, dst, loc_sem.at[i])
        c.start()
        return c

    def remote(src, dst, i, dev):
        return pltpu.make_async_remote_copy(src_ref=src, dst_ref=dst, send_sem=snd_sem.at[i], recv_sem=rcv_sem.at[i],
                                            device_id=dev, device_id_type=MESH)

    c_gain = local(gain_hbm, gain_in, 0)
    ksplit = ((0, 7), (7, 13), (13, 19), (19, 25))
    c_x = [local(x_hbm.at[k0:k1], xg.at[k0:k1, blk(t), :], 7 + j) for j, (k0, k1) in enumerate(ksplit)]
    c_tog = local(tog_hbm, tog, 2)
    c_frg = local(frg_hbm, frg, 3)
    c_up = local(up_hbm, up, 4)
    c_gate = local(gate_hbm, gate, 5)
    c_down = local(down_hbm, down, 6)
    c_g = local(g_hbm, gg.at[:, blk(t), :], 1)

    barrier = pltpu.get_barrier_semaphore()
    for dev in ({"tp": t1}, {"tp": t2}, {"tp": t3}, {"dp": odp}):
        pl.semaphore_signal(barrier, inc=1, device_id=dev, device_id_type=MESH)
    c_gain.wait()
    gain_snd[...] = jnp.zeros_like(gain_snd)
    gain_snd[0:5, 0:cl] = gain_in[...]
    placed = pltpu.roll(gain_snd[...], t * cl, 1)
    gain_snd[...] = placed
    pl.semaphore_wait(barrier, 4)
    gsend = []
    for j, dev in enumerate((t1, t2, t3)):
        c = remote(gain_snd, gain_all.at[j], 20 + j, {"tp": dev})
        c.start()
        gsend.append(c)

    def gather_start(dst, base, ready=None):
        far = []
        for j, (k0, k1) in enumerate(ksplit):
            if ready:
                ready[j].wait()
            c = remote(dst.at[k0:k1, blk(t), :], dst.at[k0:k1, blk(t), :], base + j, {"tp": t2})
            c.start()
            far.append(c)
        near = remote(dst.at[:, blk(t), :], dst.at[:, blk(t), :], base + 4, {"tp": t1})
        near.start()
        return far, near

    def gather_finish(far, near, dst, base):
        fwd = []
        for j, (k0, k1) in enumerate(ksplit):
            far[j].wait_recv()
            c = remote(dst.at[k0:k1, blk(t2), :], dst.at[k0:k1, blk(t2), :], base + 5 + j, {"tp": t1})
            c.start()
            fwd.append(c)
        return fwd

    def gather_wait(near, fwd):
        near.wait_recv()
        for c in fwd:
            c.wait_recv()

    far_x, near_x = gather_start(xg, 0, c_x)

    c_tog.wait()
    c_frg.wait()
    tpad = jnp.zeros((KPAD, 384), F32)
    tmat[...] = tpad.astype(BF16)
    ft[...] = tpad.astype(BF16)
    tmat[0:COEFS, 0:grid_pts] = tog[...].astype(BF16)
    frg_pad = jnp.concatenate([jnp.zeros((1, grid_pts), F32), frg[...]], axis=0)
    ft[0:COEFS, 0:grid_pts] = frg_pad.astype(BF16)
    for src, dst in ((tmat, tt), (ft, fmat)):
        wide = jnp.concatenate([src[...].astype(F32) * 0.5, jnp.zeros((128 - KPAD, 384), F32)], axis=0)
        for j in range(3):
            tr = wide[:, 128 * j:128 * (j + 1)].T
            rows = min(128, pp - 128 * j)
            dst[128 * j:128 * j + rows, :] = tr[0:rows, 0:KPAD].astype(BF16)
    c_up.wait()
    c_gate.wait()
    c_down.wait()
    for l in range(5):
        upt[l] = up[l].astype(F32).T.astype(BF16)
        downt[l] = down[l].astype(F32).T.astype(BF16)
    gatet[...] = gate[...].astype(F32).T.astype(BF16)
    ya[...] = jnp.zeros_like(ya)
    yb[...] = jnp.zeros_like(yb)
    for c in gsend:
        c.wait_recv()
    gain_full = placed + gain_all[0] + gain_all[1] + gain_all[2]
    for l in range(5):
        gcol[l] = jnp.broadcast_to(gain_full[l:l + 1, :], (ch, ch)).T

    fwd_x = gather_finish(far_x, near_x, xg, 0)
    gather_wait(near_x, fwd_x)
    for c in far_x:
        c.wait_send()
    c_g.wait()
    far_g, near_g = gather_start(gg, 10)

    x0 = xg[0].astype(F32)
    mean_s = jnp.sum(x0, axis=0, keepdims=True) / ch
    cent = x0 - mean_s
    inv_s = lax.rsqrt(jnp.sum(cent * cent, axis=0, keepdims=True) / ch + NORM_EPS)
    hat_s = cent * inv_s
    acc = jnp.zeros((ch, nat), F32)
    for k in range(1, COEFS):
        v = xg[k].astype(F32)
        acc = acc + v * v
    inv_v = lax.rsqrt(jnp.sum(acc, axis=0, keepdims=True) / (ch * (COEFS - 1)) + NORM_EPS)
    xn[0] = (hat_s * gcol[0]).astype(BF16)
    for k in range(1, COEFS):
        xn[k] = (xg[k].astype(F32) * inv_v * gcol[degree_of(k)]).astype(BF16)

    def by_degree(lhs_of, get, lo=0, hi=COEFS):
        for l in range(5):
            k = max(l * l, lo)
            k1 = min((l + 1) * (l + 1), hi)
            while k < k1:
                n = min(2, k1 - k)
                r = rows_dot(lhs_of(l), get(k) if n == 1 else jnp.concatenate([get(k), get(k + 1)], axis=1))
                for j in range(n):
                    yield k + j, r[:, nat * j:nat * (j + 1)]
                k += n

    def over_degree(a_of, b_of, l):
        ks = range(l * l, (l + 1) * (l + 1))
        return lanes_dot(jnp.concatenate([a_of(k) for k in ks], axis=1), jnp.concatenate([b_of(k) for k in ks], axis=1))

    def spread(get, lhs_of):
        for k, r in by_degree(lhs_of, get):
            ya[pl.ds(k, 64, stride=YSTRIDE), :] = r[0:64]
            yb[pl.ds(k, 64, stride=YSTRIDE), :] = r[64:128]

    spread(lambda k: xn[k], lambda l: upt[l])
    a_r = rows_dot(gatet[...], xn[0]).astype(BF16)
    amat[...] = a_r
    a_h = a_r.astype(F32) * 0.5
    mb[0] = (a_h * (1.0 + jnp.tanh(a_h))).astype(BF16)

    def pair(i):
        base = pl.multiple_of(i * YSTRIDE, 8)
        return jnp.concatenate([ya[pl.ds(base, KPAD), :], yb[pl.ds(base, KPAD), :]], axis=1).astype(BF16)

    def put(i, r):
        zs[pl.ds(i, KPAD, stride=136), :] = r[:, 0:128]
        zs[pl.ds(i + 64, KPAD, stride=136), :] = r[:, 128:256]

    def stage_u(p, dst):
        dst[...] = rows_dot(tt[...], pair(p)).astype(BF16)

    def stage_s(p, src, dst):
        h = src[...].astype(F32)
        w = 1.0 + jnp.tanh(h)
        s = h * w
        dst[...] = s.astype(BF16)
        hs[pl.ds(pl.multiple_of(p * pp, 16), pp), :] = w + s * (2.0 - w)

    def stage_z(p, src, lhs):
        put(p, rows_dot(lhs[:, 0:pp], src[...]))

    stage_u(0, gbuf[0])
    stage_u(1, gbuf[1])

    def fwd_body(it, carry):
        for half_step in range(2):
            p = it * UNROLL + 2 * half_step
            now, other = 2 * (half_step % 2), 2 * ((half_step + 1) % 2)
            for j in range(2):
                stage_z(jnp.maximum(p + j - 2, 0), sbuf[other + j], ft)
                stage_u(p + j + 2, gbuf[other + j])
                stage_s(p + j, gbuf[now + j], sbuf[now + j])
        return carry

    lax.fori_loop(0, 48 // UNROLL, fwd_body, 0)
    fwd_g = gather_finish(far_g, near_g, gg, 10)
    lax.fori_loop(48 // UNROLL, 64 // UNROLL, fwd_body, 0)
    stage_z(62, sbuf[2], ft)
    stage_z(63, sbuf[3], ft)

    for k in range(1, COEFS):
        mb[k] = zs[k * 136:k * 136 + 128, :].astype(BF16)
    for k, r in by_degree(lambda l: downt[l], lambda k: mb[k]):
        dpart[k] = r.astype(BF16)

    def scatter_near(part, rb, base):
        cs = []
        for j, b in enumerate((t3, t1)):
            c = remote(part.at[:, blk(b), :], rb.at[j], base + j, {"tp": t1})
            c.start()
            cs.append(c)
        return cs

    near_d = scatter_near(dpart, rb1, 23)

    gather_wait(near_g, fwd_g)
    spread(lambda k: gg[k], lambda l: down[l])
    dm0 = rows_dot(down[0], gg[0]).astype(BF16).astype(F32)
    a_h = amat[...].astype(F32) * 0.5
    w_a = 1.0 + jnp.tanh(a_h)
    da = (dm0 * (0.5 * w_a * (1.0 + a_h * (2.0 - w_a)))).astype(BF16)

    for l in range(5):
        gdn[l] = over_degree(lambda k: mb[k], lambda k: gg[k], l)
    gdn[5] = lanes_dot(da, xn[0])
    half = 64
    mine = pl.ds(pl.multiple_of(dp * half, half), half)
    theirs = pl.ds(pl.multiple_of(odp * half, half), half)
    ex_dn = remote(gdn.at[:, theirs, :], gdn_rb, 26, {"dp": odp})
    ex_dn.start()

    def stage_g(p, dst):
        dst[...] = rows_dot(fmat[...], pair(p)).astype(BF16)

    def stage_e(p, src, dst):
        gp = hs[pl.ds(pl.multiple_of(p * pp, 16), pp), :]
        dst[...] = (src[...].astype(F32) * gp).astype(BF16)

    stage_g(0, gbuf[0])
    stage_g(1, gbuf[1])

    def bwd_body(it, carry):
        for half_step in range(2):
            p = it * UNROLL + 2 * half_step
            now, other = 2 * (half_step % 2), 2 * ((half_step + 1) % 2)
            for j in range(2):
                stage_z(jnp.maximum(p + j - 2, 0), sbuf[other + j], tmat)
                stage_g(p + j + 2, gbuf[other + j])
                stage_e(p + j, gbuf[now + j], sbuf[now + j])
        return carry

    def grad_up(lo):
        def dy(k):
            return jnp.concatenate([dyb[k, lo:lo + QR, :], dyb[k, 64 + lo:64 + lo + QR, :]], axis=0)

        for k in range(COEFS):
            for o in (lo, 64 + lo):
                dyb[k, o:o + QR, :] = zs[k * 136 + o:k * 136 + o + QR, :].astype(BF16)
        for l in range(5):
            acc = over_degree(dy, lambda k: xn[k], l)
            gup[l, lo:lo + QR, :] = acc[0:QR]
            gup[l, 64 + lo:64 + lo + QR, :] = acc[QR:2 * QR]

    def rows_of(d, lo):
        return pl.ds(pl.multiple_of(d * half + lo, QR), QR)

    mid_steps = (QR + 4) // UNROLL
    late_steps = 56 // UNROLL
    lax.fori_loop(0, 8 // UNROLL, bwd_body, 0)
    near_d[0].wait_recv()
    sb[...] = (dpart[:, blk(t2), :].astype(F32) + rb1[0].astype(F32)).astype(BF16)
    far_d = remote(sb, rb2, 25, {"tp": t2})
    far_d.start()
    lax.fori_loop(8 // UNROLL, mid_steps, bwd_body, 0)

    grad_up(0)
    ex_up0 = remote(gup.at[:, rows_of(odp, 0), :], gup_rb.at[:, 0:QR, :], 33, {"dp": odp})
    ex_up0.start()

    lax.fori_loop(mid_steps, late_steps, bwd_body, 0)

    ex_dn.wait_recv()
    gfin_dn[:, mine, :] = (gdn[:, mine, :] + gdn_rb[...]).astype(BF16)
    near_d[1].wait_recv()
    far_d.wait_recv()
    own = dpart[:, blk(t), :].astype(F32) + rb1[1].astype(F32) + rb2[...].astype(F32)
    out_ref[...] = (xg[:, blk(t), :].astype(F32) + own).astype(BF16)
    bk_dn = remote(gfin_dn.at[:, mine, :], gfin_dn.at[:, mine, :], 34, {"dp": odp})
    bk_dn.start()

    lax.fori_loop(late_steps, 64 // UNROLL, bwd_body, 0)
    stage_z(62, sbuf[2], tmat)
    stage_z(63, sbuf[3], tmat)

    def full_dy(k):
        return jnp.concatenate([dyb[k, 0:QR, :], zs[k * 136 + QR:k * 136 + 64, :].astype(BF16),
                                dyb[k, 64:64 + QR, :], zs[k * 136 + 64 + QR:k * 136 + 128, :].astype(BF16)], axis=0)

    nsplit = ((0, 9), (9, 16), (16, 25))
    near_n = []
    for j, (k0, k1) in enumerate(nsplit):
        for k, r in by_degree(lambda l: up[l], full_dy, k0, k1):
            if k == 0:
                r = r + rows_dot(gate[...], da)
            npart[k] = r.astype(BF16)
        c = remote(npart.at[k0:k1, blk(t3), :], nrb1.at[0, k0:k1], 27 + j, {"tp": t1})
        c.start()
        near_n.append(c)
    grad_up(QR)
    near_o = remote(npart.at[:, blk(t1), :], nrb1.at[1], 30, {"tp": t1})
    near_o.start()

    far_n = []

    def far_step(j):
        k0, k1 = nsplit[j]
        near_n[j].wait_recv()
        nsb[k0:k1] = (npart[k0:k1, blk(t2), :].astype(F32) + nrb1[0, k0:k1].astype(F32)).astype(BF16)

    def far_send(j):
        k0, k1 = nsplit[j]
        c = remote(nsb.at[k0:k1], nrb2.at[k0:k1], 41 + j, {"tp": t2})
        c.start()
        far_n.append(c)

    far_step(0)
    ex_up1 = remote(gup.at[:, rows_of(odp, QR), :], gup_rb.at[:, QR:2 * QR, :], 36, {"dp": odp})
    ex_up1.start()
    far_step(1)
    far_send(0)
    far_step(2)
    far_send(1)
    ex_up0.wait_recv()
    gfin[:, rows_of(dp, 0), :] = (gup[:, rows_of(dp, 0), :] + gup_rb[:, 0:QR, :]).astype(BF16)
    far_send(2)

    s3 = jnp.zeros((ch, nat), F32)
    for k in range(COEFS):
        rf = npart[k].astype(F32) * gcol[degree_of(k)]
        if k == 0:
            st0 = jnp.sum(rf, axis=0, keepdims=True)
            st1 = jnp.sum(rf * hat_s, axis=0, keepdims=True)
        else:
            s3 = s3 + rf * xg[k].astype(F32)
    st2 = jnp.sum(s3, axis=0, keepdims=True)
    st_snd[...] = jnp.concatenate([st0, st1, st2, jnp.zeros((5, nat), F32)], axis=0)
    bk_up0 = remote(gfin.at[:, rows_of(dp, 0), :], gfin.at[:, rows_of(dp, 0), :], 35, {"dp": odp})
    bk_up0.start()
    ssend = []
    for j, dev in enumerate((t1, t2, t3)):
        c = remote(st_snd, st_all.at[j], 37 + j, {"tp": dev})
        c.start()
        ssend.append(c)

    bk_dn.wait_recv()
    ddown_ref[...] = gfin_dn[0:5]
    dgate_ref[...] = gfin_dn[5].astype(F32).T.astype(BF16)
    ex_up1.wait_recv()
    gfin[:, rows_of(dp, QR), :] = (gup[:, rows_of(dp, QR), :] + gup_rb[:, QR:2 * QR, :]).astype(BF16)
    for c in ssend:
        c.wait_recv()
    stat = st_snd[...] + st_all[0] + st_all[1] + st_all[2]
    b0 = stat[0:1] / ch
    b1 = stat[1:2] / ch
    b2 = (inv_v * inv_v * inv_v) * (stat[2:3] / (ch * (COEFS - 1)))
    bk_up1 = remote(gfin.at[:, rows_of(dp, QR), :], gfin.at[:, rows_of(dp, QR), :], 40, {"dp": odp})
    bk_up1.start()
    near_o.wait_recv()
    for j, (k0, k1) in enumerate(nsplit):
        far_n[j].wait_recv()
        for k in range(k0, k1):
            dn = (npart[k, blk(t), :].astype(F32) + nrb1[1, k].astype(F32) + nrb2[k].astype(F32)).astype(BF16).astype(F32)
            dhat = dn * gcol[degree_of(k), blk(t), :]
            xk = xg[k, blk(t), :].astype(F32)
            if k == 0:
                dxk = inv_s * (dhat - b0 - (xk - mean_s) * inv_s * b1)
            else:
                dxk = inv_v * dhat - xk * b2
            dx_ref[k] = (dxk + gg[k, blk(t), :].astype(F32)).astype(BF16)

    bk_up0.wait_recv()
    bk_up1.wait_recv()
    for l in range(5):
        dup_ref[l] = gfin[l].astype(F32).T.astype(BF16)
    for c in far_g + fwd_x + fwd_g + gsend + near_d + near_n + far_n + ssend + [near_x, near_g, near_o, far_d, ex_dn, ex_up0, ex_up1, bk_dn, bk_up0, bk_up1]:
        c.wait_send()


def flush(a, b, c, d, e, oa, ob, oc, od, oe, sem):
    cs = [pltpu.make_async_copy(i, o, sem.at[j]) for j, (i, o) in enumerate(zip((a, b, c, d, e), (oa, ob, oc, od, oe)))]
    for x in cs:
        x.start()
    for x in cs:
        x.wait()


def solution(mesh):
    tp_size = mesh.shape['tp']
    act_spec = P('dp', None, 'tp')
    in_specs = (act_spec, P(None, 'tp'), P(None, None, 'tp'), P(None, 'tp'), P(None, 'tp', None), P(None, None), P(None, None), act_spec)
    out_specs = (act_spec, act_spec, P(None, None, 'tp'), P(None, 'tp'), P(None, 'tp', None))

    def local_step(x_loc, gain_loc, up_loc, gate_loc, down_loc, to_grid, from_grid, grad_loc):
        nat, coefs, cl = x_loc.shape
        ch = cl * tp_size
        grid_pts = to_grid.shape[1]
        pp = -(-grid_pts // 16) * 16
        xt = x_loc.transpose(1, 2, 0)
        gt = grad_loc.transpose(1, 2, 0)
        any_spec = pl.BlockSpec(memory_space=pl.ANY)
        vmem = pl.BlockSpec(memory_space=pltpu.VMEM)
        full = pltpu.VMEM((coefs, ch, nat), BF16)
        blkb = pltpu.VMEM((coefs, cl, nat), BF16)
        sq = lambda n, d: pltpu.VMEM((n, 128, 128), d)
        shapes = (xt.shape, xt.shape, up_loc.shape, gate_loc.shape, down_loc.shape)
        outs = pl.pallas_call(
            functools.partial(kernel, tp_size, grid_pts),
            out_shape=tuple(pltpu.VMEM(sh, BF16) for sh in shapes),
            in_specs=[any_spec] * 8,
            out_specs=[vmem] * 5,
            scratch_shapes=[
                full, full, full, full, full, full, full,
                pltpu.VMEM((66 * YSTRIDE, 128), F32), pltpu.VMEM((66 * YSTRIDE, 128), F32),
                pltpu.VMEM((KPAD * 136, 128), F32), pltpu.VMEM((64 * pp, 256), F32),
                pltpu.VMEM(gain_loc.shape, F32), pltpu.VMEM((8, 128), F32), pltpu.VMEM((3, 8, 128), F32), sq(5, F32),
                sq(5, BF16), pltpu.VMEM((128, 128), BF16), sq(5, BF16), sq(5, BF16), pltpu.VMEM((128, 128), BF16), sq(5, BF16),
                pltpu.VMEM(to_grid.shape, F32), pltpu.VMEM(from_grid.shape[::-1], F32),
                pltpu.VMEM((pp, KPAD), BF16), pltpu.VMEM((KPAD, 384), BF16), pltpu.VMEM((pp, KPAD), BF16), pltpu.VMEM((KPAD, 384), BF16),
                pltpu.VMEM((2, coefs, cl, nat), BF16), blkb, blkb, pltpu.VMEM((2, coefs, cl, nat), BF16), blkb, blkb,
                pltpu.VMEM((8, 128), F32), pltpu.VMEM((3, 8, 128), F32),
                sq(6, F32), pltpu.VMEM((6, 64, 128), F32), sq(5, F32), pltpu.VMEM((5, 64, 128), F32), sq(5, BF16), sq(6, BF16),
                pltpu.VMEM((128, nat), BF16),
                pltpu.VMEM((pp, 256), BF16), pltpu.VMEM((pp, 256), BF16), pltpu.VMEM((pp, 256), BF16), pltpu.VMEM((pp, 256), BF16),
                pltpu.VMEM((pp, 256), BF16), pltpu.VMEM((pp, 256), BF16), pltpu.VMEM((pp, 256), BF16), pltpu.VMEM((pp, 256), BF16),
                pltpu.SemaphoreType.DMA((12,)), pltpu.SemaphoreType.DMA((44,)), pltpu.SemaphoreType.DMA((44,)),
            ],
            compiler_params=pltpu.CompilerParams(collective_id=0, has_side_effects=True, vmem_limit_bytes=60 * 1024 * 1024),
        )(xt, gain_loc, up_loc, gate_loc, down_loc, to_grid, from_grid.T, gt)
        out_t, dx_t, d_up, d_gate, d_down = pl.pallas_call(
            flush,
            out_shape=tuple(jax.ShapeDtypeStruct(sh, BF16) for sh in shapes),
            in_specs=[vmem] * 5,
            out_specs=[any_spec] * 5,
            scratch_shapes=[pltpu.SemaphoreType.DMA((5,))],
        )(*[pltpu.with_memory_space_constraint(o, pltpu.VMEM) for o in outs])
        return out_t.transpose(2, 0, 1), dx_t.transpose(2, 0, 1), d_up, d_gate, d_down

    return jax.shard_map(local_step, mesh=mesh, in_specs=in_specs, out_specs=out_specs, check_vma=False)
```

```python
import functools
import math
import jax
import jax.numpy as jnp
from jax import lax
from jax.experimental import pallas as pl
from jax.experimental.pallas import tpu as pltpu
from jax.sharding import PartitionSpec as P

NORM_EPS = 1e-5
MESH = pl.DeviceIdType.MESH
F32 = jnp.float32
BF16 = jnp.bfloat16
COEFS = 25
KPAD = 32
YSTRIDE = 40
UNROLL = 4
QR = 32


def degree_of(k):
    return math.isqrt(k)


def rows_dot(a, b):
    return lax.dot_general(a, b, (((1,), (0,)), ((), ())), preferred_element_type=F32)


def lanes_dot(a, b):
    return lax.dot_general(a, b, (((1,), (1,)), ((), ())), preferred_element_type=F32)


def kernel(tp_size, grid_pts, x_hbm, gain_hbm, up_hbm, gate_hbm, down_hbm, tog_hbm, frg_hbm, g_hbm,
           out_ref, dx_ref, dup_ref, dgate_ref, ddown_ref,
           xg, gg, xn, mb, dyb, dpart, npart, ya, yb, zs, hs,
           gain_in, gain_snd, gain_all, gcol, up, gate, down, upt, gatet, downt,
           tog, frg, tt, tmat, fmat, ft, rb1, sb, rb2, nrb1, nsb, nrb2,
           st_snd, st_all, gdn, gdn_rb, gup, gup_rb, gfin, gfin_dn, amat, sbuf0, sbuf1, sbuf2, sbuf3, gbuf0, gbuf1, gbuf2, gbuf3,
           loc_sem, snd_sem, rcv_sem):
    sbuf, gbuf = (sbuf0, sbuf1, sbuf2, sbuf3), (gbuf0, gbuf1, gbuf2, gbuf3)
    dp = lax.axis_index("dp")
    t = lax.axis_index("tp")
    core = lax.rem(t, 2)
    t1 = t + 1 - 2 * core
    t2 = lax.rem(t + 2, 4)
    t3 = lax.rem(t1 + 2, 4)
    odp = 1 - dp
    cl = xg.shape[1] // tp_size
    ch = xg.shape[1]
    nat = xg.shape[2]
    pp = tt.shape[0]

    def blk(i):
        return pl.ds(pl.multiple_of(i * cl, cl), cl)

    def local(src, dst, i):
        c = pltpu.make_async_copy(src, dst, loc_sem.at[i])
        c.start()
        return c

    def remote(src, dst, i, dev):
        return pltpu.make_async_remote_copy(src_ref=src, dst_ref=dst, send_sem=snd_sem.at[i], recv_sem=rcv_sem.at[i],
                                            device_id=dev, device_id_type=MESH)

    c_gain = local(gain_hbm, gain_in, 0)
    ksplit = ((0, 8), (8, 15), (15, 22), (22, 25))
    c_x = [local(x_hbm.at[k0:k1], xg.at[k0:k1, blk(t), :], 7 + j) for j, (k0, k1) in enumerate(ksplit)]
    c_tog = local(tog_hbm, tog, 2)
    c_frg = local(frg_hbm, frg, 3)
    c_up = local(up_hbm, up, 4)
    c_gate = local(gate_hbm, gate, 5)
    c_down = local(down_hbm, down, 6)
    c_g = local(g_hbm, gg.at[:, blk(t), :], 1)

    barrier = pltpu.get_barrier_semaphore()
    for dev in ({"tp": t1}, {"tp": t2}, {"tp": t3}, {"dp": odp}):
        pl.semaphore_signal(barrier, inc=1, device_id=dev, device_id_type=MESH)
    c_gain.wait()
    gain_snd[...] = jnp.zeros_like(gain_snd)
    gain_snd[0:5, 0:cl] = gain_in[...]
    placed = pltpu.roll(gain_snd[...], t * cl, 1)
    gain_snd[...] = placed
    pl.semaphore_wait(barrier, 4)
    gsend = []
    for j, dev in enumerate((t1, t2, t3)):
        c = remote(gain_snd, gain_all.at[j], 20 + j, {"tp": dev})
        c.start()
        gsend.append(c)

    def gather_start(dst, base, ready=None):
        far = []
        for j, (k0, k1) in enumerate(ksplit):
            if ready:
                ready[j].wait()
            c = remote(dst.at[k0:k1, blk(t), :], dst.at[k0:k1, blk(t), :], base + j, {"tp": t2})
            c.start()
            far.append(c)
        k0, k1 = ksplit[-1]
        c = remote(dst.at[k0:k1, blk(t), :], dst.at[k0:k1, blk(t), :], base + 8, {"tp": t3})
        c.start()
        far.append(c)
        near = remote(dst.at[:, blk(t), :], dst.at[:, blk(t), :], base + 4, {"tp": t1})
        near.start()
        return far, near

    def gather_finish(far, near, dst, base, step=None):
        fwd = []
        for j, (k0, k1) in enumerate(ksplit[:-1]):
            far[j].wait_recv()
            c = remote(dst.at[k0:k1, blk(t2), :], dst.at[k0:k1, blk(t2), :], base + 5 + j, {"tp": t1})
            c.start()
            fwd.append(c)
            if step and j == 0:
                near.wait_recv()
                step((t, t1), 0, COEFS)
            if step and j > 0:
                fwd[j - 1].wait_recv()
                step((t2, t3), *ksplit[j - 1])
        return fwd

    def gather_wait(far, near, fwd):
        near.wait_recv()
        for c in fwd:
            c.wait_recv()
        far[-2].wait_recv()
        far[-1].wait_recv()

    far_x, near_x = gather_start(xg, 0, c_x)

    c_tog.wait()
    c_frg.wait()
    tpad = jnp.zeros((KPAD, 384), F32)
    tmat[...] = tpad.astype(BF16)
    ft[...] = tpad.astype(BF16)
    tmat[0:COEFS, 0:grid_pts] = tog[...].astype(BF16)
    frg_pad = jnp.concatenate([jnp.zeros((1, grid_pts), F32), frg[...]], axis=0)
    ft[0:COEFS, 0:grid_pts] = frg_pad.astype(BF16)
    for src, dst in ((tmat, tt), (ft, fmat)):
        wide = jnp.concatenate([src[...].astype(F32) * 0.5, jnp.zeros((128 - KPAD, 384), F32)], axis=0)
        for j in range(3):
            tr = wide[:, 128 * j:128 * (j + 1)].T
            rows = min(128, pp - 128 * j)
            dst[128 * j:128 * j + rows, :] = tr[0:rows, 0:KPAD].astype(BF16)
    c_up.wait()
    c_gate.wait()
    c_down.wait()
    for l in range(5):
        upt[l] = up[l].astype(F32).T.astype(BF16)
        downt[l] = down[l].astype(F32).T.astype(BF16)
    gatet[...] = gate[...].astype(F32).T.astype(BF16)
    ya[...] = jnp.zeros_like(ya)
    yb[...] = jnp.zeros_like(yb)
    for c in gsend:
        c.wait_recv()
    gain_full = placed + gain_all[0] + gain_all[1] + gain_all[2]
    for l in range(5):
        gcol[l] = jnp.broadcast_to(gain_full[l:l + 1, :], (ch, ch)).T

    sums = [jnp.zeros((cl, nat), F32)]

    def square_step(blocks, k0, k1):
        for k in range(max(k0, 1), k1):
            for i in blocks:
                v = xg[k, blk(i), :].astype(F32)
                sums[0] = sums[0] + v * v

    fwd_x = gather_finish(far_x, near_x, xg, 0, square_step)
    fwd_x[-1].wait_recv()
    square_step((t2, t3), *ksplit[2])
    far_x[-2].wait_recv()
    far_x[-1].wait_recv()
    square_step((t2, t3), *ksplit[3])
    for c in far_x:
        c.wait_send()
    c_g.wait()
    far_g, near_g = gather_start(gg, 10)

    x0 = xg[0].astype(F32)
    mean_s = jnp.sum(x0, axis=0, keepdims=True) / ch
    cent = x0 - mean_s
    inv_s = lax.rsqrt(jnp.sum(cent * cent, axis=0, keepdims=True) / ch + NORM_EPS)
    hat_s = cent * inv_s
    inv_v = lax.rsqrt(jnp.sum(sums[0], axis=0, keepdims=True) / (ch * (COEFS - 1)) + NORM_EPS)
    xn[0] = (hat_s * gcol[0]).astype(BF16)
    for k in range(1, COEFS):
        xn[k] = (xg[k].astype(F32) * inv_v * gcol[degree_of(k)]).astype(BF16)

    def by_degree(lhs_of, get, lo=0, hi=COEFS):
        for l in range(5):
            k = max(l * l, lo)
            k1 = min((l + 1) * (l + 1), hi)
            while k < k1:
                n = min(2, k1 - k)
                r = rows_dot(lhs_of(l), get(k) if n == 1 else jnp.concatenate([get(k), get(k + 1)], axis=1))
                for j in range(n):
                    yield k + j, r[:, nat * j:nat * (j + 1)]
                k += n

    def over_degree(a_of, b_of, l):
        ks = range(l * l, (l + 1) * (l + 1))
        return lanes_dot(jnp.concatenate([a_of(k) for k in ks], axis=1), jnp.concatenate([b_of(k) for k in ks], axis=1))

    def spread(get, lhs_of):
        for k, r in by_degree(lhs_of, get):
            ya[pl.ds(k, 64, stride=YSTRIDE), :] = r[0:64]
            yb[pl.ds(k, 64, stride=YSTRIDE), :] = r[64:128]

    spread(lambda k: xn[k], lambda l: upt[l])
    a_r = rows_dot(gatet[...], xn[0]).astype(BF16)
    amat[...] = a_r
    a_h = a_r.astype(F32) * 0.5
    mb[0] = (a_h * (1.0 + jnp.tanh(a_h))).astype(BF16)

    def pair(i):
        base = pl.multiple_of(i * YSTRIDE, 8)
        return jnp.concatenate([ya[pl.ds(base, KPAD), :], yb[pl.ds(base, KPAD), :]], axis=1).astype(BF16)

    def put(i, r):
        zs[pl.ds(i, KPAD, stride=136), :] = r[:, 0:128]
        zs[pl.ds(i + 64, KPAD, stride=136), :] = r[:, 128:256]

    def stage_u(p, dst):
        dst[...] = rows_dot(tt[...], pair(p)).astype(BF16)

    def stage_s(p, src, dst):
        h = src[...].astype(F32)
        w = 1.0 + jnp.tanh(h)
        s = h * w
        dst[...] = s.astype(BF16)
        hs[pl.ds(pl.multiple_of(p * pp, 16), pp), :] = w + s * (2.0 - w)

    def stage_z(p, src, lhs):
        put(p, rows_dot(lhs[:, 0:pp], src[...]))

    stage_u(0, gbuf[0])
    stage_u(1, gbuf[1])

    def fwd_body(it, carry):
        for half_step in range(2):
            p = it * UNROLL + 2 * half_step
            now, other = 2 * (half_step % 2), 2 * ((half_step + 1) % 2)
            for j in range(2):
                stage_z(jnp.maximum(p + j - 2, 0), sbuf[other + j], ft)
                stage_u(p + j + 2, gbuf[other + j])
                stage_s(p + j, gbuf[now + j], sbuf[now + j])
        return carry

    lax.fori_loop(0, 48 // UNROLL, fwd_body, 0)
    fwd_g = gather_finish(far_g, near_g, gg, 10)
    lax.fori_loop(48 // UNROLL, 64 // UNROLL, fwd_body, 0)
    stage_z(62, sbuf[2], ft)
    stage_z(63, sbuf[3], ft)

    for k in range(1, COEFS):
        mb[k] = zs[k * 136:k * 136 + 128, :].astype(BF16)
    for k, r in by_degree(lambda l: downt[l], lambda k: mb[k]):
        dpart[k] = r.astype(BF16)

    def scatter_near(part, rb, base):
        cs = []
        for j, b in enumerate((t3, t1)):
            c = remote(part.at[:, blk(b), :], rb.at[j], base + j, {"tp": t1})
            c.start()
            cs.append(c)
        return cs

    near_d = scatter_near(dpart, rb1, 23)

    gather_wait(far_g, near_g, fwd_g)
    spread(lambda k: gg[k], lambda l: down[l])
    dm0 = rows_dot(down[0], gg[0]).astype(BF16).astype(F32)
    a_h = amat[...].astype(F32) * 0.5
    w_a = 1.0 + jnp.tanh(a_h)
    da = (dm0 * (0.5 * w_a * (1.0 + a_h * (2.0 - w_a)))).astype(BF16)

    for l in range(5):
        gdn[l] = over_degree(lambda k: mb[k], lambda k: gg[k], l)
    gdn[5] = lanes_dot(da, xn[0])
    half = 64
    mine = pl.ds(pl.multiple_of(dp * half, half), half)
    theirs = pl.ds(pl.multiple_of(odp * half, half), half)
    ex_dn = remote(gdn.at[:, theirs, :], gdn_rb, 26, {"dp": odp})
    ex_dn.start()

    def stage_g(p, dst):
        dst[...] = rows_dot(fmat[...], pair(p)).astype(BF16)

    def stage_e(p, src, dst):
        gp = hs[pl.ds(pl.multiple_of(p * pp, 16), pp), :]
        dst[...] = (src[...].astype(F32) * gp).astype(BF16)

    stage_g(0, gbuf[0])
    stage_g(1, gbuf[1])

    def bwd_body(it, carry):
        for half_step in range(2):
            p = it * UNROLL + 2 * half_step
            now, other = 2 * (half_step % 2), 2 * ((half_step + 1) % 2)
            for j in range(2):
                stage_z(jnp.maximum(p + j - 2, 0), sbuf[other + j], tmat)
                stage_g(p + j + 2, gbuf[other + j])
                stage_e(p + j, gbuf[now + j], sbuf[now + j])
        return carry

    def grad_up(lo):
        def dy(k):
            return jnp.concatenate([dyb[k, lo:lo + QR, :], dyb[k, 64 + lo:64 + lo + QR, :]], axis=0)

        for k in range(COEFS):
            for o in (lo, 64 + lo):
                dyb[k, o:o + QR, :] = zs[k * 136 + o:k * 136 + o + QR, :].astype(BF16)
        for l in range(5):
            acc = over_degree(dy, lambda k: xn[k], l)
            gup[l, lo:lo + QR, :] = acc[0:QR]
            gup[l, 64 + lo:64 + lo + QR, :] = acc[QR:2 * QR]

    def rows_of(d, lo):
        return pl.ds(pl.multiple_of(d * half + lo, QR), QR)

    mid_steps = (QR + 4) // UNROLL
    lax.fori_loop(0, 4 // UNROLL, bwd_body, 0)
    near_d[0].wait_recv()
    sb[...] = (dpart[:, blk(t2), :].astype(F32) + rb1[0].astype(F32)).astype(BF16)
    far_d = remote(sb, rb2, 25, {"tp": t2})
    far_d.start()
    lax.fori_loop(4 // UNROLL, mid_steps, bwd_body, 0)

    grad_up(0)
    ex_up0 = remote(gup.at[:, rows_of(odp, 0), :], gup_rb.at[:, 0:QR, :], 33, {"dp": odp})
    ex_up0.start()

    lax.fori_loop(mid_steps, 64 // UNROLL, bwd_body, 0)
    stage_z(62, sbuf[2], tmat)
    stage_z(63, sbuf[3], tmat)
    ex_dn.wait_recv()
    gfin_dn[:, mine, :] = (gdn[:, mine, :] + gdn_rb[...]).astype(BF16)

    def full_dy(k):
        return jnp.concatenate([dyb[k, 0:QR, :], zs[k * 136 + QR:k * 136 + 64, :].astype(BF16),
                                dyb[k, 64:64 + QR, :], zs[k * 136 + 64 + QR:k * 136 + 128, :].astype(BF16)], axis=0)

    nsplit = ((0, 9), (9, 16), (16, 25))
    near_n = []
    for j, (k0, k1) in enumerate(nsplit):
        for k, r in by_degree(lambda l: up[l], full_dy, k0, k1):
            if k == 0:
                r = r + rows_dot(gate[...], da)
            npart[k] = r.astype(BF16)
        c = remote(npart.at[k0:k1, blk(t3), :], nrb1.at[0, k0:k1], 27 + j, {"tp": t1})
        c.start()
        near_n.append(c)
        if j == 0:
            bk_dn = remote(gfin_dn.at[:, mine, :], gfin_dn.at[:, mine, :], 34, {"dp": odp})
            bk_dn.start()
    grad_up(QR)
    near_o = remote(npart.at[:, blk(t1), :], nrb1.at[1], 30, {"tp": t1})
    near_o.start()

    far_n = []

    def far_step(j):
        k0, k1 = nsplit[j]
        near_n[j].wait_recv()
        nsb[k0:k1] = (npart[k0:k1, blk(t2), :].astype(F32) + nrb1[0, k0:k1].astype(F32)).astype(BF16)

    def far_send(j):
        k0, k1 = nsplit[j]
        c = remote(nsb.at[k0:k1], nrb2.at[k0:k1], 41 + j, {"tp": t2})
        c.start()
        far_n.append(c)

    far_step(0)
    ex_up1 = remote(gup.at[:, rows_of(odp, QR), :], gup_rb.at[:, QR:2 * QR, :], 36, {"dp": odp})
    ex_up1.start()
    far_step(1)
    far_send(0)
    far_step(2)
    far_send(1)
    ex_up0.wait_recv()
    gfin[:, rows_of(dp, 0), :] = (gup[:, rows_of(dp, 0), :] + gup_rb[:, 0:QR, :]).astype(BF16)
    far_send(2)

    near_d[1].wait_recv()
    far_d.wait_recv()
    own = dpart[:, blk(t), :].astype(F32) + rb1[1].astype(F32) + rb2[...].astype(F32)
    out_ref[...] = (xg[:, blk(t), :].astype(F32) + own).astype(BF16)
    s3 = jnp.zeros((ch, nat), F32)
    for k in range(COEFS):
        rf = npart[k].astype(F32) * gcol[degree_of(k)]
        if k == 0:
            st0 = jnp.sum(rf, axis=0, keepdims=True)
            st1 = jnp.sum(rf * hat_s, axis=0, keepdims=True)
        else:
            s3 = s3 + rf * xg[k].astype(F32)
    st2 = jnp.sum(s3, axis=0, keepdims=True)
    st_snd[...] = jnp.concatenate([st0, st1, st2, jnp.zeros((5, nat), F32)], axis=0)
    bk_up0 = remote(gfin.at[:, rows_of(dp, 0), :], gfin.at[:, rows_of(dp, 0), :], 35, {"dp": odp})
    bk_up0.start()
    ssend = []
    for j, dev in enumerate((t1, t2, t3)):
        c = remote(st_snd, st_all.at[j], 37 + j, {"tp": dev})
        c.start()
        ssend.append(c)

    bk_dn.wait_recv()
    ddown_ref[...] = gfin_dn[0:5]
    dgate_ref[...] = gfin_dn[5].astype(F32).T.astype(BF16)
    ex_up1.wait_recv()
    gfin[:, rows_of(dp, QR), :] = (gup[:, rows_of(dp, QR), :] + gup_rb[:, QR:2 * QR, :]).astype(BF16)
    for c in ssend:
        c.wait_recv()
    stat = st_snd[...] + st_all[0] + st_all[1] + st_all[2]
    b0 = stat[0:1] / ch
    b1 = stat[1:2] / ch
    b2 = (inv_v * inv_v * inv_v) * (stat[2:3] / (ch * (COEFS - 1)))
    bk_up1 = remote(gfin.at[:, rows_of(dp, QR), :], gfin.at[:, rows_of(dp, QR), :], 40, {"dp": odp})
    bk_up1.start()
    near_o.wait_recv()
    for j, (k0, k1) in enumerate(nsplit):
        far_n[j].wait_recv()
        for k in range(k0, k1):
            dn = (npart[k, blk(t), :].astype(F32) + nrb1[1, k].astype(F32) + nrb2[k].astype(F32)).astype(BF16).astype(F32)
            dhat = dn * gcol[degree_of(k), blk(t), :]
            xk = xg[k, blk(t), :].astype(F32)
            if k == 0:
                dxk = inv_s * (dhat - b0 - (xk - mean_s) * inv_s * b1)
            else:
                dxk = inv_v * dhat - xk * b2
            dx_ref[k] = (dxk + gg[k, blk(t), :].astype(F32)).astype(BF16)

    bk_up0.wait_recv()
    bk_up1.wait_recv()
    for l in range(5):
        dup_ref[l] = gfin[l].astype(F32).T.astype(BF16)
    for c in far_g + fwd_x + fwd_g + gsend + near_d + near_n + far_n + ssend + [near_x, near_g, near_o, far_d, ex_dn, ex_up0, ex_up1, bk_dn, bk_up0, bk_up1]:
        c.wait_send()


def flush(a, b, c, d, e, oa, ob, oc, od, oe, sem):
    cs = [pltpu.make_async_copy(i, o, sem.at[j]) for j, (i, o) in enumerate(zip((a, b, c, d, e), (oa, ob, oc, od, oe)))]
    for x in cs:
        x.start()
    for x in cs:
        x.wait()


def solution(mesh):
    tp_size = mesh.shape['tp']
    act_spec = P('dp', None, 'tp')
    in_specs = (act_spec, P(None, 'tp'), P(None, None, 'tp'), P(None, 'tp'), P(None, 'tp', None), P(None, None), P(None, None), act_spec)
    out_specs = (act_spec, act_spec, P(None, None, 'tp'), P(None, 'tp'), P(None, 'tp', None))

    def local_step(x_loc, gain_loc, up_loc, gate_loc, down_loc, to_grid, from_grid, grad_loc):
        nat, coefs, cl = x_loc.shape
        ch = cl * tp_size
        grid_pts = to_grid.shape[1]
        pp = -(-grid_pts // 16) * 16
        xt = x_loc.transpose(1, 2, 0)
        gt = grad_loc.transpose(1, 2, 0)
        any_spec = pl.BlockSpec(memory_space=pl.ANY)
        vmem = pl.BlockSpec(memory_space=pltpu.VMEM)
        full = pltpu.VMEM((coefs, ch, nat), BF16)
        blkb = pltpu.VMEM((coefs, cl, nat), BF16)
        sq = lambda n, d: pltpu.VMEM((n, 128, 128), d)
        shapes = (xt.shape, xt.shape, up_loc.shape, gate_loc.shape, down_loc.shape)
        outs = pl.pallas_call(
            functools.partial(kernel, tp_size, grid_pts),
            out_shape=tuple(pltpu.VMEM(sh, BF16) for sh in shapes),
            in_specs=[any_spec] * 8,
            out_specs=[vmem] * 5,
            scratch_shapes=[
                full, full, full, full, full, full, full,
                pltpu.VMEM((66 * YSTRIDE, 128), F32), pltpu.VMEM((66 * YSTRIDE, 128), F32),
                pltpu.VMEM((KPAD * 136, 128), F32), pltpu.VMEM((64 * pp, 256), F32),
                pltpu.VMEM(gain_loc.shape, F32), pltpu.VMEM((8, 128), F32), pltpu.VMEM((3, 8, 128), F32), sq(5, F32),
                sq(5, BF16), pltpu.VMEM((128, 128), BF16), sq(5, BF16), sq(5, BF16), pltpu.VMEM((128, 128), BF16), sq(5, BF16),
                pltpu.VMEM(to_grid.shape, F32), pltpu.VMEM(from_grid.shape[::-1], F32),
                pltpu.VMEM((pp, KPAD), BF16), pltpu.VMEM((KPAD, 384), BF16), pltpu.VMEM((pp, KPAD), BF16), pltpu.VMEM((KPAD, 384), BF16),
                pltpu.VMEM((2, coefs, cl, nat), BF16), blkb, blkb, pltpu.VMEM((2, coefs, cl, nat), BF16), blkb, blkb,
                pltpu.VMEM((8, 128), F32), pltpu.VMEM((3, 8, 128), F32),
                sq(6, F32), pltpu.VMEM((6, 64, 128), F32), sq(5, F32), pltpu.VMEM((5, 64, 128), F32), sq(5, BF16), sq(6, BF16),
                pltpu.VMEM((128, nat), BF16),
                pltpu.VMEM((pp, 256), BF16), pltpu.VMEM((pp, 256), BF16), pltpu.VMEM((pp, 256), BF16), pltpu.VMEM((pp, 256), BF16),
                pltpu.VMEM((pp, 256), BF16), pltpu.VMEM((pp, 256), BF16), pltpu.VMEM((pp, 256), BF16), pltpu.VMEM((pp, 256), BF16),
                pltpu.SemaphoreType.DMA((12,)), pltpu.SemaphoreType.DMA((44,)), pltpu.SemaphoreType.DMA((44,)),
            ],
            compiler_params=pltpu.CompilerParams(collective_id=0, has_side_effects=True, vmem_limit_bytes=60 * 1024 * 1024),
        )(xt, gain_loc, up_loc, gate_loc, down_loc, to_grid, from_grid.T, gt)
        out_t, dx_t, d_up, d_gate, d_down = pl.pallas_call(
            flush,
            out_shape=tuple(jax.ShapeDtypeStruct(sh, BF16) for sh in shapes),
            in_specs=[vmem] * 5,
            out_specs=[any_spec] * 5,
            scratch_shapes=[pltpu.SemaphoreType.DMA((5,))],
        )(*[pltpu.with_memory_space_constraint(o, pltpu.VMEM) for o in outs])
        return out_t.transpose(2, 0, 1), dx_t.transpose(2, 0, 1), d_up, d_gate, d_down

    return jax.shard_map(local_step, mesh=mesh, in_specs=in_specs, out_specs=out_specs, check_vma=False)
```

```python
import functools
import math
import jax
import jax.numpy as jnp
from jax import lax
from jax.experimental import pallas as pl
from jax.experimental.pallas import tpu as pltpu
from jax.sharding import PartitionSpec as P

NORM_EPS = 1e-5
MESH = pl.DeviceIdType.MESH
F32 = jnp.float32
BF16 = jnp.bfloat16
COEFS = 25
KPAD = 32
YSTRIDE = 40
UNROLL = 4
QR = 48


def degree_of(k):
    return math.isqrt(k)


def rows_dot(a, b):
    return lax.dot_general(a, b, (((1,), (0,)), ((), ())), preferred_element_type=F32)


def lanes_dot(a, b):
    return lax.dot_general(a, b, (((1,), (1,)), ((), ())), preferred_element_type=F32)


def kernel(tp_size, grid_pts, x_hbm, gain_hbm, up_hbm, gate_hbm, down_hbm, tog_hbm, frg_hbm, g_hbm,
           out_ref, dx_ref, dup_ref, dgate_ref, ddown_ref,
           xg, gg, xn, mb, dyb, dpart, npart, ya, yb, zs, hs,
           gain_in, gain_snd, gain_all, gcol, up, gate, down, upt, gatet, downt,
           tog, frg, tt, tmat, fmat, ft, rb1, sb, rb2, nrb1, nsb, nrb2,
           st_snd, st_all, gdn, gdn_rb, gup, gup_rb, gfin, gfin_dn, amat, sbuf0, sbuf1, sbuf2, sbuf3, gbuf0, gbuf1, gbuf2, gbuf3,
           loc_sem, snd_sem, rcv_sem):
    sbuf, gbuf = (sbuf0, sbuf1, sbuf2, sbuf3), (gbuf0, gbuf1, gbuf2, gbuf3)
    dp = lax.axis_index("dp")
    t = lax.axis_index("tp")
    core = lax.rem(t, 2)
    t1 = t + 1 - 2 * core
    t2 = lax.rem(t + 2, 4)
    t3 = lax.rem(t1 + 2, 4)
    odp = 1 - dp
    cl = xg.shape[1] // tp_size
    ch = xg.shape[1]
    nat = xg.shape[2]
    pp = tt.shape[0]

    def blk(i):
        return pl.ds(pl.multiple_of(i * cl, cl), cl)

    def local(src, dst, i):
        c = pltpu.make_async_copy(src, dst, loc_sem.at[i])
        c.start()
        return c

    def remote(src, dst, i, dev):
        return pltpu.make_async_remote_copy(src_ref=src, dst_ref=dst, send_sem=snd_sem.at[i], recv_sem=rcv_sem.at[i],
                                            device_id=dev, device_id_type=MESH)

    c_gain = local(gain_hbm, gain_in, 0)
    ksplit = ((0, 8), (8, 15), (15, 22), (22, 25))
    c_x = [local(x_hbm.at[k0:k1], xg.at[k0:k1, blk(t), :], 7 + j) for j, (k0, k1) in enumerate(ksplit)]
    c_tog = local(tog_hbm, tog, 2)
    c_frg = local(frg_hbm, frg, 3)
    c_up = local(up_hbm, up, 4)
    c_gate = local(gate_hbm, gate, 5)
    c_down = local(down_hbm, down, 6)
    c_g = local(g_hbm, gg.at[:, blk(t), :], 1)

    barrier = pltpu.get_barrier_semaphore()
    for dev in ({"tp": t1}, {"tp": t2}, {"tp": t3}, {"dp": odp}):
        pl.semaphore_signal(barrier, inc=1, device_id=dev, device_id_type=MESH)
    c_gain.wait()
    gain_snd[...] = jnp.zeros_like(gain_snd)
    gain_snd[0:5, 0:cl] = gain_in[...]
    placed = pltpu.roll(gain_snd[...], t * cl, 1)
    gain_snd[...] = placed
    pl.semaphore_wait(barrier, 4)
    gsend = []
    for j, dev in enumerate((t1, t2, t3)):
        c = remote(gain_snd, gain_all.at[j], 20 + j, {"tp": dev})
        c.start()
        gsend.append(c)

    def gather_start(dst, base, ready=None):
        far = []
        for j, (k0, k1) in enumerate(ksplit):
            if ready:
                ready[j].wait()
            c = remote(dst.at[k0:k1, blk(t), :], dst.at[k0:k1, blk(t), :], base + j, {"tp": t2})
            c.start()
            far.append(c)
        k0, k1 = ksplit[-1]
        c = remote(dst.at[k0:k1, blk(t), :], dst.at[k0:k1, blk(t), :], base + 8, {"tp": t3})
        c.start()
        far.append(c)
        near = remote(dst.at[:, blk(t), :], dst.at[:, blk(t), :], base + 4, {"tp": t1})
        near.start()
        return far, near

    def gather_finish(far, near, dst, base, step=None):
        fwd = []
        for j, (k0, k1) in enumerate(ksplit[:-1]):
            far[j].wait_recv()
            c = remote(dst.at[k0:k1, blk(t2), :], dst.at[k0:k1, blk(t2), :], base + 5 + j, {"tp": t1})
            c.start()
            fwd.append(c)
            if step and j == 0:
                near.wait_recv()
                step((t, t1), 0, COEFS)
            if step and j > 0:
                fwd[j - 1].wait_recv()
                step((t2, t3), *ksplit[j - 1])
        return fwd

    def gather_wait(far, near, fwd):
        near.wait_recv()
        for c in fwd:
            c.wait_recv()
        far[-2].wait_recv()
        far[-1].wait_recv()

    far_x, near_x = gather_start(xg, 0, c_x)

    c_tog.wait()
    c_frg.wait()
    tpad = jnp.zeros((KPAD, 384), F32)
    tmat[...] = tpad.astype(BF16)
    ft[...] = tpad.astype(BF16)
    tmat[0:COEFS, 0:grid_pts] = tog[...].astype(BF16)
    frg_pad = jnp.concatenate([jnp.zeros((1, grid_pts), F32), frg[...]], axis=0)
    ft[0:COEFS, 0:grid_pts] = frg_pad.astype(BF16)
    for src, dst in ((tmat, tt), (ft, fmat)):
        wide = jnp.concatenate([src[...].astype(F32) * 0.5, jnp.zeros((128 - KPAD, 384), F32)], axis=0)
        for j in range(3):
            tr = wide[:, 128 * j:128 * (j + 1)].T
            rows = min(128, pp - 128 * j)
            dst[128 * j:128 * j + rows, :] = tr[0:rows, 0:KPAD].astype(BF16)
    c_up.wait()
    c_gate.wait()
    c_down.wait()
    for l in range(5):
        upt[l] = up[l].astype(F32).T.astype(BF16)
        downt[l] = down[l].astype(F32).T.astype(BF16)
    gatet[...] = gate[...].astype(F32).T.astype(BF16)
    ya[...] = jnp.zeros_like(ya)
    yb[...] = jnp.zeros_like(yb)
    for c in gsend:
        c.wait_recv()
    gain_full = placed + gain_all[0] + gain_all[1] + gain_all[2]
    for l in range(5):
        gcol[l] = jnp.broadcast_to(gain_full[l:l + 1, :], (ch, ch)).T

    sums = [jnp.zeros((cl, nat), F32)]

    def square_step(blocks, k0, k1):
        for k in range(max(k0, 1), k1):
            for i in blocks:
                v = xg[k, blk(i), :].astype(F32)
                sums[0] = sums[0] + v * v

    fwd_x = gather_finish(far_x, near_x, xg, 0, square_step)
    fwd_x[-1].wait_recv()
    square_step((t2, t3), *ksplit[2])
    far_x[-2].wait_recv()
    far_x[-1].wait_recv()
    square_step((t2, t3), *ksplit[3])
    for c in far_x:
        c.wait_send()
    c_g.wait()
    far_g, near_g = gather_start(gg, 10)

    x0 = xg[0].astype(F32)
    mean_s = jnp.sum(x0, axis=0, keepdims=True) / ch
    cent = x0 - mean_s
    inv_s = lax.rsqrt(jnp.sum(cent * cent, axis=0, keepdims=True) / ch + NORM_EPS)
    hat_s = cent * inv_s
    inv_v = lax.rsqrt(jnp.sum(sums[0], axis=0, keepdims=True) / (ch * (COEFS - 1)) + NORM_EPS)
    xn[0] = (hat_s * gcol[0]).astype(BF16)
    for k in range(1, COEFS):
        xn[k] = (xg[k].astype(F32) * inv_v * gcol[degree_of(k)]).astype(BF16)

    def by_degree(lhs_of, get, lo=0, hi=COEFS):
        for l in range(5):
            k = max(l * l, lo)
            k1 = min((l + 1) * (l + 1), hi)
            while k < k1:
                n = min(2, k1 - k)
                r = rows_dot(lhs_of(l), get(k) if n == 1 else jnp.concatenate([get(k), get(k + 1)], axis=1))
                for j in range(n):
                    yield k + j, r[:, nat * j:nat * (j + 1)]
                k += n

    def over_degree(a_of, b_of, l):
        ks = range(l * l, (l + 1) * (l + 1))
        return lanes_dot(jnp.concatenate([a_of(k) for k in ks], axis=1), jnp.concatenate([b_of(k) for k in ks], axis=1))

    def spread(get, lhs_of):
        for k, r in by_degree(lhs_of, get):
            ya[pl.ds(k, 64, stride=YSTRIDE), :] = r[0:64]
            yb[pl.ds(k, 64, stride=YSTRIDE), :] = r[64:128]

    spread(lambda k: xn[k], lambda l: upt[l])
    a_r = rows_dot(gatet[...], xn[0]).astype(BF16)
    amat[...] = a_r
    a_h = a_r.astype(F32) * 0.5
    mb[0] = (a_h * (1.0 + jnp.tanh(a_h))).astype(BF16)

    def pair(i):
        base = pl.multiple_of(i * YSTRIDE, 8)
        return jnp.concatenate([ya[pl.ds(base, KPAD), :], yb[pl.ds(base, KPAD), :]], axis=1).astype(BF16)

    def put(i, r):
        zs[pl.ds(i, KPAD, stride=136), :] = r[:, 0:128]
        zs[pl.ds(i + 64, KPAD, stride=136), :] = r[:, 128:256]

    def stage_u(p, dst):
        dst[...] = rows_dot(tt[...], pair(p)).astype(BF16)

    def stage_s(p, src, dst):
        h = src[...].astype(F32)
        w = 1.0 + jnp.tanh(h)
        s = h * w
        dst[...] = s.astype(BF16)
        hs[pl.ds(pl.multiple_of(p * pp, 16), pp), :] = w + s * (2.0 - w)

    def stage_z(p, src, lhs):
        put(p, rows_dot(lhs[:, 0:pp], src[...]))

    stage_u(0, gbuf[0])
    stage_u(1, gbuf[1])

    def fwd_body(it, carry):
        for half_step in range(2):
            p = it * UNROLL + 2 * half_step
            now, other = 2 * (half_step % 2), 2 * ((half_step + 1) % 2)
            for j in range(2):
                stage_z(jnp.maximum(p + j - 2, 0), sbuf[other + j], ft)
                stage_u(p + j + 2, gbuf[other + j])
                stage_s(p + j, gbuf[now + j], sbuf[now + j])
        return carry

    lax.fori_loop(0, 48 // UNROLL, fwd_body, 0)
    fwd_g = gather_finish(far_g, near_g, gg, 10)
    lax.fori_loop(48 // UNROLL, 64 // UNROLL, fwd_body, 0)
    stage_z(62, sbuf[2], ft)
    stage_z(63, sbuf[3], ft)

    for k in range(1, COEFS):
        mb[k] = zs[k * 136:k * 136 + 128, :].astype(BF16)
    for k, r in by_degree(lambda l: downt[l], lambda k: mb[k]):
        dpart[k] = r.astype(BF16)

    def scatter_near(part, rb, base):
        cs = []
        for j, b in enumerate((t3, t1)):
            c = remote(part.at[:, blk(b), :], rb.at[j], base + j, {"tp": t1})
            c.start()
            cs.append(c)
        return cs

    near_d = scatter_near(dpart, rb1, 23)

    gather_wait(far_g, near_g, fwd_g)
    spread(lambda k: gg[k], lambda l: down[l])
    dm0 = rows_dot(down[0], gg[0]).astype(BF16).astype(F32)
    a_h = amat[...].astype(F32) * 0.5
    w_a = 1.0 + jnp.tanh(a_h)
    da = (dm0 * (0.5 * w_a * (1.0 + a_h * (2.0 - w_a)))).astype(BF16)

    for l in range(5):
        gdn[l] = over_degree(lambda k: mb[k], lambda k: gg[k], l)
    gdn[5] = lanes_dot(da, xn[0])
    half = 64
    mine = pl.ds(pl.multiple_of(dp * half, half), half)
    theirs = pl.ds(pl.multiple_of(odp * half, half), half)
    ex_dn = remote(gdn.at[:, theirs, :], gdn_rb, 26, {"dp": odp})
    ex_dn.start()

    def stage_g(p, dst):
        dst[...] = rows_dot(fmat[...], pair(p)).astype(BF16)

    def stage_e(p, src, dst):
        gp = hs[pl.ds(pl.multiple_of(p * pp, 16), pp), :]
        dst[...] = (src[...].astype(F32) * gp).astype(BF16)

    stage_g(0, gbuf[0])
    stage_g(1, gbuf[1])

    def bwd_body(it, carry):
        for half_step in range(2):
            p = it * UNROLL + 2 * half_step
            now, other = 2 * (half_step % 2), 2 * ((half_step + 1) % 2)
            for j in range(2):
                stage_z(jnp.maximum(p + j - 2, 0), sbuf[other + j], tmat)
                stage_g(p + j + 2, gbuf[other + j])
                stage_e(p + j, gbuf[now + j], sbuf[now + j])
        return carry

    def keep_dy(lo, n):
        for k in range(COEFS):
            for o in (lo, 64 + lo):
                dyb[k, o:o + n, :] = zs[k * 136 + o:k * 136 + o + n, :].astype(BF16)

    def grad_up(lo, n):
        def dy(k):
            return jnp.concatenate([dyb[k, lo:lo + n, :], dyb[k, 64 + lo:64 + lo + n, :]], axis=0)

        for l in range(5):
            acc = over_degree(dy, lambda k: xn[k], l)
            gup[l, lo:lo + n, :] = acc[0:n]
            gup[l, 64 + lo:64 + lo + n, :] = acc[n:2 * n]

    def rows_of(d, lo):
        return pl.ds(pl.multiple_of(d * half + lo, 16), half - QR if lo else QR)

    mid_steps = (QR + 4) // UNROLL
    lax.fori_loop(0, 4 // UNROLL, bwd_body, 0)
    near_d[0].wait_recv()
    sb[...] = (dpart[:, blk(t2), :].astype(F32) + rb1[0].astype(F32)).astype(BF16)
    far_d = remote(sb, rb2, 25, {"tp": t2})
    far_d.start()
    lax.fori_loop(4 // UNROLL, mid_steps, bwd_body, 0)

    keep_dy(0, QR)
    grad_up(0, QR)
    ex_up0 = remote(gup.at[:, rows_of(odp, 0), :], gup_rb.at[:, 0:QR, :], 33, {"dp": odp})
    ex_dn.wait_recv()
    gfin_dn[:, mine, :] = (gdn[:, mine, :] + gdn_rb[...]).astype(BF16)
    ex_up0.start()
    bk_dn = remote(gfin_dn.at[:, mine, :], gfin_dn.at[:, mine, :], 34, {"dp": odp})
    bk_dn.start()

    lax.fori_loop(mid_steps, 64 // UNROLL, bwd_body, 0)
    stage_z(62, sbuf[2], tmat)
    stage_z(63, sbuf[3], tmat)

    def full_dy(k):
        return jnp.concatenate([dyb[k, 0:QR, :], zs[k * 136 + QR:k * 136 + 64, :].astype(BF16),
                                dyb[k, 64:64 + QR, :], zs[k * 136 + 64 + QR:k * 136 + 128, :].astype(BF16)], axis=0)

    nsplit = ((0, 9), (9, 16), (16, 25))
    near_n = []
    for j, (k0, k1) in enumerate(nsplit):
        for k, r in by_degree(lambda l: up[l], full_dy, k0, k1):
            if k == 0:
                r = r + rows_dot(gate[...], da)
            npart[k] = r.astype(BF16)
        c = remote(npart.at[k0:k1, blk(t3), :], nrb1.at[0, k0:k1], 27 + j, {"tp": t1})
        c.start()
        near_n.append(c)
    near_o = remote(npart.at[:, blk(t1), :], nrb1.at[1], 30, {"tp": t1})
    near_o.start()

    far_n = []

    def far_step(j):
        k0, k1 = nsplit[j]
        near_n[j].wait_recv()
        nsb[k0:k1] = (npart[k0:k1, blk(t2), :].astype(F32) + nrb1[0, k0:k1].astype(F32)).astype(BF16)

    def far_send(j):
        k0, k1 = nsplit[j]
        c = remote(nsb.at[k0:k1], nrb2.at[k0:k1], 41 + j, {"tp": t2})
        c.start()
        far_n.append(c)

    far_step(0)
    keep_dy(QR, half - QR)
    far_send(0)
    grad_up(QR, half - QR)
    far_step(1)
    far_step(2)
    ex_up1 = remote(gup.at[:, rows_of(odp, QR), :], gup_rb.at[:, QR:64, :], 36, {"dp": odp})
    ex_up1.start()
    s3 = jnp.zeros((ch, nat), F32)
    for k in range(COEFS):
        rf = npart[k].astype(F32) * gcol[degree_of(k)]
        if k == 0:
            st0 = jnp.sum(rf, axis=0, keepdims=True)
            st1 = jnp.sum(rf * hat_s, axis=0, keepdims=True)
        else:
            s3 = s3 + rf * xg[k].astype(F32)
        if k == 4:
            far_send(1)
    st2 = jnp.sum(s3, axis=0, keepdims=True)
    st_snd[...] = jnp.concatenate([st0, st1, st2, jnp.zeros((5, nat), F32)], axis=0)
    ex_up0.wait_recv()
    gfin[:, rows_of(dp, 0), :] = (gup[:, rows_of(dp, 0), :] + gup_rb[:, 0:QR, :]).astype(BF16)
    ssend = []
    for j, dev in enumerate((t1, t2, t3)):
        c = remote(st_snd, st_all.at[j], 37 + j, {"tp": dev})
        c.start()
        ssend.append(c)
    far_send(2)
    near_d[1].wait_recv()
    far_d.wait_recv()
    own = dpart[:, blk(t), :].astype(F32) + rb1[1].astype(F32) + rb2[...].astype(F32)
    out_ref[...] = (xg[:, blk(t), :].astype(F32) + own).astype(BF16)
    bk_up0 = remote(gfin.at[:, rows_of(dp, 0), :], gfin.at[:, rows_of(dp, 0), :], 35, {"dp": odp})
    bk_up0.start()

    bk_dn.wait_recv()
    ddown_ref[...] = gfin_dn[0:5]
    dgate_ref[...] = gfin_dn[5].astype(F32).T.astype(BF16)
    ex_up1.wait_recv()
    gfin[:, rows_of(dp, QR), :] = (gup[:, rows_of(dp, QR), :] + gup_rb[:, QR:64, :]).astype(BF16)
    for c in ssend:
        c.wait_recv()
    stat = st_snd[...] + st_all[0] + st_all[1] + st_all[2]
    b0 = stat[0:1] / ch
    b1 = stat[1:2] / ch
    b2 = (inv_v * inv_v * inv_v) * (stat[2:3] / (ch * (COEFS - 1)))
    bk_up1 = remote(gfin.at[:, rows_of(dp, QR), :], gfin.at[:, rows_of(dp, QR), :], 40, {"dp": odp})
    bk_up1.start()
    near_o.wait_recv()
    for j, (k0, k1) in enumerate(nsplit):
        far_n[j].wait_recv()
        for k in range(k0, k1):
            dn = (npart[k, blk(t), :].astype(F32) + nrb1[1, k].astype(F32) + nrb2[k].astype(F32)).astype(BF16).astype(F32)
            dhat = dn * gcol[degree_of(k), blk(t), :]
            xk = xg[k, blk(t), :].astype(F32)
            if k == 0:
                dxk = inv_s * (dhat - b0 - (xk - mean_s) * inv_s * b1)
            else:
                dxk = inv_v * dhat - xk * b2
            dx_ref[k] = (dxk + gg[k, blk(t), :].astype(F32)).astype(BF16)

    bk_up0.wait_recv()
    bk_up1.wait_recv()
    for l in range(5):
        dup_ref[l] = gfin[l].astype(F32).T.astype(BF16)
    for c in far_g + fwd_x + fwd_g + gsend + near_d + near_n + far_n + ssend + [near_x, near_g, near_o, far_d, ex_dn, ex_up0, ex_up1, bk_dn, bk_up0, bk_up1]:
        c.wait_send()


def flush(a, b, c, d, e, oa, ob, oc, od, oe, sem):
    cs = [pltpu.make_async_copy(i, o, sem.at[j]) for j, (i, o) in enumerate(zip((a, b, c, d, e), (oa, ob, oc, od, oe)))]
    for x in cs:
        x.start()
    for x in cs:
        x.wait()


def solution(mesh):
    tp_size = mesh.shape['tp']
    act_spec = P('dp', None, 'tp')
    in_specs = (act_spec, P(None, 'tp'), P(None, None, 'tp'), P(None, 'tp'), P(None, 'tp', None), P(None, None), P(None, None), act_spec)
    out_specs = (act_spec, act_spec, P(None, None, 'tp'), P(None, 'tp'), P(None, 'tp', None))

    def local_step(x_loc, gain_loc, up_loc, gate_loc, down_loc, to_grid, from_grid, grad_loc):
        nat, coefs, cl = x_loc.shape
        ch = cl * tp_size
        grid_pts = to_grid.shape[1]
        pp = -(-grid_pts // 16) * 16
        xt = x_loc.transpose(1, 2, 0)
        gt = grad_loc.transpose(1, 2, 0)
        any_spec = pl.BlockSpec(memory_space=pl.ANY)
        vmem = pl.BlockSpec(memory_space=pltpu.VMEM)
        full = pltpu.VMEM((coefs, ch, nat), BF16)
        blkb = pltpu.VMEM((coefs, cl, nat), BF16)
        sq = lambda n, d: pltpu.VMEM((n, 128, 128), d)
        shapes = (xt.shape, xt.shape, up_loc.shape, gate_loc.shape, down_loc.shape)
        outs = pl.pallas_call(
            functools.partial(kernel, tp_size, grid_pts),
            out_shape=tuple(pltpu.VMEM(sh, BF16) for sh in shapes),
            in_specs=[any_spec] * 8,
            out_specs=[vmem] * 5,
            scratch_shapes=[
                full, full, full, full, full, full, full,
                pltpu.VMEM((66 * YSTRIDE, 128), F32), pltpu.VMEM((66 * YSTRIDE, 128), F32),
                pltpu.VMEM((KPAD * 136, 128), F32), pltpu.VMEM((64 * pp, 256), F32),
                pltpu.VMEM(gain_loc.shape, F32), pltpu.VMEM((8, 128), F32), pltpu.VMEM((3, 8, 128), F32), sq(5, F32),
                sq(5, BF16), pltpu.VMEM((128, 128), BF16), sq(5, BF16), sq(5, BF16), pltpu.VMEM((128, 128), BF16), sq(5, BF16),
                pltpu.VMEM(to_grid.shape, F32), pltpu.VMEM(from_grid.shape[::-1], F32),
                pltpu.VMEM((pp, KPAD), BF16), pltpu.VMEM((KPAD, 384), BF16), pltpu.VMEM((pp, KPAD), BF16), pltpu.VMEM((KPAD, 384), BF16),
                pltpu.VMEM((2, coefs, cl, nat), BF16), blkb, blkb, pltpu.VMEM((2, coefs, cl, nat), BF16), blkb, blkb,
                pltpu.VMEM((8, 128), F32), pltpu.VMEM((3, 8, 128), F32),
                sq(6, F32), pltpu.VMEM((6, 64, 128), F32), sq(5, F32), pltpu.VMEM((5, 64, 128), F32), sq(5, BF16), sq(6, BF16),
                pltpu.VMEM((128, nat), BF16),
                pltpu.VMEM((pp, 256), BF16), pltpu.VMEM((pp, 256), BF16), pltpu.VMEM((pp, 256), BF16), pltpu.VMEM((pp, 256), BF16),
                pltpu.VMEM((pp, 256), BF16), pltpu.VMEM((pp, 256), BF16), pltpu.VMEM((pp, 256), BF16), pltpu.VMEM((pp, 256), BF16),
                pltpu.SemaphoreType.DMA((12,)), pltpu.SemaphoreType.DMA((44,)), pltpu.SemaphoreType.DMA((44,)),
            ],
            compiler_params=pltpu.CompilerParams(collective_id=0, has_side_effects=True, vmem_limit_bytes=60 * 1024 * 1024),
        )(xt, gain_loc, up_loc, gate_loc, down_loc, to_grid, from_grid.T, gt)
        out_t, dx_t, d_up, d_gate, d_down = pl.pallas_call(
            flush,
            out_shape=tuple(jax.ShapeDtypeStruct(sh, BF16) for sh in shapes),
            in_specs=[vmem] * 5,
            out_specs=[any_spec] * 5,
            scratch_shapes=[pltpu.SemaphoreType.DMA((5,))],
        )(*[pltpu.with_memory_space_constraint(o, pltpu.VMEM) for o in outs])
        return out_t.transpose(2, 0, 1), dx_t.transpose(2, 0, 1), d_up, d_gate, d_down

    return jax.shard_map(local_step, mesh=mesh, in_specs=in_specs, out_specs=out_specs, check_vma=False)
```

```python
import functools
import math
import jax
import jax.numpy as jnp
from jax import lax
from jax.experimental import pallas as pl
from jax.experimental.pallas import tpu as pltpu
from jax.sharding import PartitionSpec as P

NORM_EPS = 1e-5
MESH = pl.DeviceIdType.MESH
F32 = jnp.float32
BF16 = jnp.bfloat16
COEFS = 25
KPAD = 32
YSTRIDE = 40
UNROLL = 4
QR = 48


def degree_of(k):
    return math.isqrt(k)


def rows_dot(a, b):
    return lax.dot_general(a, b, (((1,), (0,)), ((), ())), preferred_element_type=F32)


def lanes_dot(a, b):
    return lax.dot_general(a, b, (((1,), (1,)), ((), ())), preferred_element_type=F32)


def kernel(tp_size, grid_pts, x_hbm, gain_hbm, up_hbm, gate_hbm, down_hbm, tog_hbm, frg_hbm, g_hbm,
           out_ref, dx_ref, dup_ref, dgate_ref, ddown_ref,
           xg, gg, xn, mb, dyb, dpart, npart, ya, yb, zs, hs,
           gain_in, gain_snd, gain_all, gcol, up, gate, down, upt, gatet, downt,
           tog, frg, tt, tmat, fmat, ft, rb1, sb, rb2, nrb1, nsb, nrb2,
           st_snd, st_all, gdn, gdn_rb, gup, gup_rb, gfin, gfin_dn, amat, sbuf0, sbuf1, sbuf2, sbuf3, gbuf0, gbuf1, gbuf2, gbuf3,
           loc_sem, snd_sem, rcv_sem):
    sbuf, gbuf = (sbuf0, sbuf1, sbuf2, sbuf3), (gbuf0, gbuf1, gbuf2, gbuf3)
    dp = lax.axis_index("dp")
    t = lax.axis_index("tp")
    core = lax.rem(t, 2)
    t1 = t + 1 - 2 * core
    t2 = lax.rem(t + 2, 4)
    t3 = lax.rem(t1 + 2, 4)
    odp = 1 - dp
    cl = xg.shape[1] // tp_size
    ch = xg.shape[1]
    nat = xg.shape[2]
    pp = tt.shape[0]

    def blk(i):
        return pl.ds(pl.multiple_of(i * cl, cl), cl)

    def local(src, dst, i):
        c = pltpu.make_async_copy(src, dst, loc_sem.at[i])
        c.start()
        return c

    def remote(src, dst, i, dev):
        return pltpu.make_async_remote_copy(src_ref=src, dst_ref=dst, send_sem=snd_sem.at[i], recv_sem=rcv_sem.at[i],
                                            device_id=dev, device_id_type=MESH)

    c_gain = local(gain_hbm, gain_in, 0)
    ksplit = ((0, 8), (8, 15), (15, 22), (22, 25))
    c_x = [local(x_hbm.at[k0:k1], xg.at[k0:k1, blk(t), :], 7 + j) for j, (k0, k1) in enumerate(ksplit)]
    c_tog = local(tog_hbm, tog, 2)
    c_frg = local(frg_hbm, frg, 3)
    c_up = local(up_hbm, up, 4)
    c_gate = local(gate_hbm, gate, 5)
    c_down = local(down_hbm, down, 6)
    c_g = local(g_hbm, gg.at[:, blk(t), :], 1)

    barrier = pltpu.get_barrier_semaphore()
    for dev in ({"tp": t1}, {"tp": t2}, {"tp": t3}, {"dp": odp}):
        pl.semaphore_signal(barrier, inc=1, device_id=dev, device_id_type=MESH)
    c_gain.wait()
    gain_snd[...] = jnp.zeros_like(gain_snd)
    gain_snd[0:5, 0:cl] = gain_in[...]
    placed = pltpu.roll(gain_snd[...], t * cl, 1)
    gain_snd[...] = placed
    pl.semaphore_wait(barrier, 4)
    gsend = []
    for j, dev in enumerate((t1, t2, t3)):
        c = remote(gain_snd, gain_all.at[j], 20 + j, {"tp": dev})
        c.start()
        gsend.append(c)

    def gather_start(dst, base, ready=None):
        far = []
        for j, (k0, k1) in enumerate(ksplit):
            if ready:
                ready[j].wait()
            c = remote(dst.at[k0:k1, blk(t), :], dst.at[k0:k1, blk(t), :], base + j, {"tp": t2})
            c.start()
            far.append(c)
        k0, k1 = ksplit[-1]
        c = remote(dst.at[k0:k1, blk(t), :], dst.at[k0:k1, blk(t), :], base + 8, {"tp": t3})
        c.start()
        far.append(c)
        near = remote(dst.at[:, blk(t), :], dst.at[:, blk(t), :], base + 4, {"tp": t1})
        near.start()
        return far, near

    def gather_finish(far, near, dst, base, step=None):
        fwd = []
        for j, (k0, k1) in enumerate(ksplit[:-1]):
            far[j].wait_recv()
            c = remote(dst.at[k0:k1, blk(t2), :], dst.at[k0:k1, blk(t2), :], base + 5 + j, {"tp": t1})
            c.start()
            fwd.append(c)
            if step and j == 0:
                near.wait_recv()
                step((t, t1), 0, COEFS)
            if step and j > 0:
                fwd[j - 1].wait_recv()
                step((t2, t3), *ksplit[j - 1])
        return fwd

    def gather_wait(far, near, fwd):
        near.wait_recv()
        for c in fwd:
            c.wait_recv()
        far[-2].wait_recv()
        far[-1].wait_recv()

    far_x, near_x = gather_start(xg, 0, c_x)

    c_tog.wait()
    c_frg.wait()
    tpad = jnp.zeros((KPAD, 384), F32)
    tmat[...] = tpad.astype(BF16)
    ft[...] = tpad.astype(BF16)
    tmat[0:COEFS, 0:grid_pts] = tog[...].astype(BF16)
    frg_pad = jnp.concatenate([jnp.zeros((1, grid_pts), F32), frg[...]], axis=0)
    ft[0:COEFS, 0:grid_pts] = frg_pad.astype(BF16)
    for src, dst in ((tmat, tt), (ft, fmat)):
        wide = jnp.concatenate([src[...].astype(F32) * 0.5, jnp.zeros((128 - KPAD, 384), F32)], axis=0)
        for j in range(3):
            tr = wide[:, 128 * j:128 * (j + 1)].T
            rows = min(128, pp - 128 * j)
            dst[128 * j:128 * j + rows, :] = tr[0:rows, 0:KPAD].astype(BF16)
    c_up.wait()
    c_gate.wait()
    c_down.wait()
    for l in range(5):
        upt[l] = up[l].astype(F32).T.astype(BF16)
        downt[l] = down[l].astype(F32).T.astype(BF16)
    gatet[...] = gate[...].astype(F32).T.astype(BF16)
    ya[...] = jnp.zeros_like(ya)
    yb[...] = jnp.zeros_like(yb)
    for c in gsend:
        c.wait_recv()
    gain_full = placed + gain_all[0] + gain_all[1] + gain_all[2]
    for l in range(5):
        gcol[l] = jnp.broadcast_to(gain_full[l:l + 1, :], (ch, ch)).T

    sums = [jnp.zeros((cl, nat), F32)]

    def square_step(blocks, k0, k1):
        for k in range(max(k0, 1), k1):
            for i in blocks:
                v = xg[k, blk(i), :].astype(F32)
                sums[0] = sums[0] + v * v

    fwd_x = gather_finish(far_x, near_x, xg, 0, square_step)
    fwd_x[-1].wait_recv()
    square_step((t2, t3), *ksplit[2])
    far_x[-2].wait_recv()
    far_x[-1].wait_recv()
    square_step((t2, t3), *ksplit[3])
    for c in far_x:
        c.wait_send()
    c_g.wait()
    far_g, near_g = gather_start(gg, 10)

    x0 = xg[0].astype(F32)
    mean_s = jnp.sum(x0, axis=0, keepdims=True) / ch
    cent = x0 - mean_s
    inv_s = lax.rsqrt(jnp.sum(cent * cent, axis=0, keepdims=True) / ch + NORM_EPS)
    hat_s = cent * inv_s
    inv_v = lax.rsqrt(jnp.sum(sums[0], axis=0, keepdims=True) / (ch * (COEFS - 1)) + NORM_EPS)
    xn[0] = (hat_s * gcol[0]).astype(BF16)
    for k in range(1, COEFS):
        xn[k] = (xg[k].astype(F32) * inv_v * gcol[degree_of(k)]).astype(BF16)

    def by_degree(lhs_of, get, lo=0, hi=COEFS):
        for l in range(5):
            k = max(l * l, lo)
            k1 = min((l + 1) * (l + 1), hi)
            while k < k1:
                n = min(2, k1 - k)
                r = rows_dot(lhs_of(l), get(k) if n == 1 else jnp.concatenate([get(k), get(k + 1)], axis=1))
                for j in range(n):
                    yield k + j, r[:, nat * j:nat * (j + 1)]
                k += n

    def over_degree(a_of, b_of, l):
        ks = range(l * l, (l + 1) * (l + 1))
        return lanes_dot(jnp.concatenate([a_of(k) for k in ks], axis=1), jnp.concatenate([b_of(k) for k in ks], axis=1))

    def spread(get, lhs_of):
        for k, r in by_degree(lhs_of, get):
            ya[pl.ds(k, 64, stride=YSTRIDE), :] = r[0:64]
            yb[pl.ds(k, 64, stride=YSTRIDE), :] = r[64:128]

    spread(lambda k: xn[k], lambda l: upt[l])
    a_r = rows_dot(gatet[...], xn[0]).astype(BF16)
    amat[...] = a_r
    a_h = a_r.astype(F32) * 0.5
    mb[0] = (a_h * (1.0 + jnp.tanh(a_h))).astype(BF16)

    def pair(i):
        base = pl.multiple_of(i * YSTRIDE, 8)
        return jnp.concatenate([ya[pl.ds(base, KPAD), :], yb[pl.ds(base, KPAD), :]], axis=1).astype(BF16)

    def put(i, r):
        zs[pl.ds(i, KPAD, stride=136), :] = r[:, 0:128]
        zs[pl.ds(i + 64, KPAD, stride=136), :] = r[:, 128:256]

    def stage_u(p, dst):
        dst[...] = rows_dot(tt[...], pair(p)).astype(BF16)

    def stage_s(p, src, dst):
        h = src[...].astype(F32)
        w = 1.0 + jnp.tanh(h)
        s = h * w
        dst[...] = s.astype(BF16)
        hs[pl.ds(pl.multiple_of(p * pp, 16), pp), :] = w + s * (2.0 - w)

    def stage_z(p, src, lhs):
        put(p, rows_dot(lhs[:, 0:pp], src[...]))

    stage_u(0, gbuf[0])
    stage_u(1, gbuf[1])

    def fwd_body(it, carry):
        for half_step in range(2):
            p = it * UNROLL + 2 * half_step
            now, other = 2 * (half_step % 2), 2 * ((half_step + 1) % 2)
            for j in range(2):
                stage_z(jnp.maximum(p + j - 2, 0), sbuf[other + j], ft)
                stage_u(p + j + 2, gbuf[other + j])
                stage_s(p + j, gbuf[now + j], sbuf[now + j])
        return carry

    lax.fori_loop(0, 48 // UNROLL, fwd_body, 0)
    fwd_g = gather_finish(far_g, near_g, gg, 10)
    lax.fori_loop(48 // UNROLL, 64 // UNROLL, fwd_body, 0)
    gather_wait(far_g, near_g, fwd_g)
    stage_z(62, sbuf[2], ft)
    stage_z(63, sbuf[3], ft)

    def stage_g(p, dst):
        dst[...] = rows_dot(fmat[...], pair(p)).astype(BF16)

    spread(lambda k: gg[k], lambda l: down[l])
    dm0 = rows_dot(down[0], gg[0]).astype(BF16).astype(F32)
    a_h = amat[...].astype(F32) * 0.5
    w_a = 1.0 + jnp.tanh(a_h)
    da = (dm0 * (0.5 * w_a * (1.0 + a_h * (2.0 - w_a)))).astype(BF16)

    stage_g(0, gbuf[0])
    stage_g(1, gbuf[1])

    for k in range(1, COEFS):
        mb[k] = zs[k * 136:k * 136 + 128, :].astype(BF16)
    for k, r in by_degree(lambda l: downt[l], lambda k: mb[k]):
        dpart[k] = r.astype(BF16)

    def scatter_near(part, rb, base):
        cs = []
        for j, b in enumerate((t3, t1)):
            c = remote(part.at[:, blk(b), :], rb.at[j], base + j, {"tp": t1})
            c.start()
            cs.append(c)
        return cs

    near_d = scatter_near(dpart, rb1, 23)

    for l in range(5):
        gdn[l] = over_degree(lambda k: mb[k], lambda k: gg[k], l)
    gdn[5] = lanes_dot(da, xn[0])
    half = 64
    mine = pl.ds(pl.multiple_of(dp * half, half), half)
    theirs = pl.ds(pl.multiple_of(odp * half, half), half)
    ex_dn = remote(gdn.at[:, theirs, :], gdn_rb, 26, {"dp": odp})
    ex_dn.start()

    def stage_e(p, src, dst):
        gp = hs[pl.ds(pl.multiple_of(p * pp, 16), pp), :]
        dst[...] = (src[...].astype(F32) * gp).astype(BF16)


    def bwd_body(it, carry):
        for half_step in range(2):
            p = it * UNROLL + 2 * half_step
            now, other = 2 * (half_step % 2), 2 * ((half_step + 1) % 2)
            for j in range(2):
                stage_z(jnp.maximum(p + j - 2, 0), sbuf[other + j], tmat)
                stage_g(p + j + 2, gbuf[other + j])
                stage_e(p + j, gbuf[now + j], sbuf[now + j])
        return carry

    def keep_dy(lo, n):
        for k in range(COEFS):
            for o in (lo, 64 + lo):
                dyb[k, o:o + n, :] = zs[k * 136 + o:k * 136 + o + n, :].astype(BF16)

    def grad_up(lo, n):
        def dy(k):
            return jnp.concatenate([dyb[k, lo:lo + n, :], dyb[k, 64 + lo:64 + lo + n, :]], axis=0)

        for l in range(5):
            acc = over_degree(dy, lambda k: xn[k], l)
            gup[l, lo:lo + n, :] = acc[0:n]
            gup[l, 64 + lo:64 + lo + n, :] = acc[n:2 * n]

    def rows_of(d, lo):
        return pl.ds(pl.multiple_of(d * half + lo, 16), half - QR if lo else QR)

    mid_steps = (QR + 4) // UNROLL
    lax.fori_loop(0, 12 // UNROLL, bwd_body, 0)
    near_d[0].wait_recv()
    sb[...] = (dpart[:, blk(t2), :].astype(F32) + rb1[0].astype(F32)).astype(BF16)
    far_d = remote(sb, rb2, 25, {"tp": t2})
    far_d.start()
    lax.fori_loop(12 // UNROLL, mid_steps, bwd_body, 0)

    keep_dy(0, QR)
    grad_up(0, QR)
    ex_up0 = remote(gup.at[:, rows_of(odp, 0), :], gup_rb.at[:, 0:QR, :], 33, {"dp": odp})
    ex_dn.wait_recv()
    gfin_dn[:, mine, :] = (gdn[:, mine, :] + gdn_rb[...]).astype(BF16)
    ex_up0.start()
    bk_dn = remote(gfin_dn.at[:, mine, :], gfin_dn.at[:, mine, :], 34, {"dp": odp})
    bk_dn.start()

    lax.fori_loop(mid_steps, 64 // UNROLL, bwd_body, 0)
    stage_z(62, sbuf[2], tmat)
    stage_z(63, sbuf[3], tmat)

    def full_dy(k):
        return jnp.concatenate([dyb[k, 0:QR, :], zs[k * 136 + QR:k * 136 + 64, :].astype(BF16),
                                dyb[k, 64:64 + QR, :], zs[k * 136 + 64 + QR:k * 136 + 128, :].astype(BF16)], axis=0)

    nsplit = ((0, 6), (6, 16), (16, 25))
    near_n = []
    for j, (k0, k1) in enumerate(nsplit):
        for k, r in by_degree(lambda l: up[l], full_dy, k0, k1):
            if k == 0:
                r = r + rows_dot(gate[...], da)
            npart[k] = r.astype(BF16)
        c = remote(npart.at[k0:k1, blk(t3), :], nrb1.at[0, k0:k1], 27 + j, {"tp": t1})
        c.start()
        near_n.append(c)
    near_o = remote(npart.at[:, blk(t1), :], nrb1.at[1], 30, {"tp": t1})
    near_o.start()

    far_n = []

    def far_step(j):
        k0, k1 = nsplit[j]
        near_n[j].wait_recv()
        nsb[k0:k1] = (npart[k0:k1, blk(t2), :].astype(F32) + nrb1[0, k0:k1].astype(F32)).astype(BF16)

    def far_send(j):
        k0, k1 = nsplit[j]
        c = remote(nsb.at[k0:k1], nrb2.at[k0:k1], 41 + j, {"tp": t2})
        c.start()
        far_n.append(c)

    far_step(0)
    keep_dy(QR, half - QR)
    far_send(0)
    far_step(1)
    grad_up(QR, half - QR)
    far_send(1)
    far_step(2)
    ex_up1 = remote(gup.at[:, rows_of(odp, QR), :], gup_rb.at[:, QR:64, :], 36, {"dp": odp})
    ex_up1.start()
    s3 = jnp.zeros((ch, nat), F32)
    for k in range(COEFS):
        rf = npart[k].astype(F32) * gcol[degree_of(k)]
        if k == 0:
            st0 = jnp.sum(rf, axis=0, keepdims=True)
            st1 = jnp.sum(rf * hat_s, axis=0, keepdims=True)
        else:
            s3 = s3 + rf * xg[k].astype(F32)
    st2 = jnp.sum(s3, axis=0, keepdims=True)
    st_snd[...] = jnp.concatenate([st0, st1, st2, jnp.zeros((5, nat), F32)], axis=0)
    ex_up0.wait_recv()
    gfin[:, rows_of(dp, 0), :] = (gup[:, rows_of(dp, 0), :] + gup_rb[:, 0:QR, :]).astype(BF16)
    ssend = []
    for j, dev in enumerate((t1, t2, t3)):
        c = remote(st_snd, st_all.at[j], 37 + j, {"tp": dev})
        c.start()
        ssend.append(c)
    far_send(2)
    near_d[1].wait_recv()
    far_d.wait_recv()
    own = dpart[:, blk(t), :].astype(F32) + rb1[1].astype(F32) + rb2[...].astype(F32)
    out_ref[...] = (xg[:, blk(t), :].astype(F32) + own).astype(BF16)
    bk_up0 = remote(gfin.at[:, rows_of(dp, 0), :], gfin.at[:, rows_of(dp, 0), :], 35, {"dp": odp})
    bk_up0.start()

    bk_dn.wait_recv()
    ddown_ref[...] = gfin_dn[0:5]
    dgate_ref[...] = gfin_dn[5].astype(F32).T.astype(BF16)
    ex_up1.wait_recv()
    gfin[:, rows_of(dp, QR), :] = (gup[:, rows_of(dp, QR), :] + gup_rb[:, QR:64, :]).astype(BF16)
    for c in ssend:
        c.wait_recv()
    stat = st_snd[...] + st_all[0] + st_all[1] + st_all[2]
    b0 = stat[0:1] / ch
    b1 = stat[1:2] / ch
    b2 = (inv_v * inv_v * inv_v) * (stat[2:3] / (ch * (COEFS - 1)))
    bk_up1 = remote(gfin.at[:, rows_of(dp, QR), :], gfin.at[:, rows_of(dp, QR), :], 40, {"dp": odp})
    bk_up1.start()
    near_o.wait_recv()
    for j, (k0, k1) in enumerate(nsplit):
        far_n[j].wait_recv()
        for k in range(k0, k1):
            dn = (npart[k, blk(t), :].astype(F32) + nrb1[1, k].astype(F32) + nrb2[k].astype(F32)).astype(BF16).astype(F32)
            dhat = dn * gcol[degree_of(k), blk(t), :]
            xk = xg[k, blk(t), :].astype(F32)
            if k == 0:
                dxk = inv_s * (dhat - b0 - (xk - mean_s) * inv_s * b1)
            else:
                dxk = inv_v * dhat - xk * b2
            dx_ref[k] = (dxk + gg[k, blk(t), :].astype(F32)).astype(BF16)

    bk_up0.wait_recv()
    bk_up1.wait_recv()
    for l in range(5):
        dup_ref[l] = gfin[l].astype(F32).T.astype(BF16)
    for c in far_g + fwd_x + fwd_g + gsend + near_d + near_n + far_n + ssend + [near_x, near_g, near_o, far_d, ex_dn, ex_up0, ex_up1, bk_dn, bk_up0, bk_up1]:
        c.wait_send()


def flush(a, b, c, d, e, oa, ob, oc, od, oe, sem):
    cs = [pltpu.make_async_copy(i, o, sem.at[j]) for j, (i, o) in enumerate(zip((a, b, c, d, e), (oa, ob, oc, od, oe)))]
    for x in cs:
        x.start()
    for x in cs:
        x.wait()


def solution(mesh):
    tp_size = mesh.shape['tp']
    act_spec = P('dp', None, 'tp')
    in_specs = (act_spec, P(None, 'tp'), P(None, None, 'tp'), P(None, 'tp'), P(None, 'tp', None), P(None, None), P(None, None), act_spec)
    out_specs = (act_spec, act_spec, P(None, None, 'tp'), P(None, 'tp'), P(None, 'tp', None))

    def local_step(x_loc, gain_loc, up_loc, gate_loc, down_loc, to_grid, from_grid, grad_loc):
        nat, coefs, cl = x_loc.shape
        ch = cl * tp_size
        grid_pts = to_grid.shape[1]
        pp = -(-grid_pts // 16) * 16
        xt = x_loc.transpose(1, 2, 0)
        gt = grad_loc.transpose(1, 2, 0)
        any_spec = pl.BlockSpec(memory_space=pl.ANY)
        vmem = pl.BlockSpec(memory_space=pltpu.VMEM)
        full = pltpu.VMEM((coefs, ch, nat), BF16)
        blkb = pltpu.VMEM((coefs, cl, nat), BF16)
        sq = lambda n, d: pltpu.VMEM((n, 128, 128), d)
        shapes = (xt.shape, xt.shape, up_loc.shape, gate_loc.shape, down_loc.shape)
        outs = pl.pallas_call(
            functools.partial(kernel, tp_size, grid_pts),
            out_shape=tuple(pltpu.VMEM(sh, BF16) for sh in shapes),
            in_specs=[any_spec] * 8,
            out_specs=[vmem] * 5,
            scratch_shapes=[
                full, full, full, full, full, full, full,
                pltpu.VMEM((66 * YSTRIDE, 128), F32), pltpu.VMEM((66 * YSTRIDE, 128), F32),
                pltpu.VMEM((KPAD * 136, 128), F32), pltpu.VMEM((64 * pp, 256), F32),
                pltpu.VMEM(gain_loc.shape, F32), pltpu.VMEM((8, 128), F32), pltpu.VMEM((3, 8, 128), F32), sq(5, F32),
                sq(5, BF16), pltpu.VMEM((128, 128), BF16), sq(5, BF16), sq(5, BF16), pltpu.VMEM((128, 128), BF16), sq(5, BF16),
                pltpu.VMEM(to_grid.shape, F32), pltpu.VMEM(from_grid.shape[::-1], F32),
                pltpu.VMEM((pp, KPAD), BF16), pltpu.VMEM((KPAD, 384), BF16), pltpu.VMEM((pp, KPAD), BF16), pltpu.VMEM((KPAD, 384), BF16),
                pltpu.VMEM((2, coefs, cl, nat), BF16), blkb, blkb, pltpu.VMEM((2, coefs, cl, nat), BF16), blkb, blkb,
                pltpu.VMEM((8, 128), F32), pltpu.VMEM((3, 8, 128), F32),
                sq(6, F32), pltpu.VMEM((6, 64, 128), F32), sq(5, F32), pltpu.VMEM((5, 64, 128), F32), sq(5, BF16), sq(6, BF16),
                pltpu.VMEM((128, nat), BF16),
                pltpu.VMEM((pp, 256), BF16), pltpu.VMEM((pp, 256), BF16), pltpu.VMEM((pp, 256), BF16), pltpu.VMEM((pp, 256), BF16),
                pltpu.VMEM((pp, 256), BF16), pltpu.VMEM((pp, 256), BF16), pltpu.VMEM((pp, 256), BF16), pltpu.VMEM((pp, 256), BF16),
                pltpu.SemaphoreType.DMA((12,)), pltpu.SemaphoreType.DMA((46,)), pltpu.SemaphoreType.DMA((46,)),
            ],
            compiler_params=pltpu.CompilerParams(collective_id=0, has_side_effects=True, vmem_limit_bytes=60 * 1024 * 1024),
        )(xt, gain_loc, up_loc, gate_loc, down_loc, to_grid, from_grid.T, gt)
        out_t, dx_t, d_up, d_gate, d_down = pl.pallas_call(
            flush,
            out_shape=tuple(jax.ShapeDtypeStruct(sh, BF16) for sh in shapes),
            in_specs=[vmem] * 5,
            out_specs=[any_spec] * 5,
            scratch_shapes=[pltpu.SemaphoreType.DMA((5,))],
        )(*[pltpu.with_memory_space_constraint(o, pltpu.VMEM) for o in outs])
        return out_t.transpose(2, 0, 1), dx_t.transpose(2, 0, 1), d_up, d_gate, d_down

    return jax.shard_map(local_step, mesh=mesh, in_specs=in_specs, out_specs=out_specs, check_vma=False)
```

```python
import functools
import math
import jax
import jax.numpy as jnp
from jax import lax
from jax.experimental import pallas as pl
from jax.experimental.pallas import tpu as pltpu
from jax.sharding import PartitionSpec as P

NORM_EPS = 1e-5
MESH = pl.DeviceIdType.MESH
F32 = jnp.float32
BF16 = jnp.bfloat16
COEFS = 25
KPAD = 32
YSTRIDE = 40
UNROLL = 4
QR = 48


def degree_of(k):
    return math.isqrt(k)


def rows_dot(a, b):
    return lax.dot_general(a, b, (((1,), (0,)), ((), ())), preferred_element_type=F32)


def lanes_dot(a, b):
    return lax.dot_general(a, b, (((1,), (1,)), ((), ())), preferred_element_type=F32)


def kernel(tp_size, grid_pts, x_hbm, gain_hbm, up_hbm, gate_hbm, down_hbm, tog_hbm, frg_hbm, g_hbm,
           out_ref, dx_ref, dup_ref, dgate_ref, ddown_ref,
           xg, gg, xn, mb, dyb, dpart, npart, ya, yb, zs, hs,
           gain_in, gain_snd, gain_all, gcol, up, gate, down, upt, gatet, downt,
           tog, frg, tt, tmat, fmat, ft, rb1, sb, rb2, nrb1, nsb, nrb2,
           st_snd, st_all, gdn, gdn_rb, gup, gup_rb, gfin, gfin_dn, amat, sbuf0, sbuf1, sbuf2, sbuf3, gbuf0, gbuf1, gbuf2, gbuf3,
           loc_sem, snd_sem, rcv_sem):
    sbuf, gbuf = (sbuf0, sbuf1, sbuf2, sbuf3), (gbuf0, gbuf1, gbuf2, gbuf3)
    dp = lax.axis_index("dp")
    t = lax.axis_index("tp")
    core = lax.rem(t, 2)
    t1 = t + 1 - 2 * core
    t2 = lax.rem(t + 2, 4)
    t3 = lax.rem(t1 + 2, 4)
    odp = 1 - dp
    cl = xg.shape[1] // tp_size
    ch = xg.shape[1]
    nat = xg.shape[2]
    pp = tt.shape[0]

    def blk(i):
        return pl.ds(pl.multiple_of(i * cl, cl), cl)

    def local(src, dst, i):
        c = pltpu.make_async_copy(src, dst, loc_sem.at[i])
        c.start()
        return c

    def remote(src, dst, i, dev):
        return pltpu.make_async_remote_copy(src_ref=src, dst_ref=dst, send_sem=snd_sem.at[i], recv_sem=rcv_sem.at[i],
                                            device_id=dev, device_id_type=MESH)

    c_gain = local(gain_hbm, gain_in, 0)
    ksplit = ((0, 8), (8, 15), (15, 22), (22, 25))
    c_x = [local(x_hbm.at[k0:k1], xg.at[k0:k1, blk(t), :], 7 + j) for j, (k0, k1) in enumerate(ksplit)]
    c_tog = local(tog_hbm, tog, 2)
    c_frg = local(frg_hbm, frg, 3)
    c_up = local(up_hbm, up, 4)
    c_gate = local(gate_hbm, gate, 5)
    c_down = local(down_hbm, down, 6)
    c_g = local(g_hbm, gg.at[:, blk(t), :], 1)

    barrier = pltpu.get_barrier_semaphore()
    for dev in ({"tp": t1}, {"tp": t2}, {"tp": t3}, {"dp": odp}):
        pl.semaphore_signal(barrier, inc=1, device_id=dev, device_id_type=MESH)
    c_gain.wait()
    gain_snd[...] = jnp.zeros_like(gain_snd)
    gain_snd[0:5, 0:cl] = gain_in[...]
    placed = pltpu.roll(gain_snd[...], t * cl, 1)
    gain_snd[...] = placed
    pl.semaphore_wait(barrier, 4)
    gsend = []
    for j, dev in enumerate((t1, t2, t3)):
        c = remote(gain_snd, gain_all.at[j], 20 + j, {"tp": dev})
        c.start()
        gsend.append(c)

    def gather_start(dst, base, ready=None):
        far = []
        for j, (k0, k1) in enumerate(ksplit):
            if ready:
                ready[j].wait()
            c = remote(dst.at[k0:k1, blk(t), :], dst.at[k0:k1, blk(t), :], base + j, {"tp": t2})
            c.start()
            far.append(c)
        k0, k1 = ksplit[-1]
        c = remote(dst.at[k0:k1, blk(t), :], dst.at[k0:k1, blk(t), :], base + 8, {"tp": t3})
        c.start()
        far.append(c)
        near = remote(dst.at[:, blk(t), :], dst.at[:, blk(t), :], base + 4, {"tp": t1})
        near.start()
        return far, near

    def gather_finish(far, near, dst, base, step=None):
        fwd = []
        for j, (k0, k1) in enumerate(ksplit[:-1]):
            far[j].wait_recv()
            c = remote(dst.at[k0:k1, blk(t2), :], dst.at[k0:k1, blk(t2), :], base + 5 + j, {"tp": t1})
            c.start()
            fwd.append(c)
            if step and j == 0:
                near.wait_recv()
                step((t, t1), 0, COEFS)
            if step and j > 0:
                fwd[j - 1].wait_recv()
                step((t2, t3), *ksplit[j - 1])
        return fwd

    def gather_wait(far, near, fwd):
        near.wait_recv()
        for c in fwd:
            c.wait_recv()
        far[-2].wait_recv()
        far[-1].wait_recv()

    far_x, near_x = gather_start(xg, 0, c_x)

    c_tog.wait()
    c_frg.wait()
    tpad = jnp.zeros((KPAD, 384), F32)
    tmat[...] = tpad.astype(BF16)
    ft[...] = tpad.astype(BF16)
    tmat[0:COEFS, 0:grid_pts] = tog[...].astype(BF16)
    frg_pad = jnp.concatenate([jnp.zeros((1, grid_pts), F32), frg[...]], axis=0)
    ft[0:COEFS, 0:grid_pts] = frg_pad.astype(BF16)
    for src, dst in ((tmat, tt), (ft, fmat)):
        wide = jnp.concatenate([src[...].astype(F32) * 0.5, jnp.zeros((128 - KPAD, 384), F32)], axis=0)
        for j in range(3):
            tr = wide[:, 128 * j:128 * (j + 1)].T
            rows = min(128, pp - 128 * j)
            dst[128 * j:128 * j + rows, :] = tr[0:rows, 0:KPAD].astype(BF16)
    c_up.wait()
    c_gate.wait()
    c_down.wait()
    for l in range(5):
        upt[l] = up[l].astype(F32).T.astype(BF16)
        downt[l] = down[l].astype(F32).T.astype(BF16)
    gatet[...] = gate[...].astype(F32).T.astype(BF16)
    ya[...] = jnp.zeros_like(ya)
    yb[...] = jnp.zeros_like(yb)
    for c in gsend:
        c.wait_recv()
    gain_full = placed + gain_all[0] + gain_all[1] + gain_all[2]
    for l in range(5):
        gcol[l] = jnp.broadcast_to(gain_full[l:l + 1, :], (ch, ch)).T

    sums = [jnp.zeros((cl, nat), F32)]

    def square_step(blocks, k0, k1):
        for k in range(max(k0, 1), k1):
            for i in blocks:
                v = xg[k, blk(i), :].astype(F32)
                sums[0] = sums[0] + v * v

    fwd_x = gather_finish(far_x, near_x, xg, 0, square_step)
    fwd_x[-1].wait_recv()
    square_step((t2, t3), *ksplit[2])
    far_x[-2].wait_recv()
    far_x[-1].wait_recv()
    square_step((t2, t3), *ksplit[3])
    for c in far_x:
        c.wait_send()
    c_g.wait()
    far_g, near_g = gather_start(gg, 10)

    x0 = xg[0].astype(F32)
    mean_s = jnp.sum(x0, axis=0, keepdims=True) / ch
    cent = x0 - mean_s
    inv_s = lax.rsqrt(jnp.sum(cent * cent, axis=0, keepdims=True) / ch + NORM_EPS)
    hat_s = cent * inv_s
    inv_v = lax.rsqrt(jnp.sum(sums[0], axis=0, keepdims=True) / (ch * (COEFS - 1)) + NORM_EPS)
    xn[0] = (hat_s * gcol[0]).astype(BF16)
    for k in range(1, COEFS):
        xn[k] = (xg[k].astype(F32) * inv_v * gcol[degree_of(k)]).astype(BF16)

    def by_degree(lhs_of, get, lo=0, hi=COEFS):
        for l in range(5):
            k = max(l * l, lo)
            k1 = min((l + 1) * (l + 1), hi)
            while k < k1:
                n = min(2, k1 - k)
                r = rows_dot(lhs_of(l), get(k) if n == 1 else jnp.concatenate([get(k), get(k + 1)], axis=1))
                for j in range(n):
                    yield k + j, r[:, nat * j:nat * (j + 1)]
                k += n

    def over_degree(a_of, b_of, l):
        ks = range(l * l, (l + 1) * (l + 1))
        return lanes_dot(jnp.concatenate([a_of(k) for k in ks], axis=1), jnp.concatenate([b_of(k) for k in ks], axis=1))

    def spread(get, lhs_of):
        for k, r in by_degree(lhs_of, get):
            ya[pl.ds(k, 64, stride=YSTRIDE), :] = r[0:64]
            yb[pl.ds(k, 64, stride=YSTRIDE), :] = r[64:128]

    spread(lambda k: xn[k], lambda l: upt[l])
    a_r = rows_dot(gatet[...], xn[0]).astype(BF16)
    amat[...] = a_r
    a_h = a_r.astype(F32) * 0.5
    mb[0] = (a_h * (1.0 + jnp.tanh(a_h))).astype(BF16)

    def pair(i):
        base = pl.multiple_of(i * YSTRIDE, 8)
        return jnp.concatenate([ya[pl.ds(base, KPAD), :], yb[pl.ds(base, KPAD), :]], axis=1).astype(BF16)

    def put(i, r):
        zs[pl.ds(i, KPAD, stride=136), :] = r[:, 0:128]
        zs[pl.ds(i + 64, KPAD, stride=136), :] = r[:, 128:256]

    def stage_u(p, dst):
        dst[...] = rows_dot(tt[...], pair(p)).astype(BF16)

    def stage_s(p, src, dst):
        h = src[...].astype(F32)
        w = 1.0 + jnp.tanh(h)
        s = h * w
        dst[...] = s.astype(BF16)
        hs[pl.ds(pl.multiple_of(p * pp, 16), pp), :] = w + s * (2.0 - w)

    def stage_z(p, src, lhs):
        put(p, rows_dot(lhs[:, 0:pp], src[...]))

    stage_u(0, gbuf[0])
    stage_u(1, gbuf[1])

    def fwd_body(it, carry):
        for half_step in range(2):
            p = it * UNROLL + 2 * half_step
            now, other = 2 * (half_step % 2), 2 * ((half_step + 1) % 2)
            for j in range(2):
                stage_z(jnp.maximum(p + j - 2, 0), sbuf[other + j], ft)
                stage_u(p + j + 2, gbuf[other + j])
                stage_s(p + j, gbuf[now + j], sbuf[now + j])
        return carry

    lax.fori_loop(0, 48 // UNROLL, fwd_body, 0)
    fwd_g = gather_finish(far_g, near_g, gg, 10)
    lax.fori_loop(48 // UNROLL, 64 // UNROLL, fwd_body, 0)
    gather_wait(far_g, near_g, fwd_g)
    stage_z(62, sbuf[2], ft)
    stage_z(63, sbuf[3], ft)

    def stage_g(p, dst):
        dst[...] = rows_dot(fmat[...], pair(p)).astype(BF16)

    spread(lambda k: gg[k], lambda l: down[l])
    dm0 = rows_dot(down[0], gg[0]).astype(BF16).astype(F32)
    a_h = amat[...].astype(F32) * 0.5
    w_a = 1.0 + jnp.tanh(a_h)
    da = (dm0 * (0.5 * w_a * (1.0 + a_h * (2.0 - w_a)))).astype(BF16)

    stage_g(0, gbuf[0])
    stage_g(1, gbuf[1])

    for k in range(1, COEFS):
        mb[k] = zs[k * 136:k * 136 + 128, :].astype(BF16)
    for k, r in by_degree(lambda l: downt[l], lambda k: mb[k]):
        dpart[k] = r.astype(BF16)

    def scatter_near(part, rb, base):
        cs = []
        for j, b in enumerate((t3, t1)):
            c = remote(part.at[:, blk(b), :], rb.at[j], base + j, {"tp": t1})
            c.start()
            cs.append(c)
        return cs

    near_d = scatter_near(dpart, rb1, 23)

    for l in range(5):
        gdn[l] = over_degree(lambda k: mb[k], lambda k: gg[k], l)
    gdn[5] = lanes_dot(da, xn[0])
    half = 64
    mine = pl.ds(pl.multiple_of(dp * half, half), half)
    theirs = pl.ds(pl.multiple_of(odp * half, half), half)
    ex_dn = remote(gdn.at[:, theirs, :], gdn_rb, 26, {"dp": odp})
    ex_dn.start()

    def stage_e(p, src, dst):
        gp = hs[pl.ds(pl.multiple_of(p * pp, 16), pp), :]
        dst[...] = (src[...].astype(F32) * gp).astype(BF16)


    def bwd_body(it, carry):
        for half_step in range(2):
            p = it * UNROLL + 2 * half_step
            now, other = 2 * (half_step % 2), 2 * ((half_step + 1) % 2)
            for j in range(2):
                stage_z(jnp.maximum(p + j - 2, 0), sbuf[other + j], tmat)
                stage_g(p + j + 2, gbuf[other + j])
                stage_e(p + j, gbuf[now + j], sbuf[now + j])
        return carry

    def keep_dy(lo, n):
        for k in range(COEFS):
            for o in (lo, 64 + lo):
                dyb[k, o:o + n, :] = zs[k * 136 + o:k * 136 + o + n, :].astype(BF16)

    def grad_up(lo, n):
        def dy(k):
            return jnp.concatenate([dyb[k, lo:lo + n, :], dyb[k, 64 + lo:64 + lo + n, :]], axis=0)

        for l in range(5):
            acc = over_degree(dy, lambda k: xn[k], l)
            gup[l, lo:lo + n, :] = acc[0:n]
            gup[l, 64 + lo:64 + lo + n, :] = acc[n:2 * n]

    def rows_of(d, lo):
        return pl.ds(pl.multiple_of(d * half + lo, 16), half - QR if lo else QR)

    mid_steps = (QR + 4) // UNROLL
    lax.fori_loop(0, 8 // UNROLL, bwd_body, 0)
    near_d[0].wait_recv()
    sb[...] = (dpart[:, blk(t2), :].astype(F32) + rb1[0].astype(F32)).astype(BF16)
    far_d = remote(sb, rb2, 25, {"tp": t2})
    far_d.start()
    lax.fori_loop(8 // UNROLL, mid_steps, bwd_body, 0)

    keep_dy(0, QR)
    grad_up(0, QR)
    ex_up0 = remote(gup.at[:, rows_of(odp, 0), :], gup_rb.at[:, 0:QR, :], 33, {"dp": odp})
    ex_dn.wait_recv()
    gfin_dn[:, mine, :] = (gdn[:, mine, :] + gdn_rb[...]).astype(BF16)
    ex_up0.start()
    bk_dn = remote(gfin_dn.at[:, mine, :], gfin_dn.at[:, mine, :], 34, {"dp": odp})
    bk_dn.start()

    lax.fori_loop(mid_steps, 64 // UNROLL, bwd_body, 0)
    stage_z(62, sbuf[2], tmat)
    stage_z(63, sbuf[3], tmat)

    def full_dy(k):
        return jnp.concatenate([dyb[k, 0:QR, :], zs[k * 136 + QR:k * 136 + 64, :].astype(BF16),
                                dyb[k, 64:64 + QR, :], zs[k * 136 + 64 + QR:k * 136 + 128, :].astype(BF16)], axis=0)

    nsplit = ((0, 9), (9, 16), (16, 25))
    near_n = []
    for j, (k0, k1) in enumerate(nsplit):
        for k, r in by_degree(lambda l: up[l], full_dy, k0, k1):
            if k == 0:
                r = r + rows_dot(gate[...], da)
            npart[k] = r.astype(BF16)
        c = remote(npart.at[k0:k1, blk(t3), :], nrb1.at[0, k0:k1], 27 + j, {"tp": t1})
        c.start()
        near_n.append(c)
    near_o = remote(npart.at[:, blk(t1), :], nrb1.at[1], 30, {"tp": t1})
    near_o.start()

    far_n = []

    def far_step(j):
        k0, k1 = nsplit[j]
        near_n[j].wait_recv()
        nsb[k0:k1] = (npart[k0:k1, blk(t2), :].astype(F32) + nrb1[0, k0:k1].astype(F32)).astype(BF16)

    def far_send(j):
        k0, k1 = nsplit[j]
        c = remote(nsb.at[k0:k1], nrb2.at[k0:k1], 41 + j, {"tp": t2})
        c.start()
        far_n.append(c)

    far_step(0)
    keep_dy(QR, half - QR)
    far_send(0)
    grad_up(QR, half - QR)
    far_step(1)
    far_step(2)
    ex_up1 = remote(gup.at[:, rows_of(odp, QR), :], gup_rb.at[:, QR:64, :], 36, {"dp": odp})
    ex_up1.start()
    s3 = jnp.zeros((ch, nat), F32)
    for k in range(COEFS):
        rf = npart[k].astype(F32) * gcol[degree_of(k)]
        if k == 0:
            st0 = jnp.sum(rf, axis=0, keepdims=True)
            st1 = jnp.sum(rf * hat_s, axis=0, keepdims=True)
        else:
            s3 = s3 + rf * xg[k].astype(F32)
        if k == 4:
            far_send(1)
    st2 = jnp.sum(s3, axis=0, keepdims=True)
    st_snd[...] = jnp.concatenate([st0, st1, st2, jnp.zeros((5, nat), F32)], axis=0)
    ex_up0.wait_recv()
    gfin[:, rows_of(dp, 0), :] = (gup[:, rows_of(dp, 0), :] + gup_rb[:, 0:QR, :]).astype(BF16)
    ssend = []
    for j, dev in enumerate((t1, t2, t3)):
        c = remote(st_snd, st_all.at[j], 37 + j, {"tp": dev})
        c.start()
        ssend.append(c)
    far_send(2)
    near_d[1].wait_recv()
    far_d.wait_recv()
    own = dpart[:, blk(t), :].astype(F32) + rb1[1].astype(F32) + rb2[...].astype(F32)
    out_ref[...] = (xg[:, blk(t), :].astype(F32) + own).astype(BF16)
    bk_up0 = remote(gfin.at[:, rows_of(dp, 0), :], gfin.at[:, rows_of(dp, 0), :], 35, {"dp": odp})
    bk_up0.start()

    bk_dn.wait_recv()
    ddown_ref[...] = gfin_dn[0:5]
    dgate_ref[...] = gfin_dn[5].astype(F32).T.astype(BF16)
    ex_up1.wait_recv()
    gfin[:, rows_of(dp, QR), :] = (gup[:, rows_of(dp, QR), :] + gup_rb[:, QR:64, :]).astype(BF16)
    for c in ssend:
        c.wait_recv()
    stat = st_snd[...] + st_all[0] + st_all[1] + st_all[2]
    b0 = stat[0:1] / ch
    b1 = stat[1:2] / ch
    b2 = (inv_v * inv_v * inv_v) * (stat[2:3] / (ch * (COEFS - 1)))
    bk_up1 = remote(gfin.at[:, rows_of(dp, QR), :], gfin.at[:, rows_of(dp, QR), :], 40, {"dp": odp})
    bk_up1.start()
    near_o.wait_recv()
    for j, (k0, k1) in enumerate(nsplit):
        far_n[j].wait_recv()
        for k in range(k0, k1):
            dn = (npart[k, blk(t), :].astype(F32) + nrb1[1, k].astype(F32) + nrb2[k].astype(F32)).astype(BF16).astype(F32)
            dhat = dn * gcol[degree_of(k), blk(t), :]
            xk = xg[k, blk(t), :].astype(F32)
            if k == 0:
                dxk = inv_s * (dhat - b0 - (xk - mean_s) * inv_s * b1)
            else:
                dxk = inv_v * dhat - xk * b2
            dx_ref[k] = (dxk + gg[k, blk(t), :].astype(F32)).astype(BF16)

    bk_up0.wait_recv()
    bk_up1.wait_recv()
    for l in range(5):
        dup_ref[l] = gfin[l].astype(F32).T.astype(BF16)
    for c in far_g + fwd_x + fwd_g + gsend + near_d + near_n + far_n + ssend + [near_x, near_g, near_o, far_d, ex_dn, ex_up0, ex_up1, bk_dn, bk_up0, bk_up1]:
        c.wait_send()


def flush(a, b, c, d, e, oa, ob, oc, od, oe, sem):
    cs = [pltpu.make_async_copy(i, o, sem.at[j]) for j, (i, o) in enumerate(zip((a, b, c, d, e), (oa, ob, oc, od, oe)))]
    for x in cs:
        x.start()
    for x in cs:
        x.wait()


def solution(mesh):
    tp_size = mesh.shape['tp']
    act_spec = P('dp', None, 'tp')
    in_specs = (act_spec, P(None, 'tp'), P(None, None, 'tp'), P(None, 'tp'), P(None, 'tp', None), P(None, None), P(None, None), act_spec)
    out_specs = (act_spec, act_spec, P(None, None, 'tp'), P(None, 'tp'), P(None, 'tp', None))

    def local_step(x_loc, gain_loc, up_loc, gate_loc, down_loc, to_grid, from_grid, grad_loc):
        nat, coefs, cl = x_loc.shape
        ch = cl * tp_size
        grid_pts = to_grid.shape[1]
        pp = -(-grid_pts // 16) * 16
        xt = x_loc.transpose(1, 2, 0)
        gt = grad_loc.transpose(1, 2, 0)
        any_spec = pl.BlockSpec(memory_space=pl.ANY)
        vmem = pl.BlockSpec(memory_space=pltpu.VMEM)
        full = pltpu.VMEM((coefs, ch, nat), BF16)
        blkb = pltpu.VMEM((coefs, cl, nat), BF16)
        sq = lambda n, d: pltpu.VMEM((n, 128, 128), d)
        shapes = (xt.shape, xt.shape, up_loc.shape, gate_loc.shape, down_loc.shape)
        outs = pl.pallas_call(
            functools.partial(kernel, tp_size, grid_pts),
            out_shape=tuple(pltpu.VMEM(sh, BF16) for sh in shapes),
            in_specs=[any_spec] * 8,
            out_specs=[vmem] * 5,
            scratch_shapes=[
                full, full, full, full, full, full, full,
                pltpu.VMEM((66 * YSTRIDE, 128), F32), pltpu.VMEM((66 * YSTRIDE, 128), F32),
                pltpu.VMEM((KPAD * 136, 128), F32), pltpu.VMEM((64 * pp, 256), F32),
                pltpu.VMEM(gain_loc.shape, F32), pltpu.VMEM((8, 128), F32), pltpu.VMEM((3, 8, 128), F32), sq(5, F32),
                sq(5, BF16), pltpu.VMEM((128, 128), BF16), sq(5, BF16), sq(5, BF16), pltpu.VMEM((128, 128), BF16), sq(5, BF16),
                pltpu.VMEM(to_grid.shape, F32), pltpu.VMEM(from_grid.shape[::-1], F32),
                pltpu.VMEM((pp, KPAD), BF16), pltpu.VMEM((KPAD, 384), BF16), pltpu.VMEM((pp, KPAD), BF16), pltpu.VMEM((KPAD, 384), BF16),
                pltpu.VMEM((2, coefs, cl, nat), BF16), blkb, blkb, pltpu.VMEM((2, coefs, cl, nat), BF16), blkb, blkb,
                pltpu.VMEM((8, 128), F32), pltpu.VMEM((3, 8, 128), F32),
                sq(6, F32), pltpu.VMEM((6, 64, 128), F32), sq(5, F32), pltpu.VMEM((5, 64, 128), F32), sq(5, BF16), sq(6, BF16),
                pltpu.VMEM((128, nat), BF16),
                pltpu.VMEM((pp, 256), BF16), pltpu.VMEM((pp, 256), BF16), pltpu.VMEM((pp, 256), BF16), pltpu.VMEM((pp, 256), BF16),
                pltpu.VMEM((pp, 256), BF16), pltpu.VMEM((pp, 256), BF16), pltpu.VMEM((pp, 256), BF16), pltpu.VMEM((pp, 256), BF16),
                pltpu.SemaphoreType.DMA((12,)), pltpu.SemaphoreType.DMA((44,)), pltpu.SemaphoreType.DMA((44,)),
            ],
            compiler_params=pltpu.CompilerParams(collective_id=0, has_side_effects=True, vmem_limit_bytes=60 * 1024 * 1024),
        )(xt, gain_loc, up_loc, gate_loc, down_loc, to_grid, from_grid.T, gt)
        out_t, dx_t, d_up, d_gate, d_down = pl.pallas_call(
            flush,
            out_shape=tuple(jax.ShapeDtypeStruct(sh, BF16) for sh in shapes),
            in_specs=[vmem] * 5,
            out_specs=[any_spec] * 5,
            scratch_shapes=[pltpu.SemaphoreType.DMA((5,))],
        )(*[pltpu.with_memory_space_constraint(o, pltpu.VMEM) for o in outs])
        return out_t.transpose(2, 0, 1), dx_t.transpose(2, 0, 1), d_up, d_gate, d_down

    return jax.shard_map(local_step, mesh=mesh, in_specs=in_specs, out_specs=out_specs, check_vma=False)
```

```python
import functools
import math
import jax
import jax.numpy as jnp
from jax import lax
from jax.experimental import pallas as pl
from jax.experimental.pallas import tpu as pltpu
from jax.sharding import PartitionSpec as P

NORM_EPS = 1e-5
MESH = pl.DeviceIdType.MESH
F32 = jnp.float32
BF16 = jnp.bfloat16
COEFS = 25
KPAD = 32
YSTRIDE = 40
UNROLL = 4
QR = 48


def degree_of(k):
    return math.isqrt(k)


def rows_dot(a, b):
    return lax.dot_general(a, b, (((1,), (0,)), ((), ())), preferred_element_type=F32)


def lanes_dot(a, b):
    return lax.dot_general(a, b, (((1,), (1,)), ((), ())), preferred_element_type=F32)


def kernel(tp_size, grid_pts, x_hbm, gain_hbm, up_hbm, gate_hbm, down_hbm, tog_hbm, frg_hbm, g_hbm,
           out_ref, dx_ref, dup_ref, dgate_ref, ddown_ref,
           xg, gg, xn, mb, dyb, dpart, npart, ya, yb, zs, hs,
           gain_in, gain_snd, gain_all, gcol, up, gate, down, upt, gatet, downt,
           tog, frg, tt, tmat, fmat, ft, rb1, sb, rb2, nrb1, nsb, nrb2,
           st_snd, st_all, gdn, gdn_rb, gup, gup_rb, gfin, gfin_dn, amat, sbuf0, sbuf1, sbuf2, sbuf3, gbuf0, gbuf1, gbuf2, gbuf3,
           loc_sem, snd_sem, rcv_sem):
    sbuf, gbuf = (sbuf0, sbuf1, sbuf2, sbuf3), (gbuf0, gbuf1, gbuf2, gbuf3)
    dp = lax.axis_index("dp")
    t = lax.axis_index("tp")
    core = lax.rem(t, 2)
    t1 = t + 1 - 2 * core
    t2 = lax.rem(t + 2, 4)
    t3 = lax.rem(t1 + 2, 4)
    odp = 1 - dp
    cl = xg.shape[1] // tp_size
    ch = xg.shape[1]
    nat = xg.shape[2]
    pp = tt.shape[0]

    def blk(i):
        return pl.ds(pl.multiple_of(i * cl, cl), cl)

    def local(src, dst, i):
        c = pltpu.make_async_copy(src, dst, loc_sem.at[i])
        c.start()
        return c

    def remote(src, dst, i, dev):
        return pltpu.make_async_remote_copy(src_ref=src, dst_ref=dst, send_sem=snd_sem.at[i], recv_sem=rcv_sem.at[i],
                                            device_id=dev, device_id_type=MESH)

    c_gain = local(gain_hbm, gain_in, 0)
    ksplit = ((0, 8), (8, 15), (15, 22), (22, 25))
    c_x = [local(x_hbm.at[k0:k1], xg.at[k0:k1, blk(t), :], 7 + j) for j, (k0, k1) in enumerate(ksplit)]
    c_tog = local(tog_hbm, tog, 2)
    c_frg = local(frg_hbm, frg, 3)
    c_up = local(up_hbm, up, 4)
    c_gate = local(gate_hbm, gate, 5)
    c_down = local(down_hbm, down, 6)
    c_g = local(g_hbm, gg.at[:, blk(t), :], 1)

    barrier = pltpu.get_barrier_semaphore()
    for dev in ({"tp": t1}, {"tp": t2}, {"tp": t3}, {"dp": odp}):
        pl.semaphore_signal(barrier, inc=1, device_id=dev, device_id_type=MESH)
    c_gain.wait()
    gain_snd[...] = jnp.zeros_like(gain_snd)
    gain_snd[0:5, 0:cl] = gain_in[...]
    placed = pltpu.roll(gain_snd[...], t * cl, 1)
    gain_snd[...] = placed
    pl.semaphore_wait(barrier, 4)
    gsend = []
    for j, dev in enumerate((t1, t2, t3)):
        c = remote(gain_snd, gain_all.at[j], 20 + j, {"tp": dev})
        c.start()
        gsend.append(c)

    def gather_start(dst, base, ready=None):
        far = []
        for j, (k0, k1) in enumerate(ksplit):
            if ready:
                ready[j].wait()
            c = remote(dst.at[k0:k1, blk(t), :], dst.at[k0:k1, blk(t), :], base + j, {"tp": t2})
            c.start()
            far.append(c)
        k0, k1 = ksplit[-1]
        c = remote(dst.at[k0:k1, blk(t), :], dst.at[k0:k1, blk(t), :], base + 8, {"tp": t3})
        c.start()
        far.append(c)
        near = remote(dst.at[:, blk(t), :], dst.at[:, blk(t), :], base + 4, {"tp": t1})
        near.start()
        return far, near

    def gather_finish(far, near, dst, base, step=None):
        fwd = []
        for j, (k0, k1) in enumerate(ksplit[:-1]):
            far[j].wait_recv()
            c = remote(dst.at[k0:k1, blk(t2), :], dst.at[k0:k1, blk(t2), :], base + 5 + j, {"tp": t1})
            c.start()
            fwd.append(c)
            if step and j == 0:
                near.wait_recv()
                step((t, t1), 0, COEFS)
            if step and j > 0:
                fwd[j - 1].wait_recv()
                step((t2, t3), *ksplit[j - 1])
        return fwd

    def gather_wait(far, near, fwd):
        near.wait_recv()
        for c in fwd:
            c.wait_recv()
        far[-2].wait_recv()
        far[-1].wait_recv()

    far_x, near_x = gather_start(xg, 0, c_x)

    c_tog.wait()
    c_frg.wait()
    tpad = jnp.zeros((KPAD, 384), F32)
    tmat[...] = tpad.astype(BF16)
    ft[...] = tpad.astype(BF16)
    tmat[0:COEFS, 0:grid_pts] = tog[...].astype(BF16)
    frg_pad = jnp.concatenate([jnp.zeros((1, grid_pts), F32), frg[...]], axis=0)
    ft[0:COEFS, 0:grid_pts] = frg_pad.astype(BF16)
    for src, dst in ((tmat, tt), (ft, fmat)):
        wide = jnp.concatenate([src[...].astype(F32) * 0.5, jnp.zeros((128 - KPAD, 384), F32)], axis=0)
        for j in range(3):
            tr = wide[:, 128 * j:128 * (j + 1)].T
            rows = min(128, pp - 128 * j)
            dst[128 * j:128 * j + rows, :] = tr[0:rows, 0:KPAD].astype(BF16)
    c_up.wait()
    c_gate.wait()
    c_down.wait()
    for l in range(5):
        upt[l] = up[l].astype(F32).T.astype(BF16)
        downt[l] = down[l].astype(F32).T.astype(BF16)
    gatet[...] = gate[...].astype(F32).T.astype(BF16)
    ya[...] = jnp.zeros_like(ya)
    yb[...] = jnp.zeros_like(yb)
    for c in gsend:
        c.wait_recv()
    gain_full = placed + gain_all[0] + gain_all[1] + gain_all[2]
    for l in range(5):
        gcol[l] = jnp.broadcast_to(gain_full[l:l + 1, :], (ch, ch)).T

    sums = [jnp.zeros((cl, nat), F32)]

    def square_step(blocks, k0, k1):
        for k in range(max(k0, 1), k1):
            for i in blocks:
                v = xg[k, blk(i), :].astype(F32)
                sums[0] = sums[0] + v * v

    fwd_x = gather_finish(far_x, near_x, xg, 0, square_step)
    for c in far_x:
        c.wait_send()
    c_g.wait()
    far_g, near_g = gather_start(gg, 10)
    fwd_x[-1].wait_recv()
    square_step((t2, t3), *ksplit[2])
    far_x[-2].wait_recv()
    far_x[-1].wait_recv()
    square_step((t2, t3), *ksplit[3])

    x0 = xg[0].astype(F32)
    mean_s = jnp.sum(x0, axis=0, keepdims=True) / ch
    cent = x0 - mean_s
    inv_s = lax.rsqrt(jnp.sum(cent * cent, axis=0, keepdims=True) / ch + NORM_EPS)
    hat_s = cent * inv_s
    inv_v = lax.rsqrt(jnp.sum(sums[0], axis=0, keepdims=True) / (ch * (COEFS - 1)) + NORM_EPS)
    xn[0] = (hat_s * gcol[0]).astype(BF16)
    for k in range(1, COEFS):
        xn[k] = (xg[k].astype(F32) * inv_v * gcol[degree_of(k)]).astype(BF16)

    def by_degree(lhs_of, get, lo=0, hi=COEFS):
        for l in range(5):
            k = max(l * l, lo)
            k1 = min((l + 1) * (l + 1), hi)
            while k < k1:
                n = min(2, k1 - k)
                r = rows_dot(lhs_of(l), get(k) if n == 1 else jnp.concatenate([get(k), get(k + 1)], axis=1))
                for j in range(n):
                    yield k + j, r[:, nat * j:nat * (j + 1)]
                k += n

    def over_degree(a_of, b_of, l):
        ks = range(l * l, (l + 1) * (l + 1))
        return lanes_dot(jnp.concatenate([a_of(k) for k in ks], axis=1), jnp.concatenate([b_of(k) for k in ks], axis=1))

    def spread(get, lhs_of):
        for k, r in by_degree(lhs_of, get):
            ya[pl.ds(k, 64, stride=YSTRIDE), :] = r[0:64]
            yb[pl.ds(k, 64, stride=YSTRIDE), :] = r[64:128]

    spread(lambda k: xn[k], lambda l: upt[l])
    a_r = rows_dot(gatet[...], xn[0]).astype(BF16)
    amat[...] = a_r
    a_h = a_r.astype(F32) * 0.5
    mb[0] = (a_h * (1.0 + jnp.tanh(a_h))).astype(BF16)

    def pair(i):
        base = pl.multiple_of(i * YSTRIDE, 8)
        return jnp.concatenate([ya[pl.ds(base, KPAD), :], yb[pl.ds(base, KPAD), :]], axis=1).astype(BF16)

    def put(i, r):
        zs[pl.ds(i, KPAD, stride=136), :] = r[:, 0:128]
        zs[pl.ds(i + 64, KPAD, stride=136), :] = r[:, 128:256]

    def stage_u(p, dst):
        dst[...] = rows_dot(tt[...], pair(p)).astype(BF16)

    def stage_s(p, src, dst):
        h = src[...].astype(F32)
        w = 1.0 + jnp.tanh(h)
        s = h * w
        dst[...] = s.astype(BF16)
        hs[pl.ds(pl.multiple_of(p * pp, 16), pp), :] = w + s * (2.0 - w)

    def stage_z(p, src, lhs):
        put(p, rows_dot(lhs[:, 0:pp], src[...]))

    stage_u(0, gbuf[0])
    stage_u(1, gbuf[1])

    def fwd_body(it, carry):
        for half_step in range(2):
            p = it * UNROLL + 2 * half_step
            now, other = 2 * (half_step % 2), 2 * ((half_step + 1) % 2)
            for j in range(2):
                stage_z(jnp.maximum(p + j - 2, 0), sbuf[other + j], ft)
                stage_u(p + j + 2, gbuf[other + j])
                stage_s(p + j, gbuf[now + j], sbuf[now + j])
        return carry

    lax.fori_loop(0, 48 // UNROLL, fwd_body, 0)
    fwd_g = gather_finish(far_g, near_g, gg, 10)
    lax.fori_loop(48 // UNROLL, 64 // UNROLL, fwd_body, 0)
    gather_wait(far_g, near_g, fwd_g)
    stage_z(62, sbuf[2], ft)
    stage_z(63, sbuf[3], ft)

    def stage_g(p, dst):
        dst[...] = rows_dot(fmat[...], pair(p)).astype(BF16)

    spread(lambda k: gg[k], lambda l: down[l])
    dm0 = rows_dot(down[0], gg[0]).astype(BF16).astype(F32)
    a_h = amat[...].astype(F32) * 0.5
    w_a = 1.0 + jnp.tanh(a_h)
    da = (dm0 * (0.5 * w_a * (1.0 + a_h * (2.0 - w_a)))).astype(BF16)

    stage_g(0, gbuf[0])
    stage_g(1, gbuf[1])

    for k in range(1, COEFS):
        mb[k] = zs[k * 136:k * 136 + 128, :].astype(BF16)
    for k, r in by_degree(lambda l: downt[l], lambda k: mb[k]):
        dpart[k] = r.astype(BF16)

    def scatter_near(part, rb, base):
        cs = []
        for j, b in enumerate((t3, t1)):
            c = remote(part.at[:, blk(b), :], rb.at[j], base + j, {"tp": t1})
            c.start()
            cs.append(c)
        return cs

    near_d = scatter_near(dpart, rb1, 23)

    for l in range(5):
        gdn[l] = over_degree(lambda k: mb[k], lambda k: gg[k], l)
    gdn[5] = lanes_dot(da, xn[0])
    half = 64
    mine = pl.ds(pl.multiple_of(dp * half, half), half)
    theirs = pl.ds(pl.multiple_of(odp * half, half), half)
    ex_dn = remote(gdn.at[:, theirs, :], gdn_rb, 26, {"dp": odp})
    ex_dn.start()

    def stage_e(p, src, dst):
        gp = hs[pl.ds(pl.multiple_of(p * pp, 16), pp), :]
        dst[...] = (src[...].astype(F32) * gp).astype(BF16)


    def bwd_body(it, carry):
        for half_step in range(2):
            p = it * UNROLL + 2 * half_step
            now, other = 2 * (half_step % 2), 2 * ((half_step + 1) % 2)
            for j in range(2):
                stage_z(jnp.maximum(p + j - 2, 0), sbuf[other + j], tmat)
                stage_g(p + j + 2, gbuf[other + j])
                stage_e(p + j, gbuf[now + j], sbuf[now + j])
        return carry

    def keep_dy(lo, n):
        for k in range(COEFS):
            for o in (lo, 64 + lo):
                dyb[k, o:o + n, :] = zs[k * 136 + o:k * 136 + o + n, :].astype(BF16)

    def grad_up(lo, n):
        def dy(k):
            return jnp.concatenate([dyb[k, lo:lo + n, :], dyb[k, 64 + lo:64 + lo + n, :]], axis=0)

        for l in range(5):
            acc = over_degree(dy, lambda k: xn[k], l)
            gup[l, lo:lo + n, :] = acc[0:n]
            gup[l, 64 + lo:64 + lo + n, :] = acc[n:2 * n]

    def rows_of(d, lo):
        return pl.ds(pl.multiple_of(d * half + lo, 16), half - QR if lo else QR)

    mid_steps = (QR + 4) // UNROLL
    lax.fori_loop(0, 12 // UNROLL, bwd_body, 0)
    near_d[0].wait_recv()
    sb[...] = (dpart[:, blk(t2), :].astype(F32) + rb1[0].astype(F32)).astype(BF16)
    far_d = remote(sb, rb2, 25, {"tp": t2})
    far_d.start()
    lax.fori_loop(12 // UNROLL, mid_steps, bwd_body, 0)

    keep_dy(0, QR)
    grad_up(0, QR)
    ex_up0 = remote(gup.at[:, rows_of(odp, 0), :], gup_rb.at[:, 0:QR, :], 33, {"dp": odp})
    ex_dn.wait_recv()
    gfin_dn[:, mine, :] = (gdn[:, mine, :] + gdn_rb[...]).astype(BF16)
    ex_up0.start()
    bk_dn = remote(gfin_dn.at[:, mine, :], gfin_dn.at[:, mine, :], 34, {"dp": odp})
    bk_dn.start()

    lax.fori_loop(mid_steps, 64 // UNROLL, bwd_body, 0)
    stage_z(62, sbuf[2], tmat)
    stage_z(63, sbuf[3], tmat)

    def full_dy(k):
        return jnp.concatenate([dyb[k, 0:QR, :], zs[k * 136 + QR:k * 136 + 64, :].astype(BF16),
                                dyb[k, 64:64 + QR, :], zs[k * 136 + 64 + QR:k * 136 + 128, :].astype(BF16)], axis=0)

    nsplit = ((0, 6), (6, 16), (16, 25))
    near_n = []
    for j, (k0, k1) in enumerate(nsplit):
        for k, r in by_degree(lambda l: up[l], full_dy, k0, k1):
            if k == 0:
                r = r + rows_dot(gate[...], da)
            npart[k] = r.astype(BF16)
        c = remote(npart.at[k0:k1, blk(t3), :], nrb1.at[0, k0:k1], 27 + j, {"tp": t1})
        c.start()
        near_n.append(c)
    near_o = remote(npart.at[:, blk(t1), :], nrb1.at[1], 30, {"tp": t1})
    near_o.start()

    far_n = []

    def far_step(j):
        k0, k1 = nsplit[j]
        near_n[j].wait_recv()
        nsb[k0:k1] = (npart[k0:k1, blk(t2), :].astype(F32) + nrb1[0, k0:k1].astype(F32)).astype(BF16)

    def far_send(j):
        k0, k1 = nsplit[j]
        c = remote(nsb.at[k0:k1], nrb2.at[k0:k1], 41 + j, {"tp": t2})
        c.start()
        far_n.append(c)

    far_step(0)
    keep_dy(QR, half - QR)
    far_send(0)
    far_step(1)
    grad_up(QR, half - QR)
    far_send(1)
    far_step(2)
    ex_up1 = remote(gup.at[:, rows_of(odp, QR), :], gup_rb.at[:, QR:64, :], 36, {"dp": odp})
    ex_up1.start()
    s3 = jnp.zeros((ch, nat), F32)
    for k in range(COEFS):
        rf = npart[k].astype(F32) * gcol[degree_of(k)]
        if k == 0:
            st0 = jnp.sum(rf, axis=0, keepdims=True)
            st1 = jnp.sum(rf * hat_s, axis=0, keepdims=True)
        else:
            s3 = s3 + rf * xg[k].astype(F32)
    st2 = jnp.sum(s3, axis=0, keepdims=True)
    st_snd[...] = jnp.concatenate([st0, st1, st2, jnp.zeros((5, nat), F32)], axis=0)
    ex_up0.wait_recv()
    gfin[:, rows_of(dp, 0), :] = (gup[:, rows_of(dp, 0), :] + gup_rb[:, 0:QR, :]).astype(BF16)
    ssend = []
    for j, dev in enumerate((t1, t2, t3)):
        c = remote(st_snd, st_all.at[j], 37 + j, {"tp": dev})
        c.start()
        ssend.append(c)
    far_send(2)
    near_d[1].wait_recv()
    far_d.wait_recv()
    own = dpart[:, blk(t), :].astype(F32) + rb1[1].astype(F32) + rb2[...].astype(F32)
    out_ref[...] = (xg[:, blk(t), :].astype(F32) + own).astype(BF16)
    bk_up0 = remote(gfin.at[:, rows_of(dp, 0), :], gfin.at[:, rows_of(dp, 0), :], 35, {"dp": odp})
    bk_up0.start()

    bk_dn.wait_recv()
    ddown_ref[...] = gfin_dn[0:5]
    dgate_ref[...] = gfin_dn[5].astype(F32).T.astype(BF16)
    ex_up1.wait_recv()
    gfin[:, rows_of(dp, QR), :] = (gup[:, rows_of(dp, QR), :] + gup_rb[:, QR:64, :]).astype(BF16)
    for c in ssend:
        c.wait_recv()
    stat = st_snd[...] + st_all[0] + st_all[1] + st_all[2]
    b0 = stat[0:1] / ch
    b1 = stat[1:2] / ch
    b2 = (inv_v * inv_v * inv_v) * (stat[2:3] / (ch * (COEFS - 1)))
    bk_up1 = remote(gfin.at[:, rows_of(dp, QR), :], gfin.at[:, rows_of(dp, QR), :], 40, {"dp": odp})
    bk_up1.start()
    near_o.wait_recv()
    for j, (k0, k1) in enumerate(nsplit):
        far_n[j].wait_recv()
        for k in range(k0, k1):
            dn = (npart[k, blk(t), :].astype(F32) + nrb1[1, k].astype(F32) + nrb2[k].astype(F32)).astype(BF16).astype(F32)
            dhat = dn * gcol[degree_of(k), blk(t), :]
            xk = xg[k, blk(t), :].astype(F32)
            if k == 0:
                dxk = inv_s * (dhat - b0 - (xk - mean_s) * inv_s * b1)
            else:
                dxk = inv_v * dhat - xk * b2
            dx_ref[k] = (dxk + gg[k, blk(t), :].astype(F32)).astype(BF16)

    bk_up0.wait_recv()
    bk_up1.wait_recv()
    for l in range(5):
        dup_ref[l] = gfin[l].astype(F32).T.astype(BF16)
    for c in far_g + fwd_x + fwd_g + gsend + near_d + near_n + far_n + ssend + [near_x, near_g, near_o, far_d, ex_dn, ex_up0, ex_up1, bk_dn, bk_up0, bk_up1]:
        c.wait_send()


def flush(a, b, c, d, e, oa, ob, oc, od, oe, sem):
    cs = [pltpu.make_async_copy(i, o, sem.at[j]) for j, (i, o) in enumerate(zip((a, b, c, d, e), (oa, ob, oc, od, oe)))]
    for x in cs:
        x.start()
    for x in cs:
        x.wait()


def solution(mesh):
    tp_size = mesh.shape['tp']
    act_spec = P('dp', None, 'tp')
    in_specs = (act_spec, P(None, 'tp'), P(None, None, 'tp'), P(None, 'tp'), P(None, 'tp', None), P(None, None), P(None, None), act_spec)
    out_specs = (act_spec, act_spec, P(None, None, 'tp'), P(None, 'tp'), P(None, 'tp', None))

    def local_step(x_loc, gain_loc, up_loc, gate_loc, down_loc, to_grid, from_grid, grad_loc):
        nat, coefs, cl = x_loc.shape
        ch = cl * tp_size
        grid_pts = to_grid.shape[1]
        pp = -(-grid_pts // 16) * 16
        xt = x_loc.transpose(1, 2, 0)
        gt = grad_loc.transpose(1, 2, 0)
        any_spec = pl.BlockSpec(memory_space=pl.ANY)
        vmem = pl.BlockSpec(memory_space=pltpu.VMEM)
        full = pltpu.VMEM((coefs, ch, nat), BF16)
        blkb = pltpu.VMEM((coefs, cl, nat), BF16)
        sq = lambda n, d: pltpu.VMEM((n, 128, 128), d)
        shapes = (xt.shape, xt.shape, up_loc.shape, gate_loc.shape, down_loc.shape)
        outs = pl.pallas_call(
            functools.partial(kernel, tp_size, grid_pts),
            out_shape=tuple(pltpu.VMEM(sh, BF16) for sh in shapes),
            in_specs=[any_spec] * 8,
            out_specs=[vmem] * 5,
            scratch_shapes=[
                full, full, full, full, full, full, full,
                pltpu.VMEM((66 * YSTRIDE, 128), F32), pltpu.VMEM((66 * YSTRIDE, 128), F32),
                pltpu.VMEM((KPAD * 136, 128), F32), pltpu.VMEM((64 * pp, 256), F32),
                pltpu.VMEM(gain_loc.shape, F32), pltpu.VMEM((8, 128), F32), pltpu.VMEM((3, 8, 128), F32), sq(5, F32),
                sq(5, BF16), pltpu.VMEM((128, 128), BF16), sq(5, BF16), sq(5, BF16), pltpu.VMEM((128, 128), BF16), sq(5, BF16),
                pltpu.VMEM(to_grid.shape, F32), pltpu.VMEM(from_grid.shape[::-1], F32),
                pltpu.VMEM((pp, KPAD), BF16), pltpu.VMEM((KPAD, 384), BF16), pltpu.VMEM((pp, KPAD), BF16), pltpu.VMEM((KPAD, 384), BF16),
                pltpu.VMEM((2, coefs, cl, nat), BF16), blkb, blkb, pltpu.VMEM((2, coefs, cl, nat), BF16), blkb, blkb,
                pltpu.VMEM((8, 128), F32), pltpu.VMEM((3, 8, 128), F32),
                sq(6, F32), pltpu.VMEM((6, 64, 128), F32), sq(5, F32), pltpu.VMEM((5, 64, 128), F32), sq(5, BF16), sq(6, BF16),
                pltpu.VMEM((128, nat), BF16),
                pltpu.VMEM((pp, 256), BF16), pltpu.VMEM((pp, 256), BF16), pltpu.VMEM((pp, 256), BF16), pltpu.VMEM((pp, 256), BF16),
                pltpu.VMEM((pp, 256), BF16), pltpu.VMEM((pp, 256), BF16), pltpu.VMEM((pp, 256), BF16), pltpu.VMEM((pp, 256), BF16),
                pltpu.SemaphoreType.DMA((12,)), pltpu.SemaphoreType.DMA((46,)), pltpu.SemaphoreType.DMA((46,)),
            ],
            compiler_params=pltpu.CompilerParams(collective_id=0, has_side_effects=True, vmem_limit_bytes=60 * 1024 * 1024),
        )(xt, gain_loc, up_loc, gate_loc, down_loc, to_grid, from_grid.T, gt)
        out_t, dx_t, d_up, d_gate, d_down = pl.pallas_call(
            flush,
            out_shape=tuple(jax.ShapeDtypeStruct(sh, BF16) for sh in shapes),
            in_specs=[vmem] * 5,
            out_specs=[any_spec] * 5,
            scratch_shapes=[pltpu.SemaphoreType.DMA((5,))],
        )(*[pltpu.with_memory_space_constraint(o, pltpu.VMEM) for o in outs])
        return out_t.transpose(2, 0, 1), dx_t.transpose(2, 0, 1), d_up, d_gate, d_down

    return jax.shard_map(local_step, mesh=mesh, in_specs=in_specs, out_specs=out_specs, check_vma=False)
```

```python
import functools
import math
import jax
import jax.numpy as jnp
from jax import lax
from jax.experimental import pallas as pl
from jax.experimental.pallas import tpu as pltpu
from jax.sharding import PartitionSpec as P

NORM_EPS = 1e-5
MESH = pl.DeviceIdType.MESH
F32 = jnp.float32
BF16 = jnp.bfloat16
COEFS = 25
KPAD = 32
YSTRIDE = 40
UNROLL = 4
QR = 48


def degree_of(k):
    return math.isqrt(k)


def rows_dot(a, b):
    return lax.dot_general(a, b, (((1,), (0,)), ((), ())), preferred_element_type=F32)


def lanes_dot(a, b):
    return lax.dot_general(a, b, (((1,), (1,)), ((), ())), preferred_element_type=F32)


def kernel(tp_size, grid_pts, x_hbm, gain_hbm, up_hbm, gate_hbm, down_hbm, tog_hbm, frg_hbm, g_hbm,
           out_ref, dx_ref, dup_ref, dgate_ref, ddown_ref,
           xg, gg, xn, mb, dyb, dpart, npart, ya, yb, zs, hs,
           gain_in, gain_snd, gain_all, gcol, up, gate, down, upt, gatet, downt,
           tog, frg, tt, tmat, fmat, ft, rb1, sb, rb2, nrb1, nsb, nrb2,
           st_snd, st_all, gdn, gdn_rb, gup, gup_rb, gfin, gfin_dn, amat, sbuf0, sbuf1, sbuf2, sbuf3, gbuf0, gbuf1, gbuf2, gbuf3,
           loc_sem, snd_sem, rcv_sem):
    sbuf, gbuf = (sbuf0, sbuf1, sbuf2, sbuf3), (gbuf0, gbuf1, gbuf2, gbuf3)
    dp = lax.axis_index("dp")
    t = lax.axis_index("tp")
    core = lax.rem(t, 2)
    t1 = t + 1 - 2 * core
    t2 = lax.rem(t + 2, 4)
    t3 = lax.rem(t1 + 2, 4)
    odp = 1 - dp
    cl = xg.shape[1] // tp_size
    ch = xg.shape[1]
    nat = xg.shape[2]
    pp = tt.shape[0]

    def blk(i):
        return pl.ds(pl.multiple_of(i * cl, cl), cl)

    def local(src, dst, i):
        c = pltpu.make_async_copy(src, dst, loc_sem.at[i])
        c.start()
        return c

    def remote(src, dst, i, dev):
        return pltpu.make_async_remote_copy(src_ref=src, dst_ref=dst, send_sem=snd_sem.at[i], recv_sem=rcv_sem.at[i],
                                            device_id=dev, device_id_type=MESH)

    c_gain = local(gain_hbm, gain_in, 0)
    ksplit = ((0, 8), (8, 15), (15, 22), (22, 25))
    c_x = [local(x_hbm.at[k0:k1], xg.at[k0:k1, blk(t), :], 7 + j) for j, (k0, k1) in enumerate(ksplit)]
    c_tog = local(tog_hbm, tog, 2)
    c_frg = local(frg_hbm, frg, 3)
    c_up = local(up_hbm, up, 4)
    c_gate = local(gate_hbm, gate, 5)
    c_down = local(down_hbm, down, 6)
    c_g = local(g_hbm, gg.at[:, blk(t), :], 1)

    barrier = pltpu.get_barrier_semaphore()
    for dev in ({"tp": t1}, {"tp": t2}, {"tp": t3}, {"dp": odp}):
        pl.semaphore_signal(barrier, inc=1, device_id=dev, device_id_type=MESH)
    c_gain.wait()
    gain_snd[...] = jnp.zeros_like(gain_snd)
    gain_snd[0:5, 0:cl] = gain_in[...]
    placed = pltpu.roll(gain_snd[...], t * cl, 1)
    gain_snd[...] = placed
    pl.semaphore_wait(barrier, 4)
    gsend = []
    for j, dev in enumerate((t1, t2, t3)):
        c = remote(gain_snd, gain_all.at[j], 20 + j, {"tp": dev})
        c.start()
        gsend.append(c)

    def gather_start(dst, base, ready=None):
        far = []
        for j, (k0, k1) in enumerate(ksplit):
            if ready:
                ready[j].wait()
            c = remote(dst.at[k0:k1, blk(t), :], dst.at[k0:k1, blk(t), :], base + j, {"tp": t2})
            c.start()
            far.append(c)
        k0, k1 = ksplit[-1]
        c = remote(dst.at[k0:k1, blk(t), :], dst.at[k0:k1, blk(t), :], base + 8, {"tp": t3})
        c.start()
        far.append(c)
        near = remote(dst.at[:, blk(t), :], dst.at[:, blk(t), :], base + 4, {"tp": t1})
        near.start()
        return far, near

    def gather_finish(far, near, dst, base, step=None):
        fwd = []
        for j, (k0, k1) in enumerate(ksplit[:-1]):
            far[j].wait_recv()
            c = remote(dst.at[k0:k1, blk(t2), :], dst.at[k0:k1, blk(t2), :], base + 5 + j, {"tp": t1})
            c.start()
            fwd.append(c)
            if step and j == 0:
                near.wait_recv()
                step((t, t1), 0, COEFS)
            if step and j > 0:
                fwd[j - 1].wait_recv()
                step((t2, t3), *ksplit[j - 1])
        return fwd

    def gather_wait(far, near, fwd):
        near.wait_recv()
        for c in fwd:
            c.wait_recv()
        far[-2].wait_recv()
        far[-1].wait_recv()

    far_x, near_x = gather_start(xg, 0, c_x)

    c_tog.wait()
    c_frg.wait()
    tpad = jnp.zeros((KPAD, 384), F32)
    tmat[...] = tpad.astype(BF16)
    ft[...] = tpad.astype(BF16)
    tmat[0:COEFS, 0:grid_pts] = tog[...].astype(BF16)
    frg_pad = jnp.concatenate([jnp.zeros((1, grid_pts), F32), frg[...]], axis=0)
    ft[0:COEFS, 0:grid_pts] = frg_pad.astype(BF16)
    for src, dst in ((tmat, tt), (ft, fmat)):
        wide = jnp.concatenate([src[...].astype(F32) * 0.5, jnp.zeros((128 - KPAD, 384), F32)], axis=0)
        for j in range(3):
            tr = wide[:, 128 * j:128 * (j + 1)].T
            rows = min(128, pp - 128 * j)
            dst[128 * j:128 * j + rows, :] = tr[0:rows, 0:KPAD].astype(BF16)
    c_up.wait()
    c_gate.wait()
    c_down.wait()
    for l in range(5):
        upt[l] = up[l].astype(F32).T.astype(BF16)
        downt[l] = down[l].astype(F32).T.astype(BF16)
    gatet[...] = gate[...].astype(F32).T.astype(BF16)
    ya[...] = jnp.zeros_like(ya)
    yb[...] = jnp.zeros_like(yb)
    for c in gsend:
        c.wait_recv()
    gain_full = placed + gain_all[0] + gain_all[1] + gain_all[2]
    for l in range(5):
        gcol[l] = jnp.broadcast_to(gain_full[l:l + 1, :], (ch, ch)).T

    sums = [jnp.zeros((cl, nat), F32)]

    def square_step(blocks, k0, k1):
        for k in range(max(k0, 1), k1):
            for i in blocks:
                v = xg[k, blk(i), :].astype(F32)
                sums[0] = sums[0] + v * v

    fwd_x = gather_finish(far_x, near_x, xg, 0, square_step)
    for c in far_x:
        c.wait_send()
    c_g.wait()
    far_g, near_g = gather_start(gg, 10)
    fwd_x[-1].wait_recv()
    square_step((t2, t3), *ksplit[2])
    far_x[-2].wait_recv()
    far_x[-1].wait_recv()
    square_step((t2, t3), *ksplit[3])

    x0 = xg[0].astype(F32)
    mean_s = jnp.sum(x0, axis=0, keepdims=True) / ch
    cent = x0 - mean_s
    inv_s = lax.rsqrt(jnp.sum(cent * cent, axis=0, keepdims=True) / ch + NORM_EPS)
    hat_s = cent * inv_s
    inv_v = lax.rsqrt(jnp.sum(sums[0], axis=0, keepdims=True) / (ch * (COEFS - 1)) + NORM_EPS)
    xn[0] = (hat_s * gcol[0]).astype(BF16)
    for k in range(1, COEFS):
        xn[k] = (xg[k].astype(F32) * inv_v * gcol[degree_of(k)]).astype(BF16)

    def by_degree(lhs_of, get, lo=0, hi=COEFS):
        for l in range(5):
            k = max(l * l, lo)
            k1 = min((l + 1) * (l + 1), hi)
            while k < k1:
                n = min(2, k1 - k)
                r = rows_dot(lhs_of(l), get(k) if n == 1 else jnp.concatenate([get(k), get(k + 1)], axis=1))
                for j in range(n):
                    yield k + j, r[:, nat * j:nat * (j + 1)]
                k += n

    def over_degree(a_of, b_of, l):
        ks = range(l * l, (l + 1) * (l + 1))
        return lanes_dot(jnp.concatenate([a_of(k) for k in ks], axis=1), jnp.concatenate([b_of(k) for k in ks], axis=1))

    def spread(get, lhs_of):
        for k, r in by_degree(lhs_of, get):
            ya[pl.ds(k, 64, stride=YSTRIDE), :] = r[0:64]
            yb[pl.ds(k, 64, stride=YSTRIDE), :] = r[64:128]

    spread(lambda k: xn[k], lambda l: upt[l])
    a_r = rows_dot(gatet[...], xn[0]).astype(BF16)
    amat[...] = a_r
    a_h = a_r.astype(F32) * 0.5
    mb[0] = (a_h * (1.0 + jnp.tanh(a_h))).astype(BF16)

    def pair(i):
        base = pl.multiple_of(i * YSTRIDE, 8)
        return jnp.concatenate([ya[pl.ds(base, KPAD), :], yb[pl.ds(base, KPAD), :]], axis=1).astype(BF16)

    def put(i, r):
        zs[pl.ds(i, KPAD, stride=136), :] = r[:, 0:128]
        zs[pl.ds(i + 64, KPAD, stride=136), :] = r[:, 128:256]

    def stage_u(p, dst):
        dst[...] = rows_dot(tt[...], pair(p)).astype(BF16)

    def stage_s(p, src, dst):
        h = src[...].astype(F32)
        w = 1.0 + jnp.tanh(h)
        s = h * w
        dst[...] = s.astype(BF16)
        hs[pl.ds(pl.multiple_of(p * pp, 16), pp), :] = w + s * (2.0 - w)

    def stage_z(p, src, lhs):
        put(p, rows_dot(lhs[:, 0:pp], src[...]))

    stage_u(0, gbuf[0])
    stage_u(1, gbuf[1])

    def fwd_body(it, carry):
        for half_step in range(2):
            p = it * UNROLL + 2 * half_step
            now, other = 2 * (half_step % 2), 2 * ((half_step + 1) % 2)
            for j in range(2):
                stage_z(jnp.maximum(p + j - 2, 0), sbuf[other + j], ft)
                stage_u(p + j + 2, gbuf[other + j])
                stage_s(p + j, gbuf[now + j], sbuf[now + j])
        return carry

    lax.fori_loop(0, 48 // UNROLL, fwd_body, 0)
    fwd_g = gather_finish(far_g, near_g, gg, 10)
    lax.fori_loop(48 // UNROLL, 64 // UNROLL, fwd_body, 0)
    stage_z(62, sbuf[2], ft)
    stage_z(63, sbuf[3], ft)

    for k in range(1, COEFS):
        mb[k] = zs[k * 136:k * 136 + 128, :].astype(BF16)
    for k, r in by_degree(lambda l: downt[l], lambda k: mb[k]):
        dpart[k] = r.astype(BF16)

    def scatter_near(part, rb, base):
        cs = []
        for j, b in enumerate((t3, t1)):
            c = remote(part.at[:, blk(b), :], rb.at[j], base + j, {"tp": t1})
            c.start()
            cs.append(c)
        return cs

    near_d = scatter_near(dpart, rb1, 23)

    gather_wait(far_g, near_g, fwd_g)
    spread(lambda k: gg[k], lambda l: down[l])
    dm0 = rows_dot(down[0], gg[0]).astype(BF16).astype(F32)
    a_h = amat[...].astype(F32) * 0.5
    w_a = 1.0 + jnp.tanh(a_h)
    da = (dm0 * (0.5 * w_a * (1.0 + a_h * (2.0 - w_a)))).astype(BF16)

    for l in range(5):
        gdn[l] = over_degree(lambda k: mb[k], lambda k: gg[k], l)
    gdn[5] = lanes_dot(da, xn[0])
    half = 64
    mine = pl.ds(pl.multiple_of(dp * half, half), half)
    theirs = pl.ds(pl.multiple_of(odp * half, half), half)
    ex_dn = remote(gdn.at[:, theirs, :], gdn_rb, 26, {"dp": odp})
    ex_dn.start()

    def stage_g(p, dst):
        dst[...] = rows_dot(fmat[...], pair(p)).astype(BF16)

    def stage_e(p, src, dst):
        gp = hs[pl.ds(pl.multiple_of(p * pp, 16), pp), :]
        dst[...] = (src[...].astype(F32) * gp).astype(BF16)

    stage_g(0, gbuf[0])
    stage_g(1, gbuf[1])

    def bwd_body(it, carry):
        for half_step in range(2):
            p = it * UNROLL + 2 * half_step
            now, other = 2 * (half_step % 2), 2 * ((half_step + 1) % 2)
            for j in range(2):
                stage_z(jnp.maximum(p + j - 2, 0), sbuf[other + j], tmat)
                stage_g(p + j + 2, gbuf[other + j])
                stage_e(p + j, gbuf[now + j], sbuf[now + j])
        return carry

    def keep_dy(lo, n):
        for k in range(COEFS):
            for o in (lo, 64 + lo):
                dyb[k, o:o + n, :] = zs[k * 136 + o:k * 136 + o + n, :].astype(BF16)

    def grad_up(lo, n):
        def dy(k):
            return jnp.concatenate([dyb[k, lo:lo + n, :], dyb[k, 64 + lo:64 + lo + n, :]], axis=0)

        for l in range(5):
            acc = over_degree(dy, lambda k: xn[k], l)
            gup[l, lo:lo + n, :] = acc[0:n]
            gup[l, 64 + lo:64 + lo + n, :] = acc[n:2 * n]

    def rows_of(d, lo):
        return pl.ds(pl.multiple_of(d * half + lo, 16), half - QR if lo else QR)

    mid_steps = (QR + 4) // UNROLL
    lax.fori_loop(0, 4 // UNROLL, bwd_body, 0)
    near_d[0].wait_recv()
    sb[...] = (dpart[:, blk(t2), :].astype(F32) + rb1[0].astype(F32)).astype(BF16)
    far_d = remote(sb, rb2, 25, {"tp": t2})
    far_d.start()
    lax.fori_loop(4 // UNROLL, mid_steps, bwd_body, 0)

    keep_dy(0, QR)
    grad_up(0, QR)
    ex_up0 = remote(gup.at[:, rows_of(odp, 0), :], gup_rb.at[:, 0:QR, :], 33, {"dp": odp})
    ex_dn.wait_recv()
    gfin_dn[:, mine, :] = (gdn[:, mine, :] + gdn_rb[...]).astype(BF16)
    ex_up0.start()
    bk_dn = remote(gfin_dn.at[:, mine, :], gfin_dn.at[:, mine, :], 34, {"dp": odp})
    bk_dn.start()

    lax.fori_loop(mid_steps, 64 // UNROLL, bwd_body, 0)
    stage_z(62, sbuf[2], tmat)
    stage_z(63, sbuf[3], tmat)

    def full_dy(k):
        return jnp.concatenate([dyb[k, 0:QR, :], zs[k * 136 + QR:k * 136 + 64, :].astype(BF16),
                                dyb[k, 64:64 + QR, :], zs[k * 136 + 64 + QR:k * 136 + 128, :].astype(BF16)], axis=0)

    nsplit = ((0, 9), (9, 16), (16, 25))
    near_n = []
    for j, (k0, k1) in enumerate(nsplit):
        for k, r in by_degree(lambda l: up[l], full_dy, k0, k1):
            if k == 0:
                r = r + rows_dot(gate[...], da)
            npart[k] = r.astype(BF16)
        c = remote(npart.at[k0:k1, blk(t3), :], nrb1.at[0, k0:k1], 27 + j, {"tp": t1})
        c.start()
        near_n.append(c)
    near_o = remote(npart.at[:, blk(t1), :], nrb1.at[1], 30, {"tp": t1})
    near_o.start()

    far_n = []

    def far_step(j):
        k0, k1 = nsplit[j]
        near_n[j].wait_recv()
        nsb[k0:k1] = (npart[k0:k1, blk(t2), :].astype(F32) + nrb1[0, k0:k1].astype(F32)).astype(BF16)

    def far_send(j):
        k0, k1 = nsplit[j]
        c = remote(nsb.at[k0:k1], nrb2.at[k0:k1], 41 + j, {"tp": t2})
        c.start()
        far_n.append(c)

    far_step(0)
    keep_dy(QR, half - QR)
    far_send(0)
    grad_up(QR, half - QR)
    far_step(1)
    far_step(2)
    ex_up1 = remote(gup.at[:, rows_of(odp, QR), :], gup_rb.at[:, QR:64, :], 36, {"dp": odp})
    ex_up1.start()
    s3 = jnp.zeros((ch, nat), F32)
    for k in range(COEFS):
        rf = npart[k].astype(F32) * gcol[degree_of(k)]
        if k == 0:
            st0 = jnp.sum(rf, axis=0, keepdims=True)
            st1 = jnp.sum(rf * hat_s, axis=0, keepdims=True)
        else:
            s3 = s3 + rf * xg[k].astype(F32)
        if k == 4:
            far_send(1)
    st2 = jnp.sum(s3, axis=0, keepdims=True)
    st_snd[...] = jnp.concatenate([st0, st1, st2, jnp.zeros((5, nat), F32)], axis=0)
    ex_up0.wait_recv()
    gfin[:, rows_of(dp, 0), :] = (gup[:, rows_of(dp, 0), :] + gup_rb[:, 0:QR, :]).astype(BF16)
    ssend = []
    for j, dev in enumerate((t1, t2, t3)):
        c = remote(st_snd, st_all.at[j], 37 + j, {"tp": dev})
        c.start()
        ssend.append(c)
    far_send(2)
    near_d[1].wait_recv()
    far_d.wait_recv()
    own = dpart[:, blk(t), :].astype(F32) + rb1[1].astype(F32) + rb2[...].astype(F32)
    out_ref[...] = (xg[:, blk(t), :].astype(F32) + own).astype(BF16)
    bk_up0 = remote(gfin.at[:, rows_of(dp, 0), :], gfin.at[:, rows_of(dp, 0), :], 35, {"dp": odp})
    bk_up0.start()

    bk_dn.wait_recv()
    ddown_ref[...] = gfin_dn[0:5]
    dgate_ref[...] = gfin_dn[5].astype(F32).T.astype(BF16)
    ex_up1.wait_recv()
    gfin[:, rows_of(dp, QR), :] = (gup[:, rows_of(dp, QR), :] + gup_rb[:, QR:64, :]).astype(BF16)
    for c in ssend:
        c.wait_recv()
    stat = st_snd[...] + st_all[0] + st_all[1] + st_all[2]
    b0 = stat[0:1] / ch
    b1 = stat[1:2] / ch
    b2 = (inv_v * inv_v * inv_v) * (stat[2:3] / (ch * (COEFS - 1)))
    bk_up1 = remote(gfin.at[:, rows_of(dp, QR), :], gfin.at[:, rows_of(dp, QR), :], 40, {"dp": odp})
    bk_up1.start()
    near_o.wait_recv()
    for j, (k0, k1) in enumerate(nsplit):
        far_n[j].wait_recv()
        for k in range(k0, k1):
            dn = (npart[k, blk(t), :].astype(F32) + nrb1[1, k].astype(F32) + nrb2[k].astype(F32)).astype(BF16).astype(F32)
            dhat = dn * gcol[degree_of(k), blk(t), :]
            xk = xg[k, blk(t), :].astype(F32)
            if k == 0:
                dxk = inv_s * (dhat - b0 - (xk - mean_s) * inv_s * b1)
            else:
                dxk = inv_v * dhat - xk * b2
            dx_ref[k] = (dxk + gg[k, blk(t), :].astype(F32)).astype(BF16)

    bk_up0.wait_recv()
    bk_up1.wait_recv()
    for l in range(5):
        dup_ref[l] = gfin[l].astype(F32).T.astype(BF16)
    for c in far_g + fwd_x + fwd_g + gsend + near_d + near_n + far_n + ssend + [near_x, near_g, near_o, far_d, ex_dn, ex_up0, ex_up1, bk_dn, bk_up0, bk_up1]:
        c.wait_send()


def flush(a, b, c, d, e, oa, ob, oc, od, oe, sem):
    cs = [pltpu.make_async_copy(i, o, sem.at[j]) for j, (i, o) in enumerate(zip((a, b, c, d, e), (oa, ob, oc, od, oe)))]
    for x in cs:
        x.start()
    for x in cs:
        x.wait()


def solution(mesh):
    tp_size = mesh.shape['tp']
    act_spec = P('dp', None, 'tp')
    in_specs = (act_spec, P(None, 'tp'), P(None, None, 'tp'), P(None, 'tp'), P(None, 'tp', None), P(None, None), P(None, None), act_spec)
    out_specs = (act_spec, act_spec, P(None, None, 'tp'), P(None, 'tp'), P(None, 'tp', None))

    def local_step(x_loc, gain_loc, up_loc, gate_loc, down_loc, to_grid, from_grid, grad_loc):
        nat, coefs, cl = x_loc.shape
        ch = cl * tp_size
        grid_pts = to_grid.shape[1]
        pp = -(-grid_pts // 16) * 16
        xt = x_loc.transpose(1, 2, 0)
        gt = grad_loc.transpose(1, 2, 0)
        any_spec = pl.BlockSpec(memory_space=pl.ANY)
        vmem = pl.BlockSpec(memory_space=pltpu.VMEM)
        full = pltpu.VMEM((coefs, ch, nat), BF16)
        blkb = pltpu.VMEM((coefs, cl, nat), BF16)
        sq = lambda n, d: pltpu.VMEM((n, 128, 128), d)
        shapes = (xt.shape, xt.shape, up_loc.shape, gate_loc.shape, down_loc.shape)
        outs = pl.pallas_call(
            functools.partial(kernel, tp_size, grid_pts),
            out_shape=tuple(pltpu.VMEM(sh, BF16) for sh in shapes),
            in_specs=[any_spec] * 8,
            out_specs=[vmem] * 5,
            scratch_shapes=[
                full, full, full, full, full, full, full,
                pltpu.VMEM((66 * YSTRIDE, 128), F32), pltpu.VMEM((66 * YSTRIDE, 128), F32),
                pltpu.VMEM((KPAD * 136, 128), F32), pltpu.VMEM((64 * pp, 256), F32),
                pltpu.VMEM(gain_loc.shape, F32), pltpu.VMEM((8, 128), F32), pltpu.VMEM((3, 8, 128), F32), sq(5, F32),
                sq(5, BF16), pltpu.VMEM((128, 128), BF16), sq(5, BF16), sq(5, BF16), pltpu.VMEM((128, 128), BF16), sq(5, BF16),
                pltpu.VMEM(to_grid.shape, F32), pltpu.VMEM(from_grid.shape[::-1], F32),
                pltpu.VMEM((pp, KPAD), BF16), pltpu.VMEM((KPAD, 384), BF16), pltpu.VMEM((pp, KPAD), BF16), pltpu.VMEM((KPAD, 384), BF16),
                pltpu.VMEM((2, coefs, cl, nat), BF16), blkb, blkb, pltpu.VMEM((2, coefs, cl, nat), BF16), blkb, blkb,
                pltpu.VMEM((8, 128), F32), pltpu.VMEM((3, 8, 128), F32),
                sq(6, F32), pltpu.VMEM((6, 64, 128), F32), sq(5, F32), pltpu.VMEM((5, 64, 128), F32), sq(5, BF16), sq(6, BF16),
                pltpu.VMEM((128, nat), BF16),
                pltpu.VMEM((pp, 256), BF16), pltpu.VMEM((pp, 256), BF16), pltpu.VMEM((pp, 256), BF16), pltpu.VMEM((pp, 256), BF16),
                pltpu.VMEM((pp, 256), BF16), pltpu.VMEM((pp, 256), BF16), pltpu.VMEM((pp, 256), BF16), pltpu.VMEM((pp, 256), BF16),
                pltpu.SemaphoreType.DMA((12,)), pltpu.SemaphoreType.DMA((44,)), pltpu.SemaphoreType.DMA((44,)),
            ],
            compiler_params=pltpu.CompilerParams(collective_id=0, has_side_effects=True, vmem_limit_bytes=60 * 1024 * 1024),
        )(xt, gain_loc, up_loc, gate_loc, down_loc, to_grid, from_grid.T, gt)
        out_t, dx_t, d_up, d_gate, d_down = pl.pallas_call(
            flush,
            out_shape=tuple(jax.ShapeDtypeStruct(sh, BF16) for sh in shapes),
            in_specs=[vmem] * 5,
            out_specs=[any_spec] * 5,
            scratch_shapes=[pltpu.SemaphoreType.DMA((5,))],
        )(*[pltpu.with_memory_space_constraint(o, pltpu.VMEM) for o in outs])
        return out_t.transpose(2, 0, 1), dx_t.transpose(2, 0, 1), d_up, d_gate, d_down

    return jax.shard_map(local_step, mesh=mesh, in_specs=in_specs, out_specs=out_specs, check_vma=False)
```
